32 devices in a mesh: dp: 4 (over x, y), tp: 8 (over z, core).
Axes of the slice: x: 2, y: 2, z: 4, core: 2. Of those that a mesh axis runs over, the one named last changes fastest.
Arguments:
- x: bfloat16 [512, 5120], P('dp'), parts along dimension 0
- w_gate: bfloat16 [5120, 12288], P(None, 'tp')
- w_up: bfloat16 [5120, 12288], P(None, 'tp')
- w_down: bfloat16 [12288, 5120], P('tp')
Outputs:
- output: bfloat16 [512, 5120], P('dp'), parts along dimension 0
There are 4 independent parts. The reference program is written for one: setup_inputs(seed, part) draws one part's arguments, and reference() takes and returns one part's arrays. A program takes and returns all parts, laid end to end along the dimension named above; an argument that names none is the same for every part.
All inputs are finite; a program needn't handle non-finite values.
Results may differ from the reference program's by a relative error of at most 0.016.
Values are sent between devices in bfloat16 or wider.
A program may use at most 2 GiB of HBM per device.

```python
import jax
import jax.numpy as jnp

ROWS = 128
D = 5120
FF = 12288


def setup_inputs(seed: int = 0, part: int = 0) -> dict:
    kx, kg, ku, kd = jax.random.split(jax.random.key(seed), 4)
    drawn = {
        "x": jax.random.normal(jax.random.fold_in(kx, part), (ROWS, D), jnp.float32),
        "w_gate": jax.random.normal(kg, (D, FF), jnp.float32) * D**-0.5,
        "w_up": jax.random.normal(ku, (D, FF), jnp.float32) * D**-0.5,
        "w_down": jax.random.normal(kd, (FF, D), jnp.float32) * FF**-0.5,
    }
    return {k: v.astype(jnp.bfloat16) for k, v in drawn.items()}


def reference(x, w_gate, w_up, w_down):
    gate = jnp.dot(x, w_gate, preferred_element_type=jnp.float32)
    up = jnp.dot(x, w_up, preferred_element_type=jnp.float32)
    hidden = (jax.nn.silu(gate) * up).astype(jnp.bfloat16)
    return jnp.dot(hidden, w_down, preferred_element_type=jnp.float32).astype(jnp.bfloat16)
```

```python
import functools

import jax
import jax.numpy as jnp
from jax import lax
from jax.experimental import pallas as pl
from jax.experimental.pallas import tpu as pltpu
from jax.sharding import PartitionSpec as P

MESH = pl.DeviceIdType.MESH
F32, BF16 = jnp.float32, jnp.bfloat16

GU_COLS = 256
GU_PARTS = 4
Y_COLS = 256
D2D_LAG = 4
IN_START = 14
FIN_LAG = 4


def kernel(
    x_hbm, wg_hbm, wu_hbm, wd_hbm, y_ref,
    x_v, wg_v, wu_v, wd_v, g_acc, u_acc, hid, own, snd, rcv, part, a_rcv, b_rcv,
    x_sem, wg_sem, wu_sem, wd_sem,
    d_ss, d_rs, p_ss, p_rs, f_ss, f_rs, g_ss, g_rs,
):
    tp = lax.axis_index("tp")
    core = lax.rem(tp, 2)
    z = lax.div(tp, 2)
    sibling = tp + 1 - 2 * core
    inner = jnp.logical_and(z > 0, z < 3)
    outer = jnp.logical_not(inner)
    low = z < 2
    onward = jnp.where(low, tp + 2, tp - 2)
    back = jnp.where(low, tp - 2, tp + 2)

    rows, half = x_v.shape[0], x_v.shape[0] // 2
    kd = wg_v.shape[1]
    n_j = wg_v.shape[0] // GU_PARTS
    n_k = wd_v.shape[0]
    mine = pl.ds(pl.multiple_of(core * half, half), half)
    theirs = pl.ds(pl.multiple_of((1 - core) * half, half), half)

    barrier = pltpu.get_barrier_semaphore()
    pl.semaphore_signal(barrier, inc=1, device_id={"tp": sibling}, device_id_type=MESH)
    pl.semaphore_signal(barrier, inc=1, device_id={"tp": onward}, device_id_type=MESH)

    @pl.when(inner)
    def _():
        pl.semaphore_signal(barrier, inc=1, device_id={"tp": back}, device_id_type=MESH)

    def ycols(k):
        return pl.ds(pl.multiple_of(k * Y_COLS, Y_COLS), Y_COLS)

    def x_copy(part_rows, i):
        return pltpu.make_async_copy(
            x_hbm.at[part_rows, :], x_v.at[pl.ds(i * half, half), :], x_sem.at[i]
        )

    def gu_copy(hbm, vmem, sem, j, p):
        i = j * GU_PARTS + p
        return pltpu.make_async_copy(
            hbm.at[
                pl.ds(pl.multiple_of(p * kd, kd), kd),
                pl.ds(pl.multiple_of(j * GU_COLS, GU_COLS), GU_COLS),
            ],
            vmem.at[i],
            sem.at[i],
        )

    def wd_copy(k):
        return pltpu.make_async_copy(wd_hbm.at[:, ycols(k)], wd_v.at[k], wd_sem.at[k])

    x_copy(mine, 0).start()
    x_copy(theirs, 1).start()

    def start_gu(j, c):
        for p in range(GU_PARTS):
            gu_copy(wg_hbm, wg_v, wg_sem, j, p).start()
            gu_copy(wu_hbm, wu_v, wu_sem, j, p).start()
        return c

    lax.fori_loop(0, n_j, start_gu, 0)

    def start_wd(k, c):
        wd_copy(k).start()
        return c

    lax.fori_loop(0, n_k, start_wd, 0)

    x_copy(mine, 0).wait()
    x_copy(theirs, 1).wait()

    def gate_up(j, c):
        for p in range(GU_PARTS):
            i = j * GU_PARTS + p
            xs = x_v[:, p * kd : (p + 1) * kd]
            gu_copy(wg_hbm, wg_v, wg_sem, j, p).wait()
            gu_copy(wu_hbm, wu_v, wu_sem, j, p).wait()
            g = jnp.dot(xs, wg_v[i], preferred_element_type=F32)
            u = jnp.dot(xs, wu_v[i], preferred_element_type=F32)
            if p == 0:
                g_acc[...] = g
                u_acc[...] = u
            elif p < GU_PARTS - 1:
                g_acc[...] += g
                u_acc[...] += u
            else:
                g = g_acc[...] + g
                u = u_acc[...] + u
                hid[:, pl.ds(pl.multiple_of(j * GU_COLS, GU_COLS), GU_COLS)] = (
                    jax.nn.silu(g) * u
                ).astype(BF16)
        return c

    lax.fori_loop(0, n_j, gate_up, 0)

    def d2d(k):
        return pltpu.make_async_remote_copy(
            src_ref=snd.at[k], dst_ref=rcv.at[k], send_sem=d_ss.at[k], recv_sem=d_rs.at[k],
            device_id={"tp": sibling}, device_id_type=MESH,
        )

    def to_inner(k):
        return pltpu.make_async_remote_copy(
            src_ref=part.at[k], dst_ref=a_rcv.at[k], send_sem=p_ss.at[k], recv_sem=p_rs.at[0, k],
            device_id={"tp": onward}, device_id_type=MESH,
        )

    def across(k):
        return pltpu.make_async_remote_copy(
            src_ref=part.at[k], dst_ref=b_rcv.at[k], send_sem=p_ss.at[k], recv_sem=p_rs.at[1, k],
            device_id={"tp": onward}, device_id_type=MESH,
        )

    def to_outer(k):
        return pltpu.make_async_remote_copy(
            src_ref=y_ref.at[mine, ycols(k)], dst_ref=y_ref.at[mine, ycols(k)],
            send_sem=f_ss.at[k], recv_sem=f_rs.at[k],
            device_id={"tp": back}, device_id_type=MESH,
        )

    def share(k):
        return pltpu.make_async_remote_copy(
            src_ref=y_ref.at[mine, ycols(k)], dst_ref=y_ref.at[mine, ycols(k)],
            send_sem=g_ss.at[k], recv_sem=g_rs.at[k],
            device_id={"tp": sibling}, device_id_type=MESH,
        )

    def share_arrival(k):
        return pltpu.make_async_remote_copy(
            src_ref=y_ref.at[theirs, ycols(k)], dst_ref=y_ref.at[theirs, ycols(k)],
            send_sem=g_ss.at[k], recv_sem=g_rs.at[k],
            device_id={"tp": sibling}, device_id_type=MESH,
        )

    def term(k):
        wd_copy(k).wait()
        t = jnp.dot(hid[...], wd_v[k], preferred_element_type=F32)
        own[k] = t[:half]
        snd[k] = t[half:].astype(BF16)
        d2d(k).start()

    def outer_sum(k):
        d2d(k).wait_recv()
        part[k] = (own[k] + rcv[k].astype(F32)).astype(BF16)
        to_inner(k).start()

    def inner_sum(k):
        d2d(k).wait_recv()
        to_inner(k).wait_recv()
        part[k] = (own[k] + rcv[k].astype(F32) + a_rcv[k].astype(F32)).astype(BF16)
        across(k).start()

    def inner_final(k):
        across(k).wait_recv()
        y_ref[mine, ycols(k)] = (part[k].astype(F32) + b_rcv[k].astype(F32)).astype(BF16)
        to_outer(k).start()
        share(k).start()

    def outer_final(k):
        to_outer(k).wait_recv()
        share(k).start()

    @pl.when(inner)
    def _():
        pl.semaphore_wait(barrier, 3)

    @pl.when(outer)
    def _():
        pl.semaphore_wait(barrier, 2)

    def terms(k, c):
        term(k)

        @pl.when(jnp.logical_and(outer, k >= D2D_LAG))
        def _():
            outer_sum(k - D2D_LAG)

        @pl.when(jnp.logical_and(inner, k >= IN_START))
        def _():
            inner_sum(k - IN_START)

        return c

    lax.fori_loop(0, n_k, terms, 0)

    def loop(lo, hi, f):
        def it(k, c):
            f(k)
            return c

        lax.fori_loop(lo, hi, it, 0)

    @pl.when(outer)
    def _():
        loop(n_k - D2D_LAG, n_k, outer_sum)
        loop(0, n_k, outer_final)
        loop(0, n_k, lambda k: to_inner(k).wait_send())

    @pl.when(inner)
    def _():
        first = n_k - IN_START
        loop(0, first - FIN_LAG, inner_final)

        def both(k):
            inner_sum(k)
            inner_final(k - FIN_LAG)

        loop(max(first, FIN_LAG), n_k, both)
        loop(n_k - FIN_LAG, n_k, inner_final)

        def sent(k):
            across(k).wait_send()
            to_outer(k).wait_send()

        loop(0, n_k, sent)

    def finish(k):
        d2d(k).wait_send()
        share(k).wait_send()
        share_arrival(k).wait_recv()

    loop(0, n_k, finish)


def solution(mesh):
    def step(x, w_gate, w_up, w_down):
        rows, depth = x.shape
        width = w_gate.shape[1]
        out = w_down.shape[1]
        half = rows // 2
        n_gu = (width // GU_COLS) * GU_PARTS
        n_k = out // Y_COLS
        kd = depth // GU_PARTS
        dma = pltpu.SemaphoreType.DMA
        return pl.pallas_call(
            kernel,
            out_shape=jax.ShapeDtypeStruct((rows, out), BF16),
            in_specs=[pl.BlockSpec(memory_space=pl.ANY)] * 4,
            out_specs=pl.BlockSpec(memory_space=pltpu.VMEM),
            scratch_shapes=[
                pltpu.VMEM((rows, depth), BF16),
                pltpu.VMEM((n_gu, kd, GU_COLS), BF16),
                pltpu.VMEM((n_gu, kd, GU_COLS), BF16),
                pltpu.VMEM((n_k, width, Y_COLS), BF16),
                pltpu.VMEM((rows, GU_COLS), F32),
                pltpu.VMEM((rows, GU_COLS), F32),
                pltpu.VMEM((rows, width), BF16),
                pltpu.VMEM((n_k, half, Y_COLS), F32),
                pltpu.VMEM((n_k, half, Y_COLS), BF16),
                pltpu.VMEM((n_k, half, Y_COLS), BF16),
                pltpu.VMEM((n_k, half, Y_COLS), BF16),
                pltpu.VMEM((n_k, half, Y_COLS), BF16),
                pltpu.VMEM((n_k, half, Y_COLS), BF16),
                dma((2,)),
                dma((n_gu,)),
                dma((n_gu,)),
                dma((n_k,)),
                dma((n_k,)),
                dma((n_k,)),
                dma((n_k,)),
                dma((2, n_k)),
                dma((n_k,)),
                dma((n_k,)),
                dma((n_k,)),
                dma((n_k,)),
            ],
            compiler_params=pltpu.CompilerParams(
                collective_id=0, has_side_effects=True, vmem_limit_bytes=62 * 1024 * 1024
            ),
        )(x, w_gate, w_up, w_down)

    return jax.shard_map(
        step,
        mesh=mesh,
        in_specs=(P("dp", None), P(None, "tp"), P(None, "tp"), P("tp", None)),
        out_specs=P("dp", None),
        check_vma=False,
    )
```

```python
import functools

import jax
import jax.numpy as jnp
from jax import lax
from jax.experimental import pallas as pl
from jax.experimental.pallas import tpu as pltpu
from jax.sharding import PartitionSpec as P

MESH = pl.DeviceIdType.MESH
F32, BF16 = jnp.float32, jnp.bfloat16

GU_COLS = 256
GU_PARTS = 4
Y_COLS = 256
D2D_LAG = 4
IN_START = 14
FIN_LAG = 4


def kernel(
    x_hbm, wg_hbm, wu_hbm, wd_hbm, y_ref,
    x_v, wg_v, wu_v, wd_v, g_acc, u_acc, hid, own, snd, rcv, part, a_rcv, b_rcv,
    x_sem, wg_sem, wu_sem, wd_sem,
    d_ss, d_rs, p_ss, p_rs, f_ss, f_rs, g_ss, g_rs,
):
    tp = lax.axis_index("tp")
    core = lax.rem(tp, 2)
    z = lax.div(tp, 2)
    sibling = tp + 1 - 2 * core
    inner = jnp.logical_and(z > 0, z < 3)
    outer = jnp.logical_not(inner)
    low = z < 2
    onward = jnp.where(low, tp + 2, tp - 2)
    back = jnp.where(low, tp - 2, tp + 2)

    rows, half = x_v.shape[0], x_v.shape[0] // 2
    kd = wg_v.shape[1]
    n_j = wg_v.shape[0] // GU_PARTS
    n_k = wd_v.shape[0]
    mine = pl.ds(pl.multiple_of(core * half, half), half)
    theirs = pl.ds(pl.multiple_of((1 - core) * half, half), half)

    barrier = pltpu.get_barrier_semaphore()
    pl.semaphore_signal(barrier, inc=1, device_id={"tp": sibling}, device_id_type=MESH)
    pl.semaphore_signal(barrier, inc=1, device_id={"tp": onward}, device_id_type=MESH)

    @pl.when(inner)
    def _():
        pl.semaphore_signal(barrier, inc=1, device_id={"tp": back}, device_id_type=MESH)

    def ycols(k):
        return pl.ds(pl.multiple_of(k * Y_COLS, Y_COLS), Y_COLS)

    def x_copy(part_rows, i):
        return pltpu.make_async_copy(
            x_hbm.at[part_rows, :], x_v.at[pl.ds(i * half, half), :], x_sem.at[i]
        )

    def gu_copy(hbm, vmem, sem, j, p):
        i = j * GU_PARTS + p
        return pltpu.make_async_copy(
            hbm.at[
                pl.ds(pl.multiple_of(p * kd, kd), kd),
                pl.ds(pl.multiple_of(j * GU_COLS, GU_COLS), GU_COLS),
            ],
            vmem.at[i],
            sem.at[i],
        )

    def wd_copy(k):
        return pltpu.make_async_copy(wd_hbm.at[:, ycols(k)], wd_v.at[k], wd_sem.at[k])

    x_copy(mine, 0).start()
    x_copy(theirs, 1).start()

    def start_gu(j, c):
        for p in range(GU_PARTS):
            gu_copy(wg_hbm, wg_v, wg_sem, j, p).start()
            gu_copy(wu_hbm, wu_v, wu_sem, j, p).start()
        return c

    lax.fori_loop(0, n_j, start_gu, 0)

    def start_wd(k, c):
        wd_copy(k).start()
        return c

    lax.fori_loop(0, n_k, start_wd, 0)

    x_copy(mine, 0).wait()
    x_copy(theirs, 1).wait()

    def gate_up(j, c):
        for p in range(GU_PARTS):
            i = j * GU_PARTS + p
            xs = x_v[:, p * kd : (p + 1) * kd]
            gu_copy(wg_hbm, wg_v, wg_sem, j, p).wait()
            gu_copy(wu_hbm, wu_v, wu_sem, j, p).wait()
            g = jnp.dot(xs, wg_v[i], preferred_element_type=F32)
            u = jnp.dot(xs, wu_v[i], preferred_element_type=F32)
            if p == 0:
                g_acc[...] = g
                u_acc[...] = u
            elif p < GU_PARTS - 1:
                g_acc[...] += g
                u_acc[...] += u
            else:
                g = g_acc[...] + g
                u = u_acc[...] + u
                hid[:, pl.ds(pl.multiple_of(j * GU_COLS, GU_COLS), GU_COLS)] = (
                    jax.nn.silu(g) * u
                ).astype(BF16)
        return c

    lax.fori_loop(0, n_j, gate_up, 0)

    def d2d(k):
        return pltpu.make_async_remote_copy(
            src_ref=snd.at[k], dst_ref=rcv.at[k], send_sem=d_ss.at[k], recv_sem=d_rs.at[k],
            device_id={"tp": sibling}, device_id_type=MESH,
        )

    def to_inner(k):
        return pltpu.make_async_remote_copy(
            src_ref=part.at[k], dst_ref=a_rcv.at[k], send_sem=p_ss.at[k], recv_sem=p_rs.at[0, k],
            device_id={"tp": onward}, device_id_type=MESH,
        )

    def across(k):
        return pltpu.make_async_remote_copy(
            src_ref=part.at[k], dst_ref=b_rcv.at[k], send_sem=p_ss.at[k], recv_sem=p_rs.at[1, k],
            device_id={"tp": onward}, device_id_type=MESH,
        )

    def to_outer(k):
        return pltpu.make_async_remote_copy(
            src_ref=y_ref.at[mine, ycols(k)], dst_ref=y_ref.at[mine, ycols(k)],
            send_sem=f_ss.at[k], recv_sem=f_rs.at[k],
            device_id={"tp": back}, device_id_type=MESH,
        )

    def share(k):
        return pltpu.make_async_remote_copy(
            src_ref=y_ref.at[mine, ycols(k)], dst_ref=y_ref.at[mine, ycols(k)],
            send_sem=g_ss.at[k], recv_sem=g_rs.at[k],
            device_id={"tp": sibling}, device_id_type=MESH,
        )

    def share_arrival(k):
        return pltpu.make_async_remote_copy(
            src_ref=y_ref.at[theirs, ycols(k)], dst_ref=y_ref.at[theirs, ycols(k)],
            send_sem=g_ss.at[k], recv_sem=g_rs.at[k],
            device_id={"tp": sibling}, device_id_type=MESH,
        )

    def term(k):
        wd_copy(k).wait()
        t = jnp.dot(hid[...], wd_v[k], preferred_element_type=F32)
        own[k] = t[:half]
        snd[k] = t[half:].astype(BF16)
        d2d(k).start()

    def outer_sum(k):
        d2d(k).wait_recv()
        part[k] = (own[k] + rcv[k].astype(F32)).astype(BF16)
        to_inner(k).start()

    def inner_sum(k):
        d2d(k).wait_recv()
        to_inner(k).wait_recv()
        part[k] = (own[k] + rcv[k].astype(F32) + a_rcv[k].astype(F32)).astype(BF16)
        across(k).start()

    def inner_final(k):
        across(k).wait_recv()
        y_ref[mine, ycols(k)] = (part[k].astype(F32) + b_rcv[k].astype(F32)).astype(BF16)
        to_outer(k).start()
        share(k).start()

    def outer_final(k):
        to_outer(k).wait_recv()
        share(k).start()

    @pl.when(inner)
    def _():
        pl.semaphore_wait(barrier, 3)

    @pl.when(outer)
    def _():
        pl.semaphore_wait(barrier, 2)

    def terms(k, c):
        term(k)

        @pl.when(jnp.logical_and(outer, k >= D2D_LAG))
        def _():
            outer_sum(k - D2D_LAG)

        @pl.when(jnp.logical_and(inner, k >= IN_START))
        def _():
            inner_sum(k - IN_START)

        return c

    lax.fori_loop(0, n_k, terms, 0)

    def loop(lo, hi, f):
        def it(k, c):
            f(k)
            return c

        lax.fori_loop(lo, hi, it, 0)

    @pl.when(outer)
    def _():
        loop(n_k - D2D_LAG, n_k, outer_sum)
        loop(0, n_k, outer_final)
        loop(0, n_k, lambda k: to_inner(k).wait_send())

    @pl.when(inner)
    def _():
        first = n_k - IN_START
        loop(0, first - FIN_LAG, inner_final)

        def both(k):
            inner_sum(k)
            inner_final(k - FIN_LAG)

        loop(max(first, FIN_LAG), n_k, both)
        loop(n_k - FIN_LAG, n_k, inner_final)

        def sent(k):
            across(k).wait_send()
            to_outer(k).wait_send()

        loop(0, n_k, sent)

    def finish(k):
        d2d(k).wait_send()
        share(k).wait_send()
        share_arrival(k).wait_recv()

    loop(0, n_k, finish)


def solution(mesh):
    def step(x, w_gate, w_up, w_down):
        rows, depth = x.shape
        width = w_gate.shape[1]
        out = w_down.shape[1]
        half = rows // 2
        n_gu = (width // GU_COLS) * GU_PARTS
        n_k = out // Y_COLS
        kd = depth // GU_PARTS
        dma = pltpu.SemaphoreType.DMA
        return pl.pallas_call(
            kernel,
            out_shape=pltpu.VMEM((rows, out), BF16),
            in_specs=[pl.BlockSpec(memory_space=pl.ANY)] * 4,
            out_specs=pl.BlockSpec(memory_space=pltpu.VMEM),
            scratch_shapes=[
                pltpu.VMEM((rows, depth), BF16),
                pltpu.VMEM((n_gu, kd, GU_COLS), BF16),
                pltpu.VMEM((n_gu, kd, GU_COLS), BF16),
                pltpu.VMEM((n_k, width, Y_COLS), BF16),
                pltpu.VMEM((rows, GU_COLS), F32),
                pltpu.VMEM((rows, GU_COLS), F32),
                pltpu.VMEM((rows, width), BF16),
                pltpu.VMEM((n_k, half, Y_COLS), F32),
                pltpu.VMEM((n_k, half, Y_COLS), BF16),
                pltpu.VMEM((n_k, half, Y_COLS), BF16),
                pltpu.VMEM((n_k, half, Y_COLS), BF16),
                pltpu.VMEM((n_k, half, Y_COLS), BF16),
                pltpu.VMEM((n_k, half, Y_COLS), BF16),
                dma((2,)),
                dma((n_gu,)),
                dma((n_gu,)),
                dma((n_k,)),
                dma((n_k,)),
                dma((n_k,)),
                dma((n_k,)),
                dma((2, n_k)),
                dma((n_k,)),
                dma((n_k,)),
                dma((n_k,)),
                dma((n_k,)),
            ],
            compiler_params=pltpu.CompilerParams(
                collective_id=0, has_side_effects=True, vmem_limit_bytes=58 * 1024 * 1024
            ),
        )(x, w_gate, w_up, w_down)

    return jax.shard_map(
        step,
        mesh=mesh,
        in_specs=(P("dp", None), P(None, "tp"), P(None, "tp"), P("tp", None)),
        out_specs=P("dp", None),
        check_vma=False,
    )
```

```python
import functools

import jax
import jax.numpy as jnp
from jax import lax
from jax.experimental import pallas as pl
from jax.experimental.pallas import tpu as pltpu
from jax.sharding import PartitionSpec as P

MESH = pl.DeviceIdType.MESH
F32, BF16 = jnp.float32, jnp.bfloat16

GU_COLS = 256
GU_PARTS = 4
Y_COLS = 512
D2D_LAG = 2
IN_START = 8
FIN_LAG = 2


def kernel(
    x_hbm, wg_hbm, wu_hbm, wd_hbm, y_ref,
    x_v, wg_v, wu_v, wd_v, g_acc, u_acc, hid, own, snd, rcv, part, a_rcv, b_rcv,
    x_sem, wg_sem, wu_sem, wd_sem,
    d_ss, d_rs, p_ss, p_rs, f_ss, f_rs, g_ss, g_rs,
):
    tp = lax.axis_index("tp")
    core = lax.rem(tp, 2)
    z = lax.div(tp, 2)
    sibling = tp + 1 - 2 * core
    inner = jnp.logical_and(z > 0, z < 3)
    outer = jnp.logical_not(inner)
    low = z < 2
    onward = jnp.where(low, tp + 2, tp - 2)
    back = jnp.where(low, tp - 2, tp + 2)

    rows, half = x_v.shape[0], x_v.shape[0] // 2
    kd = wg_v.shape[1]
    n_j = wg_v.shape[0] // GU_PARTS
    n_k = wd_v.shape[0]
    mine = pl.ds(pl.multiple_of(core * half, half), half)
    theirs = pl.ds(pl.multiple_of((1 - core) * half, half), half)

    barrier = pltpu.get_barrier_semaphore()
    pl.semaphore_signal(barrier, inc=1, device_id={"tp": sibling}, device_id_type=MESH)
    pl.semaphore_signal(barrier, inc=1, device_id={"tp": onward}, device_id_type=MESH)

    @pl.when(inner)
    def _():
        pl.semaphore_signal(barrier, inc=1, device_id={"tp": back}, device_id_type=MESH)

    def ycols(k):
        return pl.ds(pl.multiple_of(k * Y_COLS, Y_COLS), Y_COLS)

    def x_copy(part_rows, i):
        return pltpu.make_async_copy(
            x_hbm.at[part_rows, :], x_v.at[pl.ds(i * half, half), :], x_sem.at[i]
        )

    def gu_copy(hbm, vmem, sem, j, p):
        i = j * GU_PARTS + p
        return pltpu.make_async_copy(
            hbm.at[
                pl.ds(pl.multiple_of(p * kd, kd), kd),
                pl.ds(pl.multiple_of(j * GU_COLS, GU_COLS), GU_COLS),
            ],
            vmem.at[i],
            sem.at[i],
        )

    def wd_copy(k):
        return pltpu.make_async_copy(wd_hbm.at[:, ycols(k)], wd_v.at[k], wd_sem.at[k])

    x_copy(mine, 0).start()
    x_copy(theirs, 1).start()

    def start_gu(j, c):
        for p in range(GU_PARTS):
            gu_copy(wg_hbm, wg_v, wg_sem, j, p).start()
            gu_copy(wu_hbm, wu_v, wu_sem, j, p).start()
        return c

    lax.fori_loop(0, n_j, start_gu, 0)

    def start_wd(k, c):
        wd_copy(k).start()
        return c

    lax.fori_loop(0, n_k, start_wd, 0)

    x_copy(mine, 0).wait()
    x_copy(theirs, 1).wait()

    def gate_up(j, c):
        for p in range(GU_PARTS):
            i = j * GU_PARTS + p
            xs = x_v[:, p * kd : (p + 1) * kd]
            gu_copy(wg_hbm, wg_v, wg_sem, j, p).wait()
            gu_copy(wu_hbm, wu_v, wu_sem, j, p).wait()
            g = jnp.dot(xs, wg_v[i], preferred_element_type=F32)
            u = jnp.dot(xs, wu_v[i], preferred_element_type=F32)
            if p == 0:
                g_acc[...] = g
                u_acc[...] = u
            elif p < GU_PARTS - 1:
                g_acc[...] += g
                u_acc[...] += u
            else:
                g = g_acc[...] + g
                u = u_acc[...] + u
                hid[:, pl.ds(pl.multiple_of(j * GU_COLS, GU_COLS), GU_COLS)] = (
                    jax.nn.silu(g) * u
                ).astype(BF16)
        return c

    lax.fori_loop(0, n_j, gate_up, 0)

    def d2d(k):
        return pltpu.make_async_remote_copy(
            src_ref=snd.at[k], dst_ref=rcv.at[k], send_sem=d_ss.at[k], recv_sem=d_rs.at[k],
            device_id={"tp": sibling}, device_id_type=MESH,
        )

    def to_inner(k):
        return pltpu.make_async_remote_copy(
            src_ref=part.at[k], dst_ref=a_rcv.at[k], send_sem=p_ss.at[k], recv_sem=p_rs.at[0, k],
            device_id={"tp": onward}, device_id_type=MESH,
        )

    def across(k):
        return pltpu.make_async_remote_copy(
            src_ref=part.at[k], dst_ref=b_rcv.at[k], send_sem=p_ss.at[k], recv_sem=p_rs.at[1, k],
            device_id={"tp": onward}, device_id_type=MESH,
        )

    def to_outer(k):
        return pltpu.make_async_remote_copy(
            src_ref=y_ref.at[mine, ycols(k)], dst_ref=y_ref.at[mine, ycols(k)],
            send_sem=f_ss.at[k], recv_sem=f_rs.at[k],
            device_id={"tp": back}, device_id_type=MESH,
        )

    def share(k):
        return pltpu.make_async_remote_copy(
            src_ref=y_ref.at[mine, ycols(k)], dst_ref=y_ref.at[mine, ycols(k)],
            send_sem=g_ss.at[k], recv_sem=g_rs.at[k],
            device_id={"tp": sibling}, device_id_type=MESH,
        )

    def share_arrival(k):
        return pltpu.make_async_remote_copy(
            src_ref=y_ref.at[theirs, ycols(k)], dst_ref=y_ref.at[theirs, ycols(k)],
            send_sem=g_ss.at[k], recv_sem=g_rs.at[k],
            device_id={"tp": sibling}, device_id_type=MESH,
        )

    def term(k):
        wd_copy(k).wait()
        t = jnp.dot(hid[...], wd_v[k], preferred_element_type=F32)
        own[k] = t[:half]
        snd[k] = t[half:].astype(BF16)
        d2d(k).start()

    def outer_sum(k):
        d2d(k).wait_recv()
        part[k] = (own[k] + rcv[k].astype(F32)).astype(BF16)
        to_inner(k).start()

    def inner_sum(k):
        d2d(k).wait_recv()
        to_inner(k).wait_recv()
        part[k] = (own[k] + rcv[k].astype(F32) + a_rcv[k].astype(F32)).astype(BF16)
        across(k).start()

    def inner_final(k):
        across(k).wait_recv()
        y_ref[mine, ycols(k)] = (part[k].astype(F32) + b_rcv[k].astype(F32)).astype(BF16)
        to_outer(k).start()
        share(k).start()

    def outer_final(k):
        to_outer(k).wait_recv()
        share(k).start()

    @pl.when(inner)
    def _():
        pl.semaphore_wait(barrier, 3)

    @pl.when(outer)
    def _():
        pl.semaphore_wait(barrier, 2)

    def terms(k, c):
        term(k)

        @pl.when(jnp.logical_and(outer, k >= D2D_LAG))
        def _():
            outer_sum(k - D2D_LAG)

        @pl.when(jnp.logical_and(inner, k >= IN_START))
        def _():
            inner_sum(k - IN_START)

        return c

    lax.fori_loop(0, n_k, terms, 0)

    def loop(lo, hi, f):
        def it(k, c):
            f(k)
            return c

        lax.fori_loop(lo, hi, it, 0)

    @pl.when(outer)
    def _():
        loop(n_k - D2D_LAG, n_k, outer_sum)
        loop(0, n_k, outer_final)
        loop(0, n_k, lambda k: to_inner(k).wait_send())

    @pl.when(inner)
    def _():
        first = n_k - IN_START
        loop(0, first - FIN_LAG, inner_final)

        def both(k):
            inner_sum(k)
            inner_final(k - FIN_LAG)

        loop(max(first, FIN_LAG), n_k, both)
        loop(n_k - FIN_LAG, n_k, inner_final)

        def sent(k):
            across(k).wait_send()
            to_outer(k).wait_send()

        loop(0, n_k, sent)

    def finish(k):
        d2d(k).wait_send()
        share(k).wait_send()
        share_arrival(k).wait_recv()

    loop(0, n_k, finish)


def solution(mesh):
    def step(x, w_gate, w_up, w_down):
        rows, depth = x.shape
        width = w_gate.shape[1]
        out = w_down.shape[1]
        half = rows // 2
        n_gu = (width // GU_COLS) * GU_PARTS
        n_k = out // Y_COLS
        kd = depth // GU_PARTS
        dma = pltpu.SemaphoreType.DMA
        return pl.pallas_call(
            kernel,
            out_shape=pltpu.VMEM((rows, out), BF16),
            in_specs=[pl.BlockSpec(memory_space=pl.ANY)] * 4,
            out_specs=pl.BlockSpec(memory_space=pltpu.VMEM),
            scratch_shapes=[
                pltpu.VMEM((rows, depth), BF16),
                pltpu.VMEM((n_gu, kd, GU_COLS), BF16),
                pltpu.VMEM((n_gu, kd, GU_COLS), BF16),
                pltpu.VMEM((n_k, width, Y_COLS), BF16),
                pltpu.VMEM((rows, GU_COLS), F32),
                pltpu.VMEM((rows, GU_COLS), F32),
                pltpu.VMEM((rows, width), BF16),
                pltpu.VMEM((n_k, half, Y_COLS), F32),
                pltpu.VMEM((n_k, half, Y_COLS), BF16),
                pltpu.VMEM((n_k, half, Y_COLS), BF16),
                pltpu.VMEM((n_k, half, Y_COLS), BF16),
                pltpu.VMEM((n_k, half, Y_COLS), BF16),
                pltpu.VMEM((n_k, half, Y_COLS), BF16),
                dma((2,)),
                dma((n_gu,)),
                dma((n_gu,)),
                dma((n_k,)),
                dma((n_k,)),
                dma((n_k,)),
                dma((n_k,)),
                dma((2, n_k)),
                dma((n_k,)),
                dma((n_k,)),
                dma((n_k,)),
                dma((n_k,)),
            ],
            compiler_params=pltpu.CompilerParams(
                collective_id=0, has_side_effects=True, vmem_limit_bytes=58 * 1024 * 1024
            ),
        )(x, w_gate, w_up, w_down)

    return jax.shard_map(
        step,
        mesh=mesh,
        in_specs=(P("dp", None), P(None, "tp"), P(None, "tp"), P("tp", None)),
        out_specs=P("dp", None),
        check_vma=False,
    )
```

```python
import jax
import jax.numpy as jnp
from jax import lax
from jax.experimental import pallas as pl
from jax.experimental.pallas import tpu as pltpu
from jax.sharding import PartitionSpec as P

MESH = pl.DeviceIdType.MESH
F32, BF16 = jnp.float32, jnp.bfloat16

GU_COLS = 256
GU_PARTS = 4
UNIT = 128
PIECES = (
    (1, 1), (0, 2), (1, 2), (0, 2), (1, 3), (0, 3), (1, 4), (0, 4),
    (1, 4), (0, 4), (1, 4), (0, 2), (1, 2), (0, 1), (1, 1), (1, 1),
)
HEAD = (0,)
TAIL = (15,)
OUT_LAG = 9
IN_START, IN_RATE = 28, 3.0
HOP = 7.0


def layout():
    u, local, pieces = 0, [0, 0], []
    for owner, n in PIECES:
        pieces.append((owner, u, n, local[owner]))
        u += n
        local[owner] += n
    return pieces, u, max(local)


def kernel(
    x_hbm, wg_hbm, wu_hbm, wd_hbm, y_ref,
    x_v, wg_v, wu_v, wd_v, g_acc, u_acc, hid, own, snd, rcv, part, a_rcv, b_rcv, h_rcv,
    x_sem, wg_sem, wu_sem, wd_sem,
    d_ss, d_rs, a_ss, a_rs, b_ss, b_rs, f_ss, f_rs, g_ss, g_rs, h_ss, h_rs, t_ss,
):
    pieces, _, _ = layout()
    count = len(pieces)
    tp = lax.axis_index("tp")
    core = lax.rem(tp, 2)
    z = lax.div(tp, 2)
    sibling = tp + 1 - 2 * core
    inner = jnp.logical_and(z > 0, z < 3)
    outer = jnp.logical_not(inner)
    low = z < 2
    step = jnp.where(low, 2, -2)
    onward = tp + step
    back = tp - step
    far = tp + 2 * step

    kd = wg_v.shape[1]
    n_j = wg_v.shape[0] // GU_PARTS
    depth = x_v.shape[1]

    def signal(dev):
        pl.semaphore_signal(barrier, inc=1, device_id={"tp": dev}, device_id_type=MESH)

    barrier = pltpu.get_barrier_semaphore()
    signal(sibling)
    signal(onward)
    signal(far)
    signal(jnp.where(inner, back, onward) + 1 - 2 * core)

    @pl.when(inner)
    def _():
        signal(back)

    def cols(c):
        _, u, n, _ = pieces[c]
        return slice(u * UNIT, (u + n) * UNIT)

    def held(c):
        _, _, n, at = pieces[c]
        return slice(at, at + n)

    def made(c):
        _, u, n, _ = pieces[c]
        return slice(u, u + n)

    def gu_copy(hbm, vmem, sem, j, p):
        i = j * GU_PARTS + p
        return pltpu.make_async_copy(
            hbm.at[
                pl.ds(pl.multiple_of(p * kd, kd), kd),
                pl.ds(pl.multiple_of(j * GU_COLS, GU_COLS), GU_COLS),
            ],
            vmem.at[i],
            sem.at[i],
        )

    def wd_copy(c):
        return pltpu.make_async_copy(wd_hbm.at[:, cols(c)], wd_v.at[:, cols(c)], wd_sem.at[c])

    x_copy = pltpu.make_async_copy(x_hbm, x_v, x_sem)
    x_copy.start()

    def start_gu(j, c):
        for p in range(GU_PARTS):
            gu_copy(wg_hbm, wg_v, wg_sem, j, p).start()
            gu_copy(wu_hbm, wu_v, wu_sem, j, p).start()
        return c

    lax.fori_loop(0, n_j, start_gu, 0)
    for c in range(count):
        wd_copy(c).start()
    x_copy.wait()

    def gate_up(j, carry):
        for p in range(GU_PARTS):
            i = j * GU_PARTS + p
            xs = x_v[:, p * kd : (p + 1) * kd]
            gu_copy(wg_hbm, wg_v, wg_sem, j, p).wait()
            gu_copy(wu_hbm, wu_v, wu_sem, j, p).wait()
            g = jnp.dot(xs, wg_v[i], preferred_element_type=F32)
            u = jnp.dot(xs, wu_v[i], preferred_element_type=F32)
            if p == 0:
                g_acc[...] = g
                u_acc[...] = u
            elif p < GU_PARTS - 1:
                g_acc[...] += g
                u_acc[...] += u
            else:
                g = g_acc[...] + g
                u = u_acc[...] + u
                hid[:, pl.ds(pl.multiple_of(j * GU_COLS, GU_COLS), GU_COLS)] = (
                    jax.nn.silu(g) * u
                ).astype(BF16)
        return carry

    lax.fori_loop(0, n_j, gate_up, 0)

    def remote(src, dst, send, recv, dev):
        return pltpu.make_async_remote_copy(
            src_ref=src, dst_ref=dst, send_sem=send, recv_sem=recv,
            device_id={"tp": dev}, device_id_type=MESH,
        )

    def exchange(c):
        return remote(snd.at[made(c)], rcv.at[held(c)], d_ss.at[c], d_rs.at[c], sibling)

    def inward(c):
        src = snd.at[made(c)] if c in HEAD else part.at[held(c)]
        return remote(src, a_rcv.at[held(c)], a_ss.at[c], a_rs.at[c], onward)

    def inward_other(c):
        dev = onward + 1 - 2 * core
        return remote(snd.at[made(c)], h_rcv.at[held(c)], h_ss.at[c], h_rs.at[c], dev)

    def across(c):
        return remote(part.at[held(c)], b_rcv.at[held(c)], b_ss.at[c], b_rs.at[c], onward)

    def across_far(c):
        return remote(part.at[held(c)], b_rcv.at[held(c)], t_ss.at[c], b_rs.at[c], far)

    def across_back(c):
        return remote(part.at[held(c)], a_rcv.at[held(c)], a_ss.at[c], a_rs.at[c], back)

    def outward(c):
        return remote(y_ref.at[:, cols(c)], y_ref.at[:, cols(c)], f_ss.at[c], f_rs.at[c], back)

    def share(c):
        return remote(y_ref.at[:, cols(c)], y_ref.at[:, cols(c)], g_ss.at[c], g_rs.at[c], sibling)

    def term(c):
        owner, u, n, _ = pieces[c]
        wd_copy(c).wait()
        t = jnp.dot(hid[...], wd_v[:, cols(c)], preferred_element_type=F32)
        for i in range(n):
            ti = t[:, i * UNIT : (i + 1) * UNIT]
            own[u + i] = ti
            snd[u + i] = ti.astype(BF16)
        if c in HEAD:

            @pl.when(jnp.logical_and(core == owner, outer))
            def _():
                inward(c).start()

            @pl.when(jnp.logical_and(core != owner, outer))
            def _():
                inward_other(c).start()

            @pl.when(jnp.logical_and(core != owner, inner))
            def _():
                exchange(c).start()
        else:

            @pl.when(core != owner)
            def _():
                exchange(c).start()

    def outer_sum(c):
        exchange(c).wait_recv()
        part[held(c)] = (own[made(c)] + rcv[held(c)].astype(F32)).astype(BF16)
        inward(c).start()

    def inner_sum(c):
        exchange(c).wait_recv()
        inward(c).wait_recv()
        total = own[made(c)] + rcv[held(c)].astype(F32) + a_rcv[held(c)].astype(F32)
        if c in HEAD:
            inward_other(c).wait_recv()
            total = total + h_rcv[held(c)].astype(F32)
        part[held(c)] = total.astype(BF16)
        across(c).start()
        if c in TAIL:
            across_far(c).start()
            across_back(c).start()

    def store_sum(c, first):
        _, u, n, at = pieces[c]
        for i in range(n):
            y_ref[:, (u + i) * UNIT : (u + i + 1) * UNIT] = (
                first[at + i].astype(F32) + b_rcv[at + i].astype(F32)
            ).astype(BF16)

    def inner_final(c):
        across(c).wait_recv()
        store_sum(c, part)
        if c not in TAIL:
            outward(c).start()
        share(c).start()

    def outer_final(c):
        if c in TAIL:
            inward(c).wait_recv()
            across(c).wait_recv()
            store_sum(c, a_rcv)
        else:
            outward(c).wait_recv()
        share(c).start()

    @pl.when(inner)
    def _():
        pl.semaphore_wait(barrier, 5)

    @pl.when(outer)
    def _():
        pl.semaphore_wait(barrier, 4)

    ends = [u + n for _, u, n, _ in pieces]
    owned = [[c for c in range(count) if pieces[c][0] == k] for k in (0, 1)]
    out_left = [[c for c in owned[k] if c not in HEAD] for k in (0, 1)]
    in_left = [list(owned[k]) for k in (0, 1)]
    for c in range(count):
        term(c)
        for k in (0, 1):
            now_out = [d for d in out_left[k] if ends[d] + OUT_LAG <= ends[c]]
            now_in = [d for d in in_left[k] if IN_START + IN_RATE * pieces[d][1] <= ends[c]]
            out_left[k] = [d for d in out_left[k] if d not in now_out]
            in_left[k] = [d for d in in_left[k] if d not in now_in]
            if now_out:

                @pl.when(jnp.logical_and(outer, core == k))
                def _():
                    for d in now_out:
                        outer_sum(d)

            if now_in:

                @pl.when(jnp.logical_and(inner, core == k))
                def _():
                    for d in now_in:
                        inner_sum(d)

    for k in (0, 1):
        mine, theirs = owned[k], owned[1 - k]

        @pl.when(jnp.logical_and(outer, core == k))
        def _():
            for d in out_left[k]:
                outer_sum(d)
            for d in mine:
                outer_final(d)
            for d in mine:
                inward(d).wait_send()
                share(d).wait_send()
            for d in theirs:
                (inward_other(d) if d in HEAD else exchange(d)).wait_send()
                share(d).wait_recv()

        @pl.when(jnp.logical_and(inner, core == k))
        def _():
            events = [(ends[d], 0, d) for d in in_left[k]]
            events += [(ends[d] + HOP, 1, d) for d in mine]
            for _, what, d in sorted(events):
                (inner_final if what else inner_sum)(d)
            for d in mine:
                across(d).wait_send()
                if d in TAIL:
                    across_far(d).wait_send()
                    across_back(d).wait_send()
                else:
                    outward(d).wait_send()
                share(d).wait_send()
            for d in theirs:
                exchange(d).wait_send()
                share(d).wait_recv()


def solution(mesh):
    def step(x, w_gate, w_up, w_down):
        rows, depth = x.shape
        width = w_gate.shape[1]
        out = w_down.shape[1]
        pieces, units, most = layout()
        n_gu = (width // GU_COLS) * GU_PARTS
        kd = depth // GU_PARTS
        count = len(pieces)
        dma = pltpu.SemaphoreType.DMA
        return pl.pallas_call(
            kernel,
            out_shape=pltpu.VMEM((rows, out), BF16),
            in_specs=[pl.BlockSpec(memory_space=pl.ANY)] * 4,
            out_specs=pl.BlockSpec(memory_space=pltpu.VMEM),
            scratch_shapes=[
                pltpu.VMEM((rows, depth), BF16),
                pltpu.VMEM((n_gu, kd, GU_COLS), BF16),
                pltpu.VMEM((n_gu, kd, GU_COLS), BF16),
                pltpu.VMEM((width, out), BF16),
                pltpu.VMEM((rows, GU_COLS), F32),
                pltpu.VMEM((rows, GU_COLS), F32),
                pltpu.VMEM((rows, width), BF16),
                pltpu.VMEM((units, rows, UNIT), F32),
                pltpu.VMEM((units, rows, UNIT), BF16),
                pltpu.VMEM((most, rows, UNIT), BF16),
                pltpu.VMEM((most, rows, UNIT), BF16),
                pltpu.VMEM((most, rows, UNIT), BF16),
                pltpu.VMEM((most, rows, UNIT), BF16),
                pltpu.VMEM((pieces[max(HEAD)][3] + pieces[max(HEAD)][2], rows, UNIT), BF16),
                dma,
                dma((n_gu,)),
                dma((n_gu,)),
            ]
            + [dma((count,))] * 14,
            compiler_params=pltpu.CompilerParams(
                collective_id=0, has_side_effects=True, vmem_limit_bytes=60 * 1024 * 1024
            ),
        )(x, w_gate, w_up, w_down)

    return jax.shard_map(
        step,
        mesh=mesh,
        in_specs=(P("dp", None), P(None, "tp"), P(None, "tp"), P("tp", None)),
        out_specs=P("dp", None),
        check_vma=False,
    )
```

```python
import jax
import jax.numpy as jnp
from jax import lax
from jax.experimental import pallas as pl
from jax.experimental.pallas import tpu as pltpu
from jax.sharding import PartitionSpec as P

MESH = pl.DeviceIdType.MESH
F32, BF16 = jnp.float32, jnp.bfloat16

GU_COLS = 256
GU_PARTS = 4
UNIT = 128
GROUPS = ((1, 1),) + ((1, 0),) * 18 + ((1, 1),)
HEAD = (0,)
TAIL = (39,)
OUT_LAG = 9
IN_START, IN_RATE = 28, 3.0
HOP = 7.0


def layout():
    local, pieces = [0, 0], []
    for u, owner in enumerate(o for g in GROUPS for o in g):
        pieces.append((owner, u, 1, local[owner]))
        local[owner] += 1
    return pieces, len(pieces), max(local)


def kernel(
    x_hbm, wg_hbm, wu_hbm, wd_hbm, y_ref,
    x_v, wg_v, wu_v, wd_v, g_acc, u_acc, hid, own, snd, rcv, part, a_rcv, b_rcv, h_rcv,
    x_sem, wg_sem, wu_sem, wd_sem,
    d_ss, d_rs, a_ss, a_rs, b_ss, b_rs, f_ss, f_rs, g_ss, g_rs, h_ss, h_rs, t_ss,
):
    pieces, _, _ = layout()
    count = len(pieces)
    tp = lax.axis_index("tp")
    core = lax.rem(tp, 2)
    z = lax.div(tp, 2)
    sibling = tp + 1 - 2 * core
    inner = jnp.logical_and(z > 0, z < 3)
    outer = jnp.logical_not(inner)
    low = z < 2
    step = jnp.where(low, 2, -2)
    onward = tp + step
    back = tp - step
    far = tp + 2 * step

    kd = wg_v.shape[1]
    n_j = wg_v.shape[0] // GU_PARTS
    depth = x_v.shape[1]

    def signal(dev):
        pl.semaphore_signal(barrier, inc=1, device_id={"tp": dev}, device_id_type=MESH)

    barrier = pltpu.get_barrier_semaphore()
    signal(sibling)
    signal(onward)
    signal(far)
    signal(jnp.where(inner, back, onward) + 1 - 2 * core)

    @pl.when(inner)
    def _():
        signal(back)

    def cols(c):
        _, u, n, _ = pieces[c]
        return slice(u * UNIT, (u + n) * UNIT)

    def held(c):
        _, _, n, at = pieces[c]
        return slice(at, at + n)

    def made(c):
        _, u, n, _ = pieces[c]
        return slice(u, u + n)

    def gu_copy(hbm, vmem, sem, j, p):
        i = j * GU_PARTS + p
        return pltpu.make_async_copy(
            hbm.at[
                pl.ds(pl.multiple_of(p * kd, kd), kd),
                pl.ds(pl.multiple_of(j * GU_COLS, GU_COLS), GU_COLS),
            ],
            vmem.at[i],
            sem.at[i],
        )

    starts = [sum(map(len, GROUPS[:i])) for i in range(len(GROUPS) + 1)]

    def wd_copy(i):
        block = slice(starts[i] * UNIT, starts[i + 1] * UNIT)
        return pltpu.make_async_copy(wd_hbm.at[:, block], wd_v.at[:, block], wd_sem.at[i])

    x_copy = pltpu.make_async_copy(x_hbm, x_v, x_sem)
    x_copy.start()

    def start_gu(j, c):
        for p in range(GU_PARTS):
            gu_copy(wg_hbm, wg_v, wg_sem, j, p).start()
            gu_copy(wu_hbm, wu_v, wu_sem, j, p).start()
        return c

    lax.fori_loop(0, n_j, start_gu, 0)
    for i in range(len(GROUPS)):
        wd_copy(i).start()
    x_copy.wait()

    def gate_up(j, carry):
        for p in range(GU_PARTS):
            i = j * GU_PARTS + p
            xs = x_v[:, p * kd : (p + 1) * kd]
            gu_copy(wg_hbm, wg_v, wg_sem, j, p).wait()
            gu_copy(wu_hbm, wu_v, wu_sem, j, p).wait()
            g = jnp.dot(xs, wg_v[i], preferred_element_type=F32)
            u = jnp.dot(xs, wu_v[i], preferred_element_type=F32)
            if p == 0:
                g_acc[...] = g
                u_acc[...] = u
            elif p < GU_PARTS - 1:
                g_acc[...] += g
                u_acc[...] += u
            else:
                g = g_acc[...] + g
                u = u_acc[...] + u
                hid[:, pl.ds(pl.multiple_of(j * GU_COLS, GU_COLS), GU_COLS)] = (
                    jax.nn.silu(g) * u
                ).astype(BF16)
        return carry

    lax.fori_loop(0, n_j, gate_up, 0)

    def remote(src, dst, send, recv, dev):
        return pltpu.make_async_remote_copy(
            src_ref=src, dst_ref=dst, send_sem=send, recv_sem=recv,
            device_id={"tp": dev}, device_id_type=MESH,
        )

    def exchange(c):
        return remote(snd.at[made(c)], rcv.at[held(c)], d_ss.at[c], d_rs.at[c], sibling)

    def inward(c):
        src = snd.at[made(c)] if c in HEAD else part.at[held(c)]
        return remote(src, a_rcv.at[held(c)], a_ss.at[c], a_rs.at[c], onward)

    def inward_other(c):
        dev = onward + 1 - 2 * core
        return remote(snd.at[made(c)], h_rcv.at[held(c)], h_ss.at[c], h_rs.at[c], dev)

    def across(c):
        return remote(part.at[held(c)], b_rcv.at[held(c)], b_ss.at[c], b_rs.at[c], onward)

    def across_far(c):
        return remote(part.at[held(c)], b_rcv.at[held(c)], t_ss.at[c], b_rs.at[c], far)

    def across_back(c):
        return remote(part.at[held(c)], a_rcv.at[held(c)], a_ss.at[c], a_rs.at[c], back)

    def outward(c):
        return remote(y_ref.at[:, cols(c)], y_ref.at[:, cols(c)], f_ss.at[c], f_rs.at[c], back)

    def share(c):
        return remote(y_ref.at[:, cols(c)], y_ref.at[:, cols(c)], g_ss.at[c], g_rs.at[c], sibling)

    def term(i):
        lo, hi = starts[i], starts[i + 1]
        wd_copy(i).wait()
        t = jnp.dot(hid[...], wd_v[:, lo * UNIT : hi * UNIT], preferred_element_type=F32)
        for c in range(lo, hi):
            tc = t[:, (c - lo) * UNIT : (c - lo + 1) * UNIT]
            own[c] = tc
            snd[c] = tc.astype(BF16)
        for c in range(lo, hi):
            owner = pieces[c][0]
            if c in HEAD:

                @pl.when(jnp.logical_and(core == owner, outer))
                def _():
                    inward(c).start()

                @pl.when(jnp.logical_and(core != owner, outer))
                def _():
                    inward_other(c).start()

                @pl.when(jnp.logical_and(core != owner, inner))
                def _():
                    exchange(c).start()
            else:

                @pl.when(core != owner)
                def _():
                    exchange(c).start()

    def outer_sum(c):
        exchange(c).wait_recv()
        part[held(c)] = (own[made(c)] + rcv[held(c)].astype(F32)).astype(BF16)
        inward(c).start()

    def inner_sum(c):
        exchange(c).wait_recv()
        inward(c).wait_recv()
        total = own[made(c)] + rcv[held(c)].astype(F32) + a_rcv[held(c)].astype(F32)
        if c in HEAD:
            inward_other(c).wait_recv()
            total = total + h_rcv[held(c)].astype(F32)
        part[held(c)] = total.astype(BF16)
        across(c).start()
        if c in TAIL:
            across_far(c).start()
            across_back(c).start()

    def store_sum(c, first):
        _, u, n, at = pieces[c]
        for i in range(n):
            y_ref[:, (u + i) * UNIT : (u + i + 1) * UNIT] = (
                first[at + i].astype(F32) + b_rcv[at + i].astype(F32)
            ).astype(BF16)

    def inner_final(c):
        across(c).wait_recv()
        store_sum(c, part)
        if c not in TAIL:
            outward(c).start()
        share(c).start()

    def outer_final(c):
        if c in TAIL:
            inward(c).wait_recv()
            across(c).wait_recv()
            store_sum(c, a_rcv)
        else:
            outward(c).wait_recv()
        share(c).start()

    @pl.when(inner)
    def _():
        pl.semaphore_wait(barrier, 5)

    @pl.when(outer)
    def _():
        pl.semaphore_wait(barrier, 4)

    ends = [u + n for _, u, n, _ in pieces]
    owned = [[c for c in range(count) if pieces[c][0] == k] for k in (0, 1)]
    out_left = [[c for c in owned[k] if c not in HEAD] for k in (0, 1)]
    in_left = [list(owned[k]) for k in (0, 1)]
    for i in range(len(GROUPS)):
        term(i)
        for k in (0, 1):
            now_out = [d for d in out_left[k] if ends[d] + OUT_LAG <= starts[i + 1]]
            now_in = [d for d in in_left[k] if IN_START + IN_RATE * d <= starts[i + 1]]
            out_left[k] = [d for d in out_left[k] if d not in now_out]
            in_left[k] = [d for d in in_left[k] if d not in now_in]
            if now_out:

                @pl.when(jnp.logical_and(outer, core == k))
                def _():
                    for d in now_out:
                        outer_sum(d)

            if now_in:

                @pl.when(jnp.logical_and(inner, core == k))
                def _():
                    for d in now_in:
                        inner_sum(d)

    for k in (0, 1):
        mine, theirs = owned[k], owned[1 - k]

        @pl.when(jnp.logical_and(outer, core == k))
        def _():
            for d in out_left[k]:
                outer_sum(d)
            for d in mine:
                outer_final(d)
            for d in mine:
                inward(d).wait_send()
                share(d).wait_send()
            for d in theirs:
                (inward_other(d) if d in HEAD else exchange(d)).wait_send()
                share(d).wait_recv()

        @pl.when(jnp.logical_and(inner, core == k))
        def _():
            events = [(ends[d], 0, d) for d in in_left[k]]
            events += [(ends[d] + HOP, 1, d) for d in mine]
            for _, what, d in sorted(events):
                (inner_final if what else inner_sum)(d)
            for d in mine:
                across(d).wait_send()
                if d in TAIL:
                    across_far(d).wait_send()
                    across_back(d).wait_send()
                else:
                    outward(d).wait_send()
                share(d).wait_send()
            for d in theirs:
                exchange(d).wait_send()
                share(d).wait_recv()


def solution(mesh):
    def step(x, w_gate, w_up, w_down):
        rows, depth = x.shape
        width = w_gate.shape[1]
        out = w_down.shape[1]
        pieces, units, most = layout()
        n_gu = (width // GU_COLS) * GU_PARTS
        kd = depth // GU_PARTS
        count = len(pieces)
        dma = pltpu.SemaphoreType.DMA
        return pl.pallas_call(
            kernel,
            out_shape=pltpu.VMEM((rows, out), BF16),
            in_specs=[pl.BlockSpec(memory_space=pl.ANY)] * 4,
            out_specs=pl.BlockSpec(memory_space=pltpu.VMEM),
            scratch_shapes=[
                pltpu.VMEM((rows, depth), BF16),
                pltpu.VMEM((n_gu, kd, GU_COLS), BF16),
                pltpu.VMEM((n_gu, kd, GU_COLS), BF16),
                pltpu.VMEM((width, out), BF16),
                pltpu.VMEM((rows, GU_COLS), F32),
                pltpu.VMEM((rows, GU_COLS), F32),
                pltpu.VMEM((rows, width), BF16),
                pltpu.VMEM((units, rows, UNIT), F32),
                pltpu.VMEM((units, rows, UNIT), BF16),
                pltpu.VMEM((most, rows, UNIT), BF16),
                pltpu.VMEM((most, rows, UNIT), BF16),
                pltpu.VMEM((most, rows, UNIT), BF16),
                pltpu.VMEM((most, rows, UNIT), BF16),
                pltpu.VMEM((pieces[max(HEAD)][3] + pieces[max(HEAD)][2], rows, UNIT), BF16),
                dma,
                dma((n_gu,)),
                dma((n_gu,)),
            ]
            + [dma((count,))] * 14,
            compiler_params=pltpu.CompilerParams(
                collective_id=0, has_side_effects=True, vmem_limit_bytes=60 * 1024 * 1024
            ),
        )(x, w_gate, w_up, w_down)

    return jax.shard_map(
        step,
        mesh=mesh,
        in_specs=(P("dp", None), P(None, "tp"), P(None, "tp"), P("tp", None)),
        out_specs=P("dp", None),
        check_vma=False,
    )
```

```python
import jax
import jax.numpy as jnp
from jax import lax
from jax.experimental import pallas as pl
from jax.experimental.pallas import tpu as pltpu
from jax.sharding import PartitionSpec as P

MESH = pl.DeviceIdType.MESH
F32, BF16 = jnp.float32, jnp.bfloat16

GU_COLS = 256
GU_PARTS = 4
UNIT = 128
EDGE = 1
OUT_LAG = 5
IN_START = 14
FIN_LAG = (4, 3)


def kernel(
    x_hbm, wg_hbm, wu_hbm, wd_hbm, y_ref,
    x_v, wg_v, wu_v, wd_v, g_acc, u_acc, hid, own, snd, rcv, part, a_rcv, b_rcv, h_rcv,
    x_sem, wg_sem, wu_sem, wd_sem,
    d_ss, d_rs, a_ss, a_rs, b_ss, b_rs, f_ss, f_rs, g_ss, g_rs, h_ss, h_rs, t_ss,
):
    pairs, units = wd_v.shape[0], 2 * wd_v.shape[0]
    last = units - 1
    tp = lax.axis_index("tp")
    core = lax.rem(tp, 2)
    z = lax.div(tp, 2)
    sibling = tp + 1 - 2 * core
    inner = jnp.logical_and(z > 0, z < 3)
    outer = jnp.logical_not(inner)
    low = z < 2
    step = jnp.where(low, 2, -2)
    onward = tp + step
    back = tp - step
    far = tp + 2 * step

    kd = wg_v.shape[1]
    n_j = wg_v.shape[0] // GU_PARTS
    depth = x_v.shape[1]

    def signal(dev):
        pl.semaphore_signal(barrier, inc=1, device_id={"tp": dev}, device_id_type=MESH)

    barrier = pltpu.get_barrier_semaphore()
    signal(sibling)
    signal(onward)
    signal(far)
    signal(jnp.where(inner, back, onward) + 1 - 2 * core)

    @pl.when(inner)
    def _():
        signal(back)

    most = pairs + 2 * EDGE
    owned = jnp.where(core == 1, most, pairs - 2 * EDGE)

    def unit(i):
        edge = jnp.where(i < 2 * EDGE, i, i + units - most)
        middle = jnp.logical_and(i >= 2 * EDGE, i < most - 2 * EDGE)
        return jnp.where(
            core == 1, jnp.where(middle, 2 * (i - EDGE), edge), 2 * (i + EDGE) + 1
        )

    def mine(u):
        middle = jnp.logical_and(u >= 2 * EDGE, u < units - 2 * EDGE)
        zero = jnp.logical_and(middle, lax.rem(u, 2) == 1)
        return jnp.where(zero, 0, 1) == core

    def cols(u):
        return pl.ds(pl.multiple_of(u * UNIT, UNIT), UNIT)

    def gu_copy(hbm, vmem, sem, j, p):
        i = j * GU_PARTS + p
        return pltpu.make_async_copy(
            hbm.at[
                pl.ds(pl.multiple_of(p * kd, kd), kd),
                pl.ds(pl.multiple_of(j * GU_COLS, GU_COLS), GU_COLS),
            ],
            vmem.at[i],
            sem.at[i],
        )

    def wd_copy(k):
        block = pl.ds(pl.multiple_of(k * 2 * UNIT, 2 * UNIT), 2 * UNIT)
        return pltpu.make_async_copy(wd_hbm.at[:, block], wd_v.at[k], wd_sem.at[k])

    def loop(lo, hi, f):
        def it(k, carry):
            f(k)
            return carry

        lax.fori_loop(lo, hi, it, 0)

    x_copy = pltpu.make_async_copy(x_hbm, x_v, x_sem)
    x_copy.start()

    def start_gu(j, c):
        for p in range(GU_PARTS):
            gu_copy(wg_hbm, wg_v, wg_sem, j, p).start()
            gu_copy(wu_hbm, wu_v, wu_sem, j, p).start()
        return c

    lax.fori_loop(0, n_j, start_gu, 0)
    loop(0, pairs, lambda k: wd_copy(k).start())
    x_copy.wait()

    def gate_up(j, carry):
        for p in range(GU_PARTS):
            i = j * GU_PARTS + p
            xs = x_v[:, p * kd : (p + 1) * kd]
            gu_copy(wg_hbm, wg_v, wg_sem, j, p).wait()
            gu_copy(wu_hbm, wu_v, wu_sem, j, p).wait()
            g = jnp.dot(xs, wg_v[i], preferred_element_type=F32)
            u = jnp.dot(xs, wu_v[i], preferred_element_type=F32)
            if p == 0:
                g_acc[...] = g
                u_acc[...] = u
            elif p < GU_PARTS - 1:
                g_acc[...] += g
                u_acc[...] += u
            else:
                g = g_acc[...] + g
                u = u_acc[...] + u
                hid[:, pl.ds(pl.multiple_of(j * GU_COLS, GU_COLS), GU_COLS)] = (
                    jax.nn.silu(g) * u
                ).astype(BF16)
        return carry

    lax.fori_loop(0, n_j, gate_up, 0)

    def remote(src, dst, send, recv, dev):
        return pltpu.make_async_remote_copy(
            src_ref=src, dst_ref=dst, send_sem=send, recv_sem=recv,
            device_id={"tp": dev}, device_id_type=MESH,
        )

    def exchange(u):
        return remote(snd.at[u], rcv.at[u], d_ss.at[u], d_rs.at[u], sibling)

    def inward(u):
        return remote(part.at[u], a_rcv.at[u], a_ss.at[u], a_rs.at[u], onward)

    def head_own():
        return remote(snd.at[0], a_rcv.at[0], a_ss.at[0], a_rs.at[0], onward)

    def head_other():
        return remote(snd.at[0], h_rcv, h_ss, h_rs, onward + 1 - 2 * core)

    def across(u):
        return remote(part.at[u], b_rcv.at[u], b_ss.at[u], b_rs.at[u], onward)

    def across_far():
        return remote(part.at[last], b_rcv.at[last], t_ss, b_rs.at[last], far)

    def across_back():
        return remote(part.at[last], a_rcv.at[last], a_ss.at[last], a_rs.at[last], back)

    def outward(u):
        return remote(y_ref.at[:, cols(u)], y_ref.at[:, cols(u)], f_ss.at[u], f_rs.at[u], back)

    def share(u):
        return remote(y_ref.at[:, cols(u)], y_ref.at[:, cols(u)], g_ss.at[u], g_rs.at[u], sibling)

    def term(k):
        wd_copy(k).wait()
        t = jnp.dot(hid[...], wd_v[k], preferred_element_type=F32)
        for i in range(2):
            ti = t[:, i * UNIT : (i + 1) * UNIT]
            own[2 * k + i] = ti
            snd[2 * k + i] = ti.astype(BF16)
        for i in range(2):
            u = 2 * k + i
            direct = jnp.logical_and(u == 0, outer)

            @pl.when(jnp.logical_and(jnp.logical_not(mine(u)), jnp.logical_not(direct)))
            def _():
                exchange(u).start()

        @pl.when(jnp.logical_and(k == 0, outer))
        def _():
            @pl.when(core == 1)
            def _():
                head_own().start()

            @pl.when(core == 0)
            def _():
                head_other().start()

    def outer_sum(u):
        exchange(u).wait_recv()
        part[u] = (own[u] + rcv[u].astype(F32)).astype(BF16)
        inward(u).start()

    def outer_sums(k):
        for i in range(2):
            u = 2 * k + i

            @pl.when(jnp.logical_and(mine(u), u > 0))
            def _():
                outer_sum(u)

    def inner_sum(i):
        u = unit(i)

        @pl.when(u == 0)
        def _():
            head_other().wait_recv()
            own[0] = own[0] + h_rcv[...].astype(F32)

        exchange(u).wait_recv()
        inward(u).wait_recv()
        part[u] = (own[u] + rcv[u].astype(F32) + a_rcv[u].astype(F32)).astype(BF16)
        across(u).start()

        @pl.when(u == last)
        def _():
            across_far().start()
            across_back().start()

    def inner_final(i):
        u = unit(i)
        across(u).wait_recv()
        y_ref[:, cols(u)] = (part[u].astype(F32) + b_rcv[u].astype(F32)).astype(BF16)

        @pl.when(u < last)
        def _():
            outward(u).start()

        share(u).start()

    def outer_final(i):
        u = unit(i)
        outward(u).wait_recv()
        share(u).start()

    @pl.when(inner)
    def _():
        pl.semaphore_wait(barrier, 5)

    @pl.when(outer)
    def _():
        pl.semaphore_wait(barrier, 4)

    def terms(k):
        term(k)

        @pl.when(jnp.logical_and(outer, k >= OUT_LAG))
        def _():
            outer_sums(k - OUT_LAG)

        @pl.when(jnp.logical_and(inner, k >= IN_START))
        def _():
            inner_sum(k - IN_START)

    loop(0, pairs, terms)

    @pl.when(outer)
    def _():
        loop(pairs - OUT_LAG, pairs, outer_sums)
        loop(0, jnp.where(core == 1, owned - 1, owned), outer_final)

        @pl.when(core == 1)
        def _():
            across_back().wait_recv()
            across(last).wait_recv()
            y_ref[:, cols(last)] = (
                a_rcv[last].astype(F32) + b_rcv[last].astype(F32)
            ).astype(BF16)
            share(last).start()

        def sent(i):
            inward(unit(i)).wait_send()

        loop(0, owned, sent)

    @pl.when(inner)
    def _():
        lag = jnp.where(core == 1, FIN_LAG[1], FIN_LAG[0])
        done = pairs - IN_START
        loop(0, done - lag, inner_final)

        def both(i):
            inner_sum(i)
            inner_final(i - lag)

        loop(done, owned, both)
        loop(owned - lag, owned, inner_final)

        def sent(i):
            u = unit(i)
            across(u).wait_send()

            @pl.when(u < last)
            def _():
                outward(u).wait_send()

            @pl.when(u == last)
            def _():
                across_far().wait_send()
                across_back().wait_send()

        loop(0, owned, sent)

    def finish(u):
        @pl.when(mine(u))
        def _():
            share(u).wait_send()

        @pl.when(jnp.logical_not(mine(u)))
        def _():
            share(u).wait_recv()
            direct = jnp.logical_and(u == 0, outer)

            @pl.when(direct)
            def _():
                head_other().wait_send()

            @pl.when(jnp.logical_not(direct))
            def _():
                exchange(u).wait_send()

    loop(0, units, finish)


def solution(mesh):
    def step(x, w_gate, w_up, w_down):
        rows, depth = x.shape
        width = w_gate.shape[1]
        out = w_down.shape[1]
        units = out // UNIT
        pairs = units // 2
        n_gu = (width // GU_COLS) * GU_PARTS
        kd = depth // GU_PARTS
        dma = pltpu.SemaphoreType.DMA
        return pl.pallas_call(
            kernel,
            out_shape=pltpu.VMEM((rows, out), BF16),
            in_specs=[pl.BlockSpec(memory_space=pl.ANY)] * 4,
            out_specs=pl.BlockSpec(memory_space=pltpu.VMEM),
            scratch_shapes=[
                pltpu.VMEM((rows, depth), BF16),
                pltpu.VMEM((n_gu, kd, GU_COLS), BF16),
                pltpu.VMEM((n_gu, kd, GU_COLS), BF16),
                pltpu.VMEM((pairs, width, 2 * UNIT), BF16),
                pltpu.VMEM((rows, GU_COLS), F32),
                pltpu.VMEM((rows, GU_COLS), F32),
                pltpu.VMEM((rows, width), BF16),
                pltpu.VMEM((units, rows, UNIT), F32),
            ]
            + [pltpu.VMEM((units, rows, UNIT), BF16)] * 5
            + [pltpu.VMEM((rows, UNIT), BF16), dma, dma((n_gu,)), dma((n_gu,)), dma((pairs,))]
            + [dma((units,))] * 10
            + [dma] * 3,
            compiler_params=pltpu.CompilerParams(
                collective_id=0, has_side_effects=True, vmem_limit_bytes=60 * 1024 * 1024
            ),
        )(x, w_gate, w_up, w_down)

    return jax.shard_map(
        step,
        mesh=mesh,
        in_specs=(P("dp", None), P(None, "tp"), P(None, "tp"), P("tp", None)),
        out_specs=P("dp", None),
        check_vma=False,
    )
```

```python
import functools

import jax
import jax.numpy as jnp
from jax import lax
from jax.experimental import pallas as pl
from jax.experimental.pallas import tpu as pltpu
from jax.sharding import PartitionSpec as P

MESH = pl.DeviceIdType.MESH
F32, BF16 = jnp.float32, jnp.bfloat16

GU_COLS = 256
GU_PARTS = 4
Y_COLS = 256
D2D_LAG = 4
IN_START = 14
FIN_LAG = 5


def kernel(
    x_hbm, wg_hbm, wu_hbm, wd_hbm, y_ref,
    x_v, wg_v, wu_v, wd_v, g_acc, u_acc, hid, own, snd, rcv, part, a_rcv, b_rcv,
    x_sem, wg_sem, wu_sem, wd_sem,
    d_ss, d_rs, p_ss, p_rs, f_ss, f_rs, g_ss, g_rs,
):
    tp = lax.axis_index("tp")
    core = lax.rem(tp, 2)
    z = lax.div(tp, 2)
    sibling = tp + 1 - 2 * core
    inner = jnp.logical_and(z > 0, z < 3)
    outer = jnp.logical_not(inner)
    low = z < 2
    onward = jnp.where(low, tp + 2, tp - 2)
    back = jnp.where(low, tp - 2, tp + 2)

    rows, half = x_v.shape[0], x_v.shape[0] // 2
    kd = wg_v.shape[1]
    n_j = wg_v.shape[0] // GU_PARTS
    n_k = wd_v.shape[0]
    mine = pl.ds(pl.multiple_of(core * half, half), half)
    theirs = pl.ds(pl.multiple_of((1 - core) * half, half), half)

    barrier = pltpu.get_barrier_semaphore()
    pl.semaphore_signal(barrier, inc=1, device_id={"tp": sibling}, device_id_type=MESH)
    pl.semaphore_signal(barrier, inc=1, device_id={"tp": onward}, device_id_type=MESH)

    @pl.when(inner)
    def _():
        pl.semaphore_signal(barrier, inc=1, device_id={"tp": back}, device_id_type=MESH)

    def ycols(k):
        return pl.ds(pl.multiple_of(k * Y_COLS, Y_COLS), Y_COLS)

    def x_copy(part_rows, i):
        return pltpu.make_async_copy(
            x_hbm.at[part_rows, :], x_v.at[pl.ds(i * half, half), :], x_sem.at[i]
        )

    def gu_copy(hbm, vmem, sem, j, p):
        i = j * GU_PARTS + p
        return pltpu.make_async_copy(
            hbm.at[
                pl.ds(pl.multiple_of(p * kd, kd), kd),
                pl.ds(pl.multiple_of(j * GU_COLS, GU_COLS), GU_COLS),
            ],
            vmem.at[i],
            sem.at[i],
        )

    def wd_copy(k):
        return pltpu.make_async_copy(wd_hbm.at[:, ycols(k)], wd_v.at[k], wd_sem.at[k])

    x_copy(mine, 0).start()
    x_copy(theirs, 1).start()

    def start_gu(j, c):
        for p in range(GU_PARTS):
            gu_copy(wg_hbm, wg_v, wg_sem, j, p).start()
            gu_copy(wu_hbm, wu_v, wu_sem, j, p).start()
        return c

    lax.fori_loop(0, n_j, start_gu, 0)

    def start_wd(k, c):
        wd_copy(k).start()
        return c

    lax.fori_loop(0, n_k, start_wd, 0)

    x_copy(mine, 0).wait()
    x_copy(theirs, 1).wait()

    def gate_up(j, c):
        for p in range(GU_PARTS):
            i = j * GU_PARTS + p
            xs = x_v[:, p * kd : (p + 1) * kd]
            gu_copy(wg_hbm, wg_v, wg_sem, j, p).wait()
            gu_copy(wu_hbm, wu_v, wu_sem, j, p).wait()
            g = jnp.dot(xs, wg_v[i], preferred_element_type=F32)
            u = jnp.dot(xs, wu_v[i], preferred_element_type=F32)
            if p == 0:
                g_acc[...] = g
                u_acc[...] = u
            elif p < GU_PARTS - 1:
                g_acc[...] += g
                u_acc[...] += u
            else:
                g = g_acc[...] + g
                u = u_acc[...] + u
                hid[:, pl.ds(pl.multiple_of(j * GU_COLS, GU_COLS), GU_COLS)] = (
                    jax.nn.silu(g) * u
                ).astype(BF16)
        return c

    lax.fori_loop(0, n_j, gate_up, 0)

    def d2d(k):
        return pltpu.make_async_remote_copy(
            src_ref=snd.at[k], dst_ref=rcv.at[k], send_sem=d_ss.at[k], recv_sem=d_rs.at[k],
            device_id={"tp": sibling}, device_id_type=MESH,
        )

    def to_inner(k):
        return pltpu.make_async_remote_copy(
            src_ref=part.at[k], dst_ref=a_rcv.at[k], send_sem=p_ss.at[k], recv_sem=p_rs.at[0, k],
            device_id={"tp": onward}, device_id_type=MESH,
        )

    def across(k):
        return pltpu.make_async_remote_copy(
            src_ref=part.at[k], dst_ref=b_rcv.at[k], send_sem=p_ss.at[k], recv_sem=p_rs.at[1, k],
            device_id={"tp": onward}, device_id_type=MESH,
        )

    def to_outer(k):
        return pltpu.make_async_remote_copy(
            src_ref=y_ref.at[mine, ycols(k)], dst_ref=y_ref.at[mine, ycols(k)],
            send_sem=f_ss.at[k], recv_sem=f_rs.at[k],
            device_id={"tp": back}, device_id_type=MESH,
        )

    def share(k):
        return pltpu.make_async_remote_copy(
            src_ref=y_ref.at[mine, ycols(k)], dst_ref=y_ref.at[mine, ycols(k)],
            send_sem=g_ss.at[k], recv_sem=g_rs.at[k],
            device_id={"tp": sibling}, device_id_type=MESH,
        )

    def share_arrival(k):
        return pltpu.make_async_remote_copy(
            src_ref=y_ref.at[theirs, ycols(k)], dst_ref=y_ref.at[theirs, ycols(k)],
            send_sem=g_ss.at[k], recv_sem=g_rs.at[k],
            device_id={"tp": sibling}, device_id_type=MESH,
        )

    def term(k):
        wd_copy(k).wait()
        t = jnp.dot(hid[...], wd_v[k], preferred_element_type=F32)
        own[k] = t[:half]
        snd[k] = t[half:].astype(BF16)
        d2d(k).start()

    def outer_sum(k):
        d2d(k).wait_recv()
        part[k] = (own[k] + rcv[k].astype(F32)).astype(BF16)
        to_inner(k).start()

    def inner_sum(k):
        d2d(k).wait_recv()
        to_inner(k).wait_recv()
        part[k] = (own[k] + rcv[k].astype(F32) + a_rcv[k].astype(F32)).astype(BF16)
        across(k).start()

    def inner_final(k):
        across(k).wait_recv()
        y_ref[mine, ycols(k)] = (part[k].astype(F32) + b_rcv[k].astype(F32)).astype(BF16)
        to_outer(k).start()
        share(k).start()

    def outer_final(k):
        to_outer(k).wait_recv()
        share(k).start()

    @pl.when(inner)
    def _():
        pl.semaphore_wait(barrier, 3)

    @pl.when(outer)
    def _():
        pl.semaphore_wait(barrier, 2)

    def terms(k, c):
        term(k)

        @pl.when(jnp.logical_and(outer, k >= D2D_LAG))
        def _():
            outer_sum(k - D2D_LAG)

        @pl.when(jnp.logical_and(inner, k >= IN_START))
        def _():
            inner_sum(k - IN_START)

        return c

    lax.fori_loop(0, n_k, terms, 0)

    def loop(lo, hi, f):
        def it(k, c):
            f(k)
            return c

        lax.fori_loop(lo, hi, it, 0)

    @pl.when(outer)
    def _():
        loop(n_k - D2D_LAG, n_k, outer_sum)
        loop(0, n_k, outer_final)
        loop(0, n_k, lambda k: to_inner(k).wait_send())

    @pl.when(inner)
    def _():
        first = n_k - IN_START
        loop(0, first - FIN_LAG, inner_final)

        def both(k):
            inner_sum(k)
            inner_final(k - FIN_LAG)

        loop(max(first, FIN_LAG), n_k, both)
        loop(n_k - FIN_LAG, n_k, inner_final)

        def sent(k):
            across(k).wait_send()
            to_outer(k).wait_send()

        loop(0, n_k, sent)

    def finish(k):
        d2d(k).wait_send()
        share(k).wait_send()
        share_arrival(k).wait_recv()

    loop(0, n_k, finish)


def solution(mesh):
    def step(x, w_gate, w_up, w_down):
        rows, depth = x.shape
        width = w_gate.shape[1]
        out = w_down.shape[1]
        half = rows // 2
        n_gu = (width // GU_COLS) * GU_PARTS
        n_k = out // Y_COLS
        kd = depth // GU_PARTS
        dma = pltpu.SemaphoreType.DMA
        return pl.pallas_call(
            kernel,
            out_shape=pltpu.VMEM((rows, out), BF16),
            in_specs=[pl.BlockSpec(memory_space=pl.ANY)] * 4,
            out_specs=pl.BlockSpec(memory_space=pltpu.VMEM),
            scratch_shapes=[
                pltpu.VMEM((rows, depth), BF16),
                pltpu.VMEM((n_gu, kd, GU_COLS), BF16),
                pltpu.VMEM((n_gu, kd, GU_COLS), BF16),
                pltpu.VMEM((n_k, width, Y_COLS), BF16),
                pltpu.VMEM((rows, GU_COLS), F32),
                pltpu.VMEM((rows, GU_COLS), F32),
                pltpu.VMEM((rows, width), BF16),
                pltpu.VMEM((n_k, half, Y_COLS), F32),
                pltpu.VMEM((n_k, half, Y_COLS), BF16),
                pltpu.VMEM((n_k, half, Y_COLS), BF16),
                pltpu.VMEM((n_k, half, Y_COLS), BF16),
                pltpu.VMEM((n_k, half, Y_COLS), BF16),
                pltpu.VMEM((n_k, half, Y_COLS), BF16),
                dma((2,)),
                dma((n_gu,)),
                dma((n_gu,)),
                dma((n_k,)),
                dma((n_k,)),
                dma((n_k,)),
                dma((n_k,)),
                dma((2, n_k)),
                dma((n_k,)),
                dma((n_k,)),
                dma((n_k,)),
                dma((n_k,)),
            ],
            compiler_params=pltpu.CompilerParams(
                collective_id=0, has_side_effects=True, vmem_limit_bytes=58 * 1024 * 1024
            ),
        )(x, w_gate, w_up, w_down)

    return jax.shard_map(
        step,
        mesh=mesh,
        in_specs=(P("dp", None), P(None, "tp"), P(None, "tp"), P("tp", None)),
        out_specs=P("dp", None),
        check_vma=False,
    )
```

```python
import jax
import jax.numpy as jnp
from jax import lax
from jax.experimental import pallas as pl
from jax.experimental.pallas import tpu as pltpu
from jax.sharding import PartitionSpec as P

MESH = pl.DeviceIdType.MESH
F32, BF16 = jnp.float32, jnp.bfloat16

GU_COLS = 256
GU_PARTS = 4
UNIT = 128
EDGE = 1
OUT_LAG = 5
IN_START = 14
FIN_LAG = (5, 4)


def kernel(
    x_hbm, wg_hbm, wu_hbm, wd_hbm, y_ref,
    x_v, wg_v, wu_v, wd_v, g_acc, u_acc, hid, own, snd, rcv, part, a_rcv, b_rcv, h_rcv,
    x_sem, wg_sem, wu_sem, wd_sem,
    d_ss, d_rs, a_ss, a_rs, b_ss, b_rs, f_ss, f_rs, g_ss, g_rs, h_ss, h_rs, t_ss,
):
    pairs, units = wd_v.shape[0], 2 * wd_v.shape[0]
    last = units - 1
    tp = lax.axis_index("tp")
    core = lax.rem(tp, 2)
    z = lax.div(tp, 2)
    sibling = tp + 1 - 2 * core
    inner = jnp.logical_and(z > 0, z < 3)
    outer = jnp.logical_not(inner)
    low = z < 2
    step = jnp.where(low, 2, -2)
    onward = tp + step
    back = tp - step
    far = tp + 2 * step

    kd = wg_v.shape[1]
    n_j = wg_v.shape[0] // GU_PARTS
    depth = x_v.shape[1]

    def signal(dev):
        pl.semaphore_signal(barrier, inc=1, device_id={"tp": dev}, device_id_type=MESH)

    barrier = pltpu.get_barrier_semaphore()
    signal(sibling)
    signal(onward)
    signal(far)
    signal(jnp.where(inner, back, onward) + 1 - 2 * core)

    @pl.when(inner)
    def _():
        signal(back)

    most = pairs + 2 * EDGE
    owned = jnp.where(core == 1, most, pairs - 2 * EDGE)

    def unit(i):
        edge = jnp.where(i < 2 * EDGE, i, i + units - most)
        middle = jnp.logical_and(i >= 2 * EDGE, i < most - 2 * EDGE)
        return jnp.where(
            core == 1, jnp.where(middle, 2 * (i - EDGE), edge), 2 * (i + EDGE) + 1
        )

    def mine(u):
        middle = jnp.logical_and(u >= 2 * EDGE, u < units - 2 * EDGE)
        zero = jnp.logical_and(middle, lax.rem(u, 2) == 1)
        return jnp.where(zero, 0, 1) == core

    def cols(u):
        return pl.ds(pl.multiple_of(u * UNIT, UNIT), UNIT)

    def gu_copy(hbm, vmem, sem, j, p):
        i = j * GU_PARTS + p
        return pltpu.make_async_copy(
            hbm.at[
                pl.ds(pl.multiple_of(p * kd, kd), kd),
                pl.ds(pl.multiple_of(j * GU_COLS, GU_COLS), GU_COLS),
            ],
            vmem.at[i],
            sem.at[i],
        )

    def wd_copy(k):
        block = pl.ds(pl.multiple_of(k * 2 * UNIT, 2 * UNIT), 2 * UNIT)
        return pltpu.make_async_copy(wd_hbm.at[:, block], wd_v.at[k], wd_sem.at[k])

    def loop(lo, hi, f):
        def it(k, carry):
            f(k)
            return carry

        lax.fori_loop(lo, hi, it, 0)

    x_copy = pltpu.make_async_copy(x_hbm, x_v, x_sem)
    x_copy.start()

    def start_gu(j, c):
        for p in range(GU_PARTS):
            gu_copy(wg_hbm, wg_v, wg_sem, j, p).start()
            gu_copy(wu_hbm, wu_v, wu_sem, j, p).start()
        return c

    lax.fori_loop(0, n_j, start_gu, 0)
    loop(0, pairs, lambda k: wd_copy(k).start())
    x_copy.wait()

    def gate_up(j, carry):
        for p in range(GU_PARTS):
            i = j * GU_PARTS + p
            xs = x_v[:, p * kd : (p + 1) * kd]
            gu_copy(wg_hbm, wg_v, wg_sem, j, p).wait()
            gu_copy(wu_hbm, wu_v, wu_sem, j, p).wait()
            g = jnp.dot(xs, wg_v[i], preferred_element_type=F32)
            u = jnp.dot(xs, wu_v[i], preferred_element_type=F32)
            if p == 0:
                g_acc[...] = g
                u_acc[...] = u
            elif p < GU_PARTS - 1:
                g_acc[...] += g
                u_acc[...] += u
            else:
                g = g_acc[...] + g
                u = u_acc[...] + u
                hid[:, pl.ds(pl.multiple_of(j * GU_COLS, GU_COLS), GU_COLS)] = (
                    jax.nn.silu(g) * u
                ).astype(BF16)
        return carry

    lax.fori_loop(0, n_j, gate_up, 0)

    def remote(src, dst, send, recv, dev):
        return pltpu.make_async_remote_copy(
            src_ref=src, dst_ref=dst, send_sem=send, recv_sem=recv,
            device_id={"tp": dev}, device_id_type=MESH,
        )

    def exchange(u):
        return remote(snd.at[u], rcv.at[u], d_ss.at[u], d_rs.at[u], sibling)

    def inward(u):
        return remote(part.at[u], a_rcv.at[u], a_ss.at[u], a_rs.at[u], onward)

    def head_own():
        return remote(snd.at[0], a_rcv.at[0], a_ss.at[0], a_rs.at[0], onward)

    def head_other():
        return remote(snd.at[0], h_rcv, h_ss, h_rs, onward + 1 - 2 * core)

    def across(u):
        return remote(part.at[u], b_rcv.at[u], b_ss.at[u], b_rs.at[u], onward)

    def across_far():
        return remote(part.at[last], b_rcv.at[last], t_ss, b_rs.at[last], far)

    def across_back():
        return remote(part.at[last], a_rcv.at[last], a_ss.at[last], a_rs.at[last], back)

    def outward(u):
        return remote(y_ref.at[:, cols(u)], y_ref.at[:, cols(u)], f_ss.at[u], f_rs.at[u], back)

    def share(u):
        return remote(y_ref.at[:, cols(u)], y_ref.at[:, cols(u)], g_ss.at[u], g_rs.at[u], sibling)

    def term(k):
        wd_copy(k).wait()
        t = jnp.dot(hid[...], wd_v[k], preferred_element_type=F32)
        for i in range(2):
            ti = t[:, i * UNIT : (i + 1) * UNIT]
            own[2 * k + i] = ti
            snd[2 * k + i] = ti.astype(BF16)
        for i in range(2):
            u = 2 * k + i
            direct = jnp.logical_and(u == 0, outer)

            @pl.when(jnp.logical_and(jnp.logical_not(mine(u)), jnp.logical_not(direct)))
            def _():
                exchange(u).start()

        @pl.when(jnp.logical_and(k == 0, outer))
        def _():
            @pl.when(core == 1)
            def _():
                head_own().start()

            @pl.when(core == 0)
            def _():
                head_other().start()

    def outer_sum(u):
        exchange(u).wait_recv()
        part[u] = (own[u] + rcv[u].astype(F32)).astype(BF16)
        inward(u).start()

    def outer_sums(k):
        for i in range(2):
            u = 2 * k + i

            @pl.when(jnp.logical_and(mine(u), u > 0))
            def _():
                outer_sum(u)

    def inner_sum(i):
        u = unit(i)

        @pl.when(u == 0)
        def _():
            head_other().wait_recv()
            own[0] = own[0] + h_rcv[...].astype(F32)

        exchange(u).wait_recv()
        inward(u).wait_recv()
        part[u] = (own[u] + rcv[u].astype(F32) + a_rcv[u].astype(F32)).astype(BF16)
        across(u).start()

        @pl.when(u == last)
        def _():
            across_far().start()
            across_back().start()

    def inner_final(i):
        u = unit(i)
        across(u).wait_recv()
        y_ref[:, cols(u)] = (part[u].astype(F32) + b_rcv[u].astype(F32)).astype(BF16)

        @pl.when(u < last)
        def _():
            outward(u).start()

        share(u).start()

    def outer_final(i):
        u = unit(i)
        outward(u).wait_recv()
        share(u).start()

    @pl.when(inner)
    def _():
        pl.semaphore_wait(barrier, 5)

    @pl.when(outer)
    def _():
        pl.semaphore_wait(barrier, 4)

    def terms(k):
        term(k)

        @pl.when(jnp.logical_and(outer, k >= OUT_LAG))
        def _():
            outer_sums(k - OUT_LAG)

        @pl.when(jnp.logical_and(inner, k >= IN_START))
        def _():
            inner_sum(k - IN_START)

    loop(0, pairs, terms)

    @pl.when(outer)
    def _():
        loop(pairs - OUT_LAG, pairs, outer_sums)
        loop(0, jnp.where(core == 1, owned - 1, owned), outer_final)

        @pl.when(core == 1)
        def _():
            across_back().wait_recv()
            across(last).wait_recv()
            y_ref[:, cols(last)] = (
                a_rcv[last].astype(F32) + b_rcv[last].astype(F32)
            ).astype(BF16)
            share(last).start()

        def sent(i):
            inward(unit(i)).wait_send()

        loop(0, owned, sent)

    @pl.when(inner)
    def _():
        lag = jnp.where(core == 1, FIN_LAG[1], FIN_LAG[0])
        done = pairs - IN_START
        loop(0, done - lag, inner_final)

        def both(i):
            inner_sum(i)
            inner_final(i - lag)

        loop(done, owned, both)
        loop(owned - lag, owned, inner_final)

        def sent(i):
            u = unit(i)
            across(u).wait_send()

            @pl.when(u < last)
            def _():
                outward(u).wait_send()

            @pl.when(u == last)
            def _():
                across_far().wait_send()
                across_back().wait_send()

        loop(0, owned, sent)

    def finish(u):
        @pl.when(mine(u))
        def _():
            share(u).wait_send()

        @pl.when(jnp.logical_not(mine(u)))
        def _():
            share(u).wait_recv()
            direct = jnp.logical_and(u == 0, outer)

            @pl.when(direct)
            def _():
                head_other().wait_send()

            @pl.when(jnp.logical_not(direct))
            def _():
                exchange(u).wait_send()

    loop(0, units, finish)


def solution(mesh):
    def step(x, w_gate, w_up, w_down):
        rows, depth = x.shape
        width = w_gate.shape[1]
        out = w_down.shape[1]
        units = out // UNIT
        pairs = units // 2
        n_gu = (width // GU_COLS) * GU_PARTS
        kd = depth // GU_PARTS
        dma = pltpu.SemaphoreType.DMA
        return pl.pallas_call(
            kernel,
            out_shape=pltpu.VMEM((rows, out), BF16),
            in_specs=[pl.BlockSpec(memory_space=pl.ANY)] * 4,
            out_specs=pl.BlockSpec(memory_space=pltpu.VMEM),
            scratch_shapes=[
                pltpu.VMEM((rows, depth), BF16),
                pltpu.VMEM((n_gu, kd, GU_COLS), BF16),
                pltpu.VMEM((n_gu, kd, GU_COLS), BF16),
                pltpu.VMEM((pairs, width, 2 * UNIT), BF16),
                pltpu.VMEM((rows, GU_COLS), F32),
                pltpu.VMEM((rows, GU_COLS), F32),
                pltpu.VMEM((rows, width), BF16),
                pltpu.VMEM((units, rows, UNIT), F32),
            ]
            + [pltpu.VMEM((units, rows, UNIT), BF16)] * 5
            + [pltpu.VMEM((rows, UNIT), BF16), dma, dma((n_gu,)), dma((n_gu,)), dma((pairs,))]
            + [dma((units,))] * 10
            + [dma] * 3,
            compiler_params=pltpu.CompilerParams(
                collective_id=0, has_side_effects=True, vmem_limit_bytes=60 * 1024 * 1024
            ),
        )(x, w_gate, w_up, w_down)

    return jax.shard_map(
        step,
        mesh=mesh,
        in_specs=(P("dp", None), P(None, "tp"), P(None, "tp"), P("tp", None)),
        out_specs=P("dp", None),
        check_vma=False,
    )
```

```python
import jax
import jax.numpy as jnp
from jax import lax
from jax.experimental import pallas as pl
from jax.experimental.pallas import tpu as pltpu
from jax.sharding import PartitionSpec as P

MESH = pl.DeviceIdType.MESH
F32, BF16 = jnp.float32, jnp.bfloat16

GU_COLS = 256
GU_PARTS = 4
UNIT = 128
EDGE = 2
OUT_LAG = 5
IN_START = 14
FIN_LAG = (5, 4)


def kernel(
    x_hbm, wg_hbm, wu_hbm, wd_hbm, y_ref,
    x_v, wg_v, wu_v, wd_v, g_acc, u_acc, hid, own, snd, rcv, part, a_rcv, b_rcv, h_rcv,
    x_sem, wg_sem, wu_sem, wd_sem,
    d_ss, d_rs, a_ss, a_rs, b_ss, b_rs, f_ss, f_rs, g_ss, g_rs, h_ss, h_rs, t_ss,
):
    pairs, units = wd_v.shape[0], 2 * wd_v.shape[0]
    last = units - 1
    tp = lax.axis_index("tp")
    core = lax.rem(tp, 2)
    z = lax.div(tp, 2)
    sibling = tp + 1 - 2 * core
    inner = jnp.logical_and(z > 0, z < 3)
    outer = jnp.logical_not(inner)
    low = z < 2
    step = jnp.where(low, 2, -2)
    onward = tp + step
    back = tp - step
    far = tp + 2 * step

    kd = wg_v.shape[1]
    n_j = wg_v.shape[0] // GU_PARTS
    depth = x_v.shape[1]

    def signal(dev):
        pl.semaphore_signal(barrier, inc=1, device_id={"tp": dev}, device_id_type=MESH)

    barrier = pltpu.get_barrier_semaphore()
    signal(sibling)
    signal(onward)
    signal(far)
    signal(jnp.where(inner, back, onward) + 1 - 2 * core)

    @pl.when(inner)
    def _():
        signal(back)

    most = pairs + 2 * EDGE
    owned = jnp.where(core == 1, most, pairs - 2 * EDGE)

    def unit(i):
        edge = jnp.where(i < 2 * EDGE, i, i + units - most)
        middle = jnp.logical_and(i >= 2 * EDGE, i < most - 2 * EDGE)
        return jnp.where(
            core == 1, jnp.where(middle, 2 * (i - EDGE), edge), 2 * (i + EDGE) + 1
        )

    def mine(u):
        middle = jnp.logical_and(u >= 2 * EDGE, u < units - 2 * EDGE)
        zero = jnp.logical_and(middle, lax.rem(u, 2) == 1)
        return jnp.where(zero, 0, 1) == core

    def cols(u):
        return pl.ds(pl.multiple_of(u * UNIT, UNIT), UNIT)

    def gu_copy(hbm, vmem, sem, j, p):
        i = j * GU_PARTS + p
        return pltpu.make_async_copy(
            hbm.at[
                pl.ds(pl.multiple_of(p * kd, kd), kd),
                pl.ds(pl.multiple_of(j * GU_COLS, GU_COLS), GU_COLS),
            ],
            vmem.at[i],
            sem.at[i],
        )

    def wd_copy(k):
        block = pl.ds(pl.multiple_of(k * 2 * UNIT, 2 * UNIT), 2 * UNIT)
        return pltpu.make_async_copy(wd_hbm.at[:, block], wd_v.at[k], wd_sem.at[k])

    def loop(lo, hi, f):
        def it(k, carry):
            f(k)
            return carry

        lax.fori_loop(lo, hi, it, 0)

    x_copy = pltpu.make_async_copy(x_hbm, x_v, x_sem)
    x_copy.start()

    def start_gu(j, c):
        for p in range(GU_PARTS):
            gu_copy(wg_hbm, wg_v, wg_sem, j, p).start()
            gu_copy(wu_hbm, wu_v, wu_sem, j, p).start()
        return c

    lax.fori_loop(0, n_j, start_gu, 0)
    loop(0, pairs, lambda k: wd_copy(k).start())
    x_copy.wait()

    def gate_up(j, carry):
        for p in range(GU_PARTS):
            i = j * GU_PARTS + p
            xs = x_v[:, p * kd : (p + 1) * kd]
            gu_copy(wg_hbm, wg_v, wg_sem, j, p).wait()
            gu_copy(wu_hbm, wu_v, wu_sem, j, p).wait()
            g = jnp.dot(xs, wg_v[i], preferred_element_type=F32)
            u = jnp.dot(xs, wu_v[i], preferred_element_type=F32)
            if p == 0:
                g_acc[...] = g
                u_acc[...] = u
            elif p < GU_PARTS - 1:
                g_acc[...] += g
                u_acc[...] += u
            else:
                g = g_acc[...] + g
                u = u_acc[...] + u
                hid[:, pl.ds(pl.multiple_of(j * GU_COLS, GU_COLS), GU_COLS)] = (
                    jax.nn.silu(g) * u
                ).astype(BF16)
        return carry

    lax.fori_loop(0, n_j, gate_up, 0)

    def remote(src, dst, send, recv, dev):
        return pltpu.make_async_remote_copy(
            src_ref=src, dst_ref=dst, send_sem=send, recv_sem=recv,
            device_id={"tp": dev}, device_id_type=MESH,
        )

    def exchange(u):
        return remote(snd.at[u], rcv.at[u], d_ss.at[u], d_rs.at[u], sibling)

    def inward(u):
        return remote(part.at[u], a_rcv.at[u], a_ss.at[u], a_rs.at[u], onward)

    def head_own():
        return remote(snd.at[0], a_rcv.at[0], a_ss.at[0], a_rs.at[0], onward)

    def head_other():
        return remote(snd.at[0], h_rcv, h_ss, h_rs, onward + 1 - 2 * core)

    def across(u):
        return remote(part.at[u], b_rcv.at[u], b_ss.at[u], b_rs.at[u], onward)

    def across_far():
        return remote(part.at[last], b_rcv.at[last], t_ss, b_rs.at[last], far)

    def across_back():
        return remote(part.at[last], a_rcv.at[last], a_ss.at[last], a_rs.at[last], back)

    def outward(u):
        return remote(y_ref.at[:, cols(u)], y_ref.at[:, cols(u)], f_ss.at[u], f_rs.at[u], back)

    def share(u):
        return remote(y_ref.at[:, cols(u)], y_ref.at[:, cols(u)], g_ss.at[u], g_rs.at[u], sibling)

    def term(k):
        wd_copy(k).wait()
        t = jnp.dot(hid[...], wd_v[k], preferred_element_type=F32)
        for i in range(2):
            ti = t[:, i * UNIT : (i + 1) * UNIT]
            own[2 * k + i] = ti
            snd[2 * k + i] = ti.astype(BF16)
        for i in range(2):
            u = 2 * k + i
            direct = jnp.logical_and(u == 0, outer)

            @pl.when(jnp.logical_and(jnp.logical_not(mine(u)), jnp.logical_not(direct)))
            def _():
                exchange(u).start()

        @pl.when(jnp.logical_and(k == 0, outer))
        def _():
            @pl.when(core == 1)
            def _():
                head_own().start()

            @pl.when(core == 0)
            def _():
                head_other().start()

    def outer_sum(u):
        exchange(u).wait_recv()
        part[u] = (own[u] + rcv[u].astype(F32)).astype(BF16)
        inward(u).start()

    def outer_sums(k):
        for i in range(2):
            u = 2 * k + i

            @pl.when(jnp.logical_and(mine(u), u > 0))
            def _():
                outer_sum(u)

    def inner_sum(i):
        u = unit(i)

        @pl.when(u == 0)
        def _():
            head_other().wait_recv()
            own[0] = own[0] + h_rcv[...].astype(F32)

        exchange(u).wait_recv()
        inward(u).wait_recv()
        part[u] = (own[u] + rcv[u].astype(F32) + a_rcv[u].astype(F32)).astype(BF16)
        across(u).start()

        @pl.when(u == last)
        def _():
            across_far().start()
            across_back().start()

    def inner_final(i):
        u = unit(i)
        across(u).wait_recv()
        y_ref[:, cols(u)] = (part[u].astype(F32) + b_rcv[u].astype(F32)).astype(BF16)

        @pl.when(u < last)
        def _():
            outward(u).start()

        share(u).start()

    def outer_final(i):
        u = unit(i)
        outward(u).wait_recv()
        share(u).start()

    @pl.when(inner)
    def _():
        pl.semaphore_wait(barrier, 5)

    @pl.when(outer)
    def _():
        pl.semaphore_wait(barrier, 4)

    def terms(k):
        term(k)

        @pl.when(jnp.logical_and(outer, k >= OUT_LAG))
        def _():
            outer_sums(k - OUT_LAG)

        @pl.when(jnp.logical_and(inner, k >= IN_START))
        def _():
            inner_sum(k - IN_START)

    loop(0, pairs, terms)

    @pl.when(outer)
    def _():
        loop(pairs - OUT_LAG, pairs, outer_sums)
        loop(0, jnp.where(core == 1, owned - 1, owned), outer_final)

        @pl.when(core == 1)
        def _():
            across_back().wait_recv()
            across(last).wait_recv()
            y_ref[:, cols(last)] = (
                a_rcv[last].astype(F32) + b_rcv[last].astype(F32)
            ).astype(BF16)
            share(last).start()

        def sent(i):
            inward(unit(i)).wait_send()

        loop(0, owned, sent)

    @pl.when(inner)
    def _():
        lag = jnp.where(core == 1, FIN_LAG[1], FIN_LAG[0])
        done = pairs - IN_START
        loop(0, done - lag, inner_final)

        def both(i):
            inner_sum(i)
            inner_final(i - lag)

        loop(done, owned, both)
        loop(owned - lag, owned, inner_final)

        def sent(i):
            u = unit(i)
            across(u).wait_send()

            @pl.when(u < last)
            def _():
                outward(u).wait_send()

            @pl.when(u == last)
            def _():
                across_far().wait_send()
                across_back().wait_send()

        loop(0, owned, sent)

    def finish(u):
        @pl.when(mine(u))
        def _():
            share(u).wait_send()

        @pl.when(jnp.logical_not(mine(u)))
        def _():
            share(u).wait_recv()
            direct = jnp.logical_and(u == 0, outer)

            @pl.when(direct)
            def _():
                head_other().wait_send()

            @pl.when(jnp.logical_not(direct))
            def _():
                exchange(u).wait_send()

    loop(0, units, finish)


def solution(mesh):
    def step(x, w_gate, w_up, w_down):
        rows, depth = x.shape
        width = w_gate.shape[1]
        out = w_down.shape[1]
        units = out // UNIT
        pairs = units // 2
        n_gu = (width // GU_COLS) * GU_PARTS
        kd = depth // GU_PARTS
        dma = pltpu.SemaphoreType.DMA
        return pl.pallas_call(
            kernel,
            out_shape=pltpu.VMEM((rows, out), BF16),
            in_specs=[pl.BlockSpec(memory_space=pl.ANY)] * 4,
            out_specs=pl.BlockSpec(memory_space=pltpu.VMEM),
            scratch_shapes=[
                pltpu.VMEM((rows, depth), BF16),
                pltpu.VMEM((n_gu, kd, GU_COLS), BF16),
                pltpu.VMEM((n_gu, kd, GU_COLS), BF16),
                pltpu.VMEM((pairs, width, 2 * UNIT), BF16),
                pltpu.VMEM((rows, GU_COLS), F32),
                pltpu.VMEM((rows, GU_COLS), F32),
                pltpu.VMEM((rows, width), BF16),
                pltpu.VMEM((units, rows, UNIT), F32),
            ]
            + [pltpu.VMEM((units, rows, UNIT), BF16)] * 5
            + [pltpu.VMEM((rows, UNIT), BF16), dma, dma((n_gu,)), dma((n_gu,)), dma((pairs,))]
            + [dma((units,))] * 10
            + [dma] * 3,
            compiler_params=pltpu.CompilerParams(
                collective_id=0, has_side_effects=True, vmem_limit_bytes=60 * 1024 * 1024
            ),
        )(x, w_gate, w_up, w_down)

    return jax.shard_map(
        step,
        mesh=mesh,
        in_specs=(P("dp", None), P(None, "tp"), P(None, "tp"), P("tp", None)),
        out_specs=P("dp", None),
        check_vma=False,
    )
```

```python
import jax
import jax.numpy as jnp
from jax import lax
from jax.experimental import pallas as pl
from jax.experimental.pallas import tpu as pltpu
from jax.sharding import PartitionSpec as P

MESH = pl.DeviceIdType.MESH
F32, BF16 = jnp.float32, jnp.bfloat16

GU_COLS = 256
GU_PARTS = 4
UNIT = 128
EDGE = 2
OUT_LAG = 5
IN_START = 14
TAKE_LAG = 3
FIN_LAG = (5, 4)


def kernel(
    x_hbm, wg_hbm, wu_hbm, wd_hbm, y_ref,
    x_v, wg_v, wu_v, wd_v, g_acc, u_acc, hid, own, snd, rcv, part, a_rcv, b_rcv, fin, h_rcv,
    x_sem, wg_sem, wu_sem, wd_sem,
    d_ss, d_rs, a_ss, a_rs, b_ss, b_rs, f_ss, f_rs, g_ss, g_rs, h_ss, h_rs, t_ss,
):
    pairs, units = wd_v.shape[0], 2 * wd_v.shape[0]
    last = units - 1
    tp = lax.axis_index("tp")
    core = lax.rem(tp, 2)
    z = lax.div(tp, 2)
    sibling = tp + 1 - 2 * core
    inner = jnp.logical_and(z > 0, z < 3)
    outer = jnp.logical_not(inner)
    low = z < 2
    step = jnp.where(low, 2, -2)
    onward = tp + step
    back = tp - step
    far = tp + 2 * step

    kd = wg_v.shape[1]
    n_j = wg_v.shape[0] // GU_PARTS
    depth = x_v.shape[1]

    def signal(dev):
        pl.semaphore_signal(barrier, inc=1, device_id={"tp": dev}, device_id_type=MESH)

    barrier = pltpu.get_barrier_semaphore()
    signal(sibling)
    signal(onward)
    signal(far)
    signal(jnp.where(inner, back, onward) + 1 - 2 * core)

    @pl.when(inner)
    def _():
        signal(back)

    most = pairs + 2 * EDGE
    owned = jnp.where(core == 1, most, pairs - 2 * EDGE)

    def unit(i, core=core):
        edge = jnp.where(i < 2 * EDGE, i, i + units - most)
        middle = jnp.logical_and(i >= 2 * EDGE, i < most - 2 * EDGE)
        return jnp.where(
            core == 1, jnp.where(middle, 2 * (i - EDGE), edge), 2 * (i + EDGE) + 1
        )

    def mine(u):
        middle = jnp.logical_and(u >= 2 * EDGE, u < units - 2 * EDGE)
        zero = jnp.logical_and(middle, lax.rem(u, 2) == 1)
        return jnp.where(zero, 0, 1) == core

    def cols(u):
        return pl.ds(pl.multiple_of(u * UNIT, UNIT), UNIT)

    def gu_copy(hbm, vmem, sem, j, p):
        i = j * GU_PARTS + p
        return pltpu.make_async_copy(
            hbm.at[
                pl.ds(pl.multiple_of(p * kd, kd), kd),
                pl.ds(pl.multiple_of(j * GU_COLS, GU_COLS), GU_COLS),
            ],
            vmem.at[i],
            sem.at[i],
        )

    def wd_copy(k):
        block = pl.ds(pl.multiple_of(k * 2 * UNIT, 2 * UNIT), 2 * UNIT)
        return pltpu.make_async_copy(wd_hbm.at[:, block], wd_v.at[k], wd_sem.at[k])

    def loop(lo, hi, f):
        def it(k, carry):
            f(k)
            return carry

        lax.fori_loop(lo, hi, it, 0)

    x_copy = pltpu.make_async_copy(x_hbm, x_v, x_sem)
    x_copy.start()

    def start_gu(j, c):
        for p in range(GU_PARTS):
            gu_copy(wg_hbm, wg_v, wg_sem, j, p).start()
            gu_copy(wu_hbm, wu_v, wu_sem, j, p).start()
        return c

    lax.fori_loop(0, n_j, start_gu, 0)
    loop(0, pairs, lambda k: wd_copy(k).start())
    x_copy.wait()

    def gate_up(j, carry):
        for p in range(GU_PARTS):
            i = j * GU_PARTS + p
            xs = x_v[:, p * kd : (p + 1) * kd]
            gu_copy(wg_hbm, wg_v, wg_sem, j, p).wait()
            gu_copy(wu_hbm, wu_v, wu_sem, j, p).wait()
            g = jnp.dot(xs, wg_v[i], preferred_element_type=F32)
            u = jnp.dot(xs, wu_v[i], preferred_element_type=F32)
            if p == 0:
                g_acc[...] = g
                u_acc[...] = u
            elif p < GU_PARTS - 1:
                g_acc[...] += g
                u_acc[...] += u
            else:
                g = g_acc[...] + g
                u = u_acc[...] + u
                hid[:, pl.ds(pl.multiple_of(j * GU_COLS, GU_COLS), GU_COLS)] = (
                    jax.nn.silu(g) * u
                ).astype(BF16)
        return carry

    lax.fori_loop(0, n_j, gate_up, 0)

    def remote(src, dst, send, recv, dev):
        return pltpu.make_async_remote_copy(
            src_ref=src, dst_ref=dst, send_sem=send, recv_sem=recv,
            device_id={"tp": dev}, device_id_type=MESH,
        )

    def exchange(u):
        return remote(snd.at[u], rcv.at[u], d_ss.at[u], d_rs.at[u], sibling)

    def inward(u):
        return remote(part.at[u], a_rcv.at[u], a_ss.at[u], a_rs.at[u], onward)

    def head_own():
        return remote(snd.at[0], a_rcv.at[0], a_ss.at[0], a_rs.at[0], onward)

    def head_other():
        return remote(snd.at[0], h_rcv, h_ss, h_rs, onward + 1 - 2 * core)

    def across(u):
        return remote(part.at[u], b_rcv.at[u], b_ss.at[u], b_rs.at[u], onward)

    def across_far():
        return remote(part.at[last], b_rcv.at[last], t_ss, b_rs.at[last], far)

    def across_back():
        return remote(part.at[last], a_rcv.at[last], a_ss.at[last], a_rs.at[last], back)

    def outward(u):
        return remote(fin.at[u], fin.at[u], f_ss.at[u], f_rs.at[u], back)

    def share(u):
        return remote(fin.at[u], fin.at[u], g_ss.at[u], g_rs.at[u], sibling)

    def term(k):
        wd_copy(k).wait()
        t = jnp.dot(hid[...], wd_v[k], preferred_element_type=F32)
        for i in range(2):
            ti = t[:, i * UNIT : (i + 1) * UNIT]
            own[2 * k + i] = ti
            snd[2 * k + i] = ti.astype(BF16)
        for i in range(2):
            u = 2 * k + i
            direct = jnp.logical_and(u == 0, outer)

            @pl.when(jnp.logical_and(jnp.logical_not(mine(u)), jnp.logical_not(direct)))
            def _():
                exchange(u).start()

        @pl.when(jnp.logical_and(k == 0, outer))
        def _():
            @pl.when(core == 1)
            def _():
                head_own().start()

            @pl.when(core == 0)
            def _():
                head_other().start()

    def outer_sum(u):
        exchange(u).wait_recv()
        part[u] = (own[u] + rcv[u].astype(F32)).astype(BF16)
        inward(u).start()

    def outer_sums(k):
        for i in range(2):
            u = 2 * k + i

            @pl.when(jnp.logical_and(mine(u), u > 0))
            def _():
                outer_sum(u)

    def inner_sum(i):
        u = unit(i)

        @pl.when(u == 0)
        def _():
            head_other().wait_recv()
            own[0] = own[0] + h_rcv[...].astype(F32)

        exchange(u).wait_recv()
        inward(u).wait_recv()
        part[u] = (own[u] + rcv[u].astype(F32) + a_rcv[u].astype(F32)).astype(BF16)
        across(u).start()

        @pl.when(u == last)
        def _():
            across_far().start()
            across_back().start()

    def inner_final(i):
        u = unit(i)
        across(u).wait_recv()
        fin[u] = (part[u].astype(F32) + b_rcv[u].astype(F32)).astype(BF16)

        @pl.when(u < last)
        def _():
            outward(u).start()

        share(u).start()
        y_ref[:, cols(u)] = fin[u]

    def outer_final(i):
        u = unit(i)
        outward(u).wait_recv()
        share(u).start()
        y_ref[:, cols(u)] = fin[u]

    others = units - owned

    def take(i):
        @pl.when(jnp.logical_and(i >= 0, i < others))
        def _():
            u = unit(i, 1 - core)
            share(u).wait_recv()
            y_ref[:, cols(u)] = fin[u]

    @pl.when(inner)
    def _():
        pl.semaphore_wait(barrier, 5)

    @pl.when(outer)
    def _():
        pl.semaphore_wait(barrier, 4)

    def terms(k):
        term(k)

        @pl.when(jnp.logical_and(outer, k >= OUT_LAG))
        def _():
            outer_sums(k - OUT_LAG)

        @pl.when(jnp.logical_and(inner, k >= IN_START))
        def _():
            inner_sum(k - IN_START)

    loop(0, pairs, terms)

    @pl.when(outer)
    def _():
        loop(pairs - OUT_LAG, pairs, outer_sums)
        mids = jnp.where(core == 1, owned - 1, owned)

        def ending(i):
            outer_final(i)
            take(i - TAKE_LAG)

        loop(0, mids, ending)

        @pl.when(core == 1)
        def _():
            across_back().wait_recv()
            across(last).wait_recv()
            fin[last] = (a_rcv[last].astype(F32) + b_rcv[last].astype(F32)).astype(BF16)
            share(last).start()
            y_ref[:, cols(last)] = fin[last]

        loop(mids - TAKE_LAG, others, take)

        def sent(i):
            inward(unit(i)).wait_send()

        loop(0, owned, sent)

    @pl.when(inner)
    def _():
        lag = jnp.where(core == 1, FIN_LAG[1], FIN_LAG[0])
        done = pairs - IN_START
        loop(0, done - lag, inner_final)
        loop(0, done - lag - TAKE_LAG, take)

        def both(i):
            inner_sum(i)
            inner_final(i - lag)
            take(i - lag - TAKE_LAG)

        def ending(i):
            inner_final(i)
            take(i - TAKE_LAG)

        loop(done, owned, both)
        loop(owned - lag, owned, ending)
        loop(owned - TAKE_LAG, others, take)

        def sent(i):
            u = unit(i)
            across(u).wait_send()

            @pl.when(u < last)
            def _():
                outward(u).wait_send()

            @pl.when(u == last)
            def _():
                across_far().wait_send()
                across_back().wait_send()

        loop(0, owned, sent)

    def finish(u):
        @pl.when(mine(u))
        def _():
            share(u).wait_send()

        @pl.when(jnp.logical_not(mine(u)))
        def _():
            direct = jnp.logical_and(u == 0, outer)

            @pl.when(direct)
            def _():
                head_other().wait_send()

            @pl.when(jnp.logical_not(direct))
            def _():
                exchange(u).wait_send()

    loop(0, units, finish)


def solution(mesh):
    def step(x, w_gate, w_up, w_down):
        rows, depth = x.shape
        width = w_gate.shape[1]
        out = w_down.shape[1]
        units = out // UNIT
        pairs = units // 2
        n_gu = (width // GU_COLS) * GU_PARTS
        kd = depth // GU_PARTS
        dma = pltpu.SemaphoreType.DMA
        return pl.pallas_call(
            kernel,
            out_shape=pltpu.VMEM((rows, out), BF16),
            in_specs=[pl.BlockSpec(memory_space=pl.ANY)] * 4,
            out_specs=pl.BlockSpec(memory_space=pltpu.VMEM),
            scratch_shapes=[
                pltpu.VMEM((rows, depth), BF16),
                pltpu.VMEM((n_gu, kd, GU_COLS), BF16),
                pltpu.VMEM((n_gu, kd, GU_COLS), BF16),
                pltpu.VMEM((pairs, width, 2 * UNIT), BF16),
                pltpu.VMEM((rows, GU_COLS), F32),
                pltpu.VMEM((rows, GU_COLS), F32),
                pltpu.VMEM((rows, width), BF16),
                pltpu.VMEM((units, rows, UNIT), F32),
            ]
            + [pltpu.VMEM((units, rows, UNIT), BF16)] * 6
            + [pltpu.VMEM((rows, UNIT), BF16), dma, dma((n_gu,)), dma((n_gu,)), dma((pairs,))]
            + [dma((units,))] * 10
            + [dma] * 3,
            compiler_params=pltpu.CompilerParams(
                collective_id=0, has_side_effects=True, vmem_limit_bytes=60 * 1024 * 1024
            ),
        )(x, w_gate, w_up, w_down)

    return jax.shard_map(
        step,
        mesh=mesh,
        in_specs=(P("dp", None), P(None, "tp"), P(None, "tp"), P("tp", None)),
        out_specs=P("dp", None),
        check_vma=False,
    )
```

```python
import functools

import jax
import jax.numpy as jnp
from jax import lax
from jax.experimental import pallas as pl
from jax.experimental.pallas import tpu as pltpu
from jax.sharding import PartitionSpec as P

MESH = pl.DeviceIdType.MESH
F32, BF16 = jnp.float32, jnp.bfloat16

GU_COLS = 256
GU_PARTS = 4
Y_COLS = 128
D2D_LAG = 8
IN_START = 28
FIN_LAG = 8


def kernel(
    x_hbm, wg_hbm, wu_hbm, wd_hbm, y_ref,
    x_v, wg_v, wu_v, wd_v, g_acc, u_acc, hid, own, snd, rcv, part, a_rcv, b_rcv,
    x_sem, wg_sem, wu_sem, wd_sem,
    d_ss, d_rs, p_ss, p_rs, f_ss, f_rs, g_ss, g_rs,
):
    tp = lax.axis_index("tp")
    core = lax.rem(tp, 2)
    z = lax.div(tp, 2)
    sibling = tp + 1 - 2 * core
    inner = jnp.logical_and(z > 0, z < 3)
    outer = jnp.logical_not(inner)
    low = z < 2
    onward = jnp.where(low, tp + 2, tp - 2)
    back = jnp.where(low, tp - 2, tp + 2)

    rows, half = x_v.shape[0], x_v.shape[0] // 2
    kd = wg_v.shape[1]
    n_j = wg_v.shape[0] // GU_PARTS
    n_k = wd_v.shape[0]
    mine = pl.ds(pl.multiple_of(core * half, half), half)
    theirs = pl.ds(pl.multiple_of((1 - core) * half, half), half)

    barrier = pltpu.get_barrier_semaphore()
    pl.semaphore_signal(barrier, inc=1, device_id={"tp": sibling}, device_id_type=MESH)
    pl.semaphore_signal(barrier, inc=1, device_id={"tp": onward}, device_id_type=MESH)

    @pl.when(inner)
    def _():
        pl.semaphore_signal(barrier, inc=1, device_id={"tp": back}, device_id_type=MESH)

    def ycols(k):
        return pl.ds(pl.multiple_of(k * Y_COLS, Y_COLS), Y_COLS)

    def x_copy(part_rows, i):
        return pltpu.make_async_copy(
            x_hbm.at[part_rows, :], x_v.at[pl.ds(i * half, half), :], x_sem.at[i]
        )

    def gu_copy(hbm, vmem, sem, j, p):
        i = j * GU_PARTS + p
        return pltpu.make_async_copy(
            hbm.at[
                pl.ds(pl.multiple_of(p * kd, kd), kd),
                pl.ds(pl.multiple_of(j * GU_COLS, GU_COLS), GU_COLS),
            ],
            vmem.at[i],
            sem.at[i],
        )

    def wd_copy(k):
        return pltpu.make_async_copy(wd_hbm.at[:, ycols(k)], wd_v.at[k], wd_sem.at[k])

    x_copy(mine, 0).start()
    x_copy(theirs, 1).start()

    def start_gu(j, c):
        for p in range(GU_PARTS):
            gu_copy(wg_hbm, wg_v, wg_sem, j, p).start()
            gu_copy(wu_hbm, wu_v, wu_sem, j, p).start()
        return c

    lax.fori_loop(0, n_j, start_gu, 0)

    def start_wd(k, c):
        wd_copy(k).start()
        return c

    lax.fori_loop(0, n_k, start_wd, 0)

    x_copy(mine, 0).wait()
    x_copy(theirs, 1).wait()

    def gate_up(j, c):
        for p in range(GU_PARTS):
            i = j * GU_PARTS + p
            xs = x_v[:, p * kd : (p + 1) * kd]
            gu_copy(wg_hbm, wg_v, wg_sem, j, p).wait()
            gu_copy(wu_hbm, wu_v, wu_sem, j, p).wait()
            g = jnp.dot(xs, wg_v[i], preferred_element_type=F32)
            u = jnp.dot(xs, wu_v[i], preferred_element_type=F32)
            if p == 0:
                g_acc[...] = g
                u_acc[...] = u
            elif p < GU_PARTS - 1:
                g_acc[...] += g
                u_acc[...] += u
            else:
                g = g_acc[...] + g
                u = u_acc[...] + u
                hid[:, pl.ds(pl.multiple_of(j * GU_COLS, GU_COLS), GU_COLS)] = (
                    jax.nn.silu(g) * u
                ).astype(BF16)
        return c

    lax.fori_loop(0, n_j, gate_up, 0)

    def d2d(k):
        return pltpu.make_async_remote_copy(
            src_ref=snd.at[k], dst_ref=rcv.at[k], send_sem=d_ss.at[k], recv_sem=d_rs.at[k],
            device_id={"tp": sibling}, device_id_type=MESH,
        )

    def to_inner(k):
        return pltpu.make_async_remote_copy(
            src_ref=part.at[k], dst_ref=a_rcv.at[k], send_sem=p_ss.at[k], recv_sem=p_rs.at[0, k],
            device_id={"tp": onward}, device_id_type=MESH,
        )

    def across(k):
        return pltpu.make_async_remote_copy(
            src_ref=part.at[k], dst_ref=b_rcv.at[k], send_sem=p_ss.at[k], recv_sem=p_rs.at[1, k],
            device_id={"tp": onward}, device_id_type=MESH,
        )

    def to_outer(k):
        return pltpu.make_async_remote_copy(
            src_ref=y_ref.at[mine, ycols(k)], dst_ref=y_ref.at[mine, ycols(k)],
            send_sem=f_ss.at[k], recv_sem=f_rs.at[k],
            device_id={"tp": back}, device_id_type=MESH,
        )

    def share(k):
        return pltpu.make_async_remote_copy(
            src_ref=y_ref.at[mine, ycols(k)], dst_ref=y_ref.at[mine, ycols(k)],
            send_sem=g_ss.at[k], recv_sem=g_rs.at[k],
            device_id={"tp": sibling}, device_id_type=MESH,
        )

    def share_arrival(k):
        return pltpu.make_async_remote_copy(
            src_ref=y_ref.at[theirs, ycols(k)], dst_ref=y_ref.at[theirs, ycols(k)],
            send_sem=g_ss.at[k], recv_sem=g_rs.at[k],
            device_id={"tp": sibling}, device_id_type=MESH,
        )

    def term(k):
        wd_copy(k).wait()
        t = jnp.dot(hid[...], wd_v[k], preferred_element_type=F32)
        own[k] = t[:half]
        snd[k] = t[half:].astype(BF16)
        d2d(k).start()

    def outer_sum(k):
        d2d(k).wait_recv()
        part[k] = (own[k] + rcv[k].astype(F32)).astype(BF16)
        to_inner(k).start()

    def inner_sum(k):
        d2d(k).wait_recv()
        to_inner(k).wait_recv()
        part[k] = (own[k] + rcv[k].astype(F32) + a_rcv[k].astype(F32)).astype(BF16)
        across(k).start()

    def inner_final(k):
        across(k).wait_recv()
        y_ref[mine, ycols(k)] = (part[k].astype(F32) + b_rcv[k].astype(F32)).astype(BF16)
        to_outer(k).start()
        share(k).start()

    def outer_final(k):
        to_outer(k).wait_recv()
        share(k).start()

    @pl.when(inner)
    def _():
        pl.semaphore_wait(barrier, 3)

    @pl.when(outer)
    def _():
        pl.semaphore_wait(barrier, 2)

    def terms(k, c):
        term(k)

        @pl.when(jnp.logical_and(outer, k >= D2D_LAG))
        def _():
            outer_sum(k - D2D_LAG)

        @pl.when(jnp.logical_and(inner, k >= IN_START))
        def _():
            inner_sum(k - IN_START)

        return c

    lax.fori_loop(0, n_k, terms, 0)

    def loop(lo, hi, f):
        def it(k, c):
            f(k)
            return c

        lax.fori_loop(lo, hi, it, 0)

    @pl.when(outer)
    def _():
        loop(n_k - D2D_LAG, n_k, outer_sum)
        loop(0, n_k, outer_final)
        loop(0, n_k, lambda k: to_inner(k).wait_send())

    @pl.when(inner)
    def _():
        first = n_k - IN_START
        loop(0, first - FIN_LAG, inner_final)

        def both(k):
            inner_sum(k)
            inner_final(k - FIN_LAG)

        loop(max(first, FIN_LAG), n_k, both)
        loop(n_k - FIN_LAG, n_k, inner_final)

        def sent(k):
            across(k).wait_send()
            to_outer(k).wait_send()

        loop(0, n_k, sent)

    def finish(k):
        d2d(k).wait_send()
        share(k).wait_send()
        share_arrival(k).wait_recv()

    loop(0, n_k, finish)


def solution(mesh):
    def step(x, w_gate, w_up, w_down):
        rows, depth = x.shape
        width = w_gate.shape[1]
        out = w_down.shape[1]
        half = rows // 2
        n_gu = (width // GU_COLS) * GU_PARTS
        n_k = out // Y_COLS
        kd = depth // GU_PARTS
        dma = pltpu.SemaphoreType.DMA
        return pl.pallas_call(
            kernel,
            out_shape=pltpu.VMEM((rows, out), BF16),
            in_specs=[pl.BlockSpec(memory_space=pl.ANY)] * 4,
            out_specs=pl.BlockSpec(memory_space=pltpu.VMEM),
            scratch_shapes=[
                pltpu.VMEM((rows, depth), BF16),
                pltpu.VMEM((n_gu, kd, GU_COLS), BF16),
                pltpu.VMEM((n_gu, kd, GU_COLS), BF16),
                pltpu.VMEM((n_k, width, Y_COLS), BF16),
                pltpu.VMEM((rows, GU_COLS), F32),
                pltpu.VMEM((rows, GU_COLS), F32),
                pltpu.VMEM((rows, width), BF16),
                pltpu.VMEM((n_k, half, Y_COLS), F32),
                pltpu.VMEM((n_k, half, Y_COLS), BF16),
                pltpu.VMEM((n_k, half, Y_COLS), BF16),
                pltpu.VMEM((n_k, half, Y_COLS), BF16),
                pltpu.VMEM((n_k, half, Y_COLS), BF16),
                pltpu.VMEM((n_k, half, Y_COLS), BF16),
                dma((2,)),
                dma((n_gu,)),
                dma((n_gu,)),
                dma((n_k,)),
                dma((n_k,)),
                dma((n_k,)),
                dma((n_k,)),
                dma((2, n_k)),
                dma((n_k,)),
                dma((n_k,)),
                dma((n_k,)),
                dma((n_k,)),
            ],
            compiler_params=pltpu.CompilerParams(
                collective_id=0, has_side_effects=True, vmem_limit_bytes=58 * 1024 * 1024
            ),
        )(x, w_gate, w_up, w_down)

    return jax.shard_map(
        step,
        mesh=mesh,
        in_specs=(P("dp", None), P(None, "tp"), P(None, "tp"), P("tp", None)),
        out_specs=P("dp", None),
        check_vma=False,
    )
```

```python
import functools

import jax
import jax.numpy as jnp
from jax import lax
from jax.experimental import pallas as pl
from jax.experimental.pallas import tpu as pltpu
from jax.sharding import PartitionSpec as P

MESH = pl.DeviceIdType.MESH
F32, BF16 = jnp.float32, jnp.bfloat16

GU_COLS = 256
GU_PARTS = 4
Y_COLS = 256
D2D_LAG = 2
IN_START = 8
FIN_LAG = 5


def kernel(
    x_hbm, wg_hbm, wu_hbm, wd_hbm, y_ref,
    x_v, wg_v, wu_v, wd_v, g_acc, u_acc, hid, own, snd, rcv, part, a_rcv, b_rcv,
    x_sem, wg_sem, wu_sem, wd_sem,
    d_ss, d_rs, p_ss, p_rs, f_ss, f_rs, g_ss, g_rs,
):
    tp = lax.axis_index("tp")
    core = lax.rem(tp, 2)
    z = lax.div(tp, 2)
    sibling = tp + 1 - 2 * core
    inner = jnp.logical_and(z > 0, z < 3)
    outer = jnp.logical_not(inner)
    low = z < 2
    onward = jnp.where(low, tp + 2, tp - 2)
    back = jnp.where(low, tp - 2, tp + 2)

    rows, half = x_v.shape[0], x_v.shape[0] // 2
    kd = wg_v.shape[1]
    n_j = wg_v.shape[0] // GU_PARTS
    n_k = wd_v.shape[0]
    mine = pl.ds(pl.multiple_of(core * half, half), half)
    theirs = pl.ds(pl.multiple_of((1 - core) * half, half), half)

    barrier = pltpu.get_barrier_semaphore()
    pl.semaphore_signal(barrier, inc=1, device_id={"tp": sibling}, device_id_type=MESH)
    pl.semaphore_signal(barrier, inc=1, device_id={"tp": onward}, device_id_type=MESH)

    @pl.when(inner)
    def _():
        pl.semaphore_signal(barrier, inc=1, device_id={"tp": back}, device_id_type=MESH)

    def ycols(k):
        return pl.ds(pl.multiple_of(k * Y_COLS, Y_COLS), Y_COLS)

    def x_copy(part_rows, i):
        return pltpu.make_async_copy(
            x_hbm.at[part_rows, :], x_v.at[pl.ds(i * half, half), :], x_sem.at[i]
        )

    def gu_copy(hbm, vmem, sem, j, p):
        i = j * GU_PARTS + p
        return pltpu.make_async_copy(
            hbm.at[
                pl.ds(pl.multiple_of(p * kd, kd), kd),
                pl.ds(pl.multiple_of(j * GU_COLS, GU_COLS), GU_COLS),
            ],
            vmem.at[i],
            sem.at[i],
        )

    def wd_copy(k):
        return pltpu.make_async_copy(wd_hbm.at[:, ycols(k)], wd_v.at[k], wd_sem.at[k])

    x_copy(mine, 0).start()
    x_copy(theirs, 1).start()

    def start_gu(j, c):
        for p in range(GU_PARTS):
            gu_copy(wg_hbm, wg_v, wg_sem, j, p).start()
            gu_copy(wu_hbm, wu_v, wu_sem, j, p).start()
        return c

    lax.fori_loop(0, n_j, start_gu, 0)

    def start_wd(k, c):
        wd_copy(k).start()
        return c

    lax.fori_loop(0, n_k, start_wd, 0)

    x_copy(mine, 0).wait()
    x_copy(theirs, 1).wait()

    def gate_up(j, c):
        for p in range(GU_PARTS):
            i = j * GU_PARTS + p
            xs = x_v[:, p * kd : (p + 1) * kd]
            gu_copy(wg_hbm, wg_v, wg_sem, j, p).wait()
            gu_copy(wu_hbm, wu_v, wu_sem, j, p).wait()
            g = jnp.dot(xs, wg_v[i], preferred_element_type=F32)
            u = jnp.dot(xs, wu_v[i], preferred_element_type=F32)
            if p == 0:
                g_acc[...] = g
                u_acc[...] = u
            elif p < GU_PARTS - 1:
                g_acc[...] += g
                u_acc[...] += u
            else:
                g = g_acc[...] + g
                u = u_acc[...] + u
                hid[:, pl.ds(pl.multiple_of(j * GU_COLS, GU_COLS), GU_COLS)] = (
                    jax.nn.silu(g) * u
                ).astype(BF16)
        return c

    lax.fori_loop(0, n_j, gate_up, 0)

    def d2d(k):
        return pltpu.make_async_remote_copy(
            src_ref=snd.at[k], dst_ref=rcv.at[k], send_sem=d_ss.at[k], recv_sem=d_rs.at[k],
            device_id={"tp": sibling}, device_id_type=MESH,
        )

    def to_inner(k):
        return pltpu.make_async_remote_copy(
            src_ref=part.at[k], dst_ref=a_rcv.at[k], send_sem=p_ss.at[k], recv_sem=p_rs.at[0, k],
            device_id={"tp": onward}, device_id_type=MESH,
        )

    def across(k):
        return pltpu.make_async_remote_copy(
            src_ref=part.at[k], dst_ref=b_rcv.at[k], send_sem=p_ss.at[k], recv_sem=p_rs.at[1, k],
            device_id={"tp": onward}, device_id_type=MESH,
        )

    def to_outer(k):
        return pltpu.make_async_remote_copy(
            src_ref=y_ref.at[mine, ycols(k)], dst_ref=y_ref.at[mine, ycols(k)],
            send_sem=f_ss.at[k], recv_sem=f_rs.at[k],
            device_id={"tp": back}, device_id_type=MESH,
        )

    def share(k):
        return pltpu.make_async_remote_copy(
            src_ref=y_ref.at[mine, ycols(k)], dst_ref=y_ref.at[mine, ycols(k)],
            send_sem=g_ss.at[k], recv_sem=g_rs.at[k],
            device_id={"tp": sibling}, device_id_type=MESH,
        )

    def share_arrival(k):
        return pltpu.make_async_remote_copy(
            src_ref=y_ref.at[theirs, ycols(k)], dst_ref=y_ref.at[theirs, ycols(k)],
            send_sem=g_ss.at[k], recv_sem=g_rs.at[k],
            device_id={"tp": sibling}, device_id_type=MESH,
        )

    def term(k):
        wd_copy(k).wait()
        t = jnp.dot(hid[...], wd_v[k], preferred_element_type=F32)
        own[k] = t[:half]
        snd[k] = t[half:].astype(BF16)
        d2d(k).start()

    def outer_sum(k):
        d2d(k).wait_recv()
        part[k] = (own[k] + rcv[k].astype(F32)).astype(BF16)
        to_inner(k).start()

    def inner_sum(k):
        d2d(k).wait_recv()
        to_inner(k).wait_recv()
        part[k] = (own[k] + rcv[k].astype(F32) + a_rcv[k].astype(F32)).astype(BF16)
        across(k).start()

    def inner_final(k):
        across(k).wait_recv()
        y_ref[mine, ycols(k)] = (part[k].astype(F32) + b_rcv[k].astype(F32)).astype(BF16)
        to_outer(k).start()
        share(k).start()

    def outer_final(k):
        to_outer(k).wait_recv()
        share(k).start()

    @pl.when(inner)
    def _():
        pl.semaphore_wait(barrier, 3)

    @pl.when(outer)
    def _():
        pl.semaphore_wait(barrier, 2)

    def terms(k, c):
        term(k)

        @pl.when(jnp.logical_and(outer, k >= D2D_LAG))
        def _():
            outer_sum(k - D2D_LAG)

        @pl.when(jnp.logical_and(inner, k >= IN_START))
        def _():
            inner_sum(k - IN_START)

        @pl.when(jnp.logical_and(inner, k >= IN_START + FIN_LAG))
        def _():
            inner_final(k - IN_START - FIN_LAG)

        return c

    lax.fori_loop(0, n_k, terms, 0)

    def loop(lo, hi, f):
        def it(k, c):
            f(k)
            return c

        lax.fori_loop(lo, hi, it, 0)

    @pl.when(outer)
    def _():
        loop(n_k - D2D_LAG, n_k, outer_sum)
        loop(0, n_k, outer_final)
        loop(0, n_k, lambda k: to_inner(k).wait_send())

    @pl.when(inner)
    def _():
        first = n_k - IN_START

        def both(k):
            inner_sum(k)
            inner_final(k - FIN_LAG)

        assert first >= FIN_LAG
        loop(first, n_k, both)
        loop(n_k - FIN_LAG, n_k, inner_final)

        def sent(k):
            across(k).wait_send()
            to_outer(k).wait_send()

        loop(0, n_k, sent)

    def finish(k):
        d2d(k).wait_send()
        share(k).wait_send()
        share_arrival(k).wait_recv()

    loop(0, n_k, finish)


def solution(mesh):
    def step(x, w_gate, w_up, w_down):
        rows, depth = x.shape
        width = w_gate.shape[1]
        out = w_down.shape[1]
        half = rows // 2
        n_gu = (width // GU_COLS) * GU_PARTS
        n_k = out // Y_COLS
        kd = depth // GU_PARTS
        dma = pltpu.SemaphoreType.DMA
        return pl.pallas_call(
            kernel,
            out_shape=pltpu.VMEM((rows, out), BF16),
            in_specs=[pl.BlockSpec(memory_space=pl.ANY)] * 4,
            out_specs=pl.BlockSpec(memory_space=pltpu.VMEM),
            scratch_shapes=[
                pltpu.VMEM((rows, depth), BF16),
                pltpu.VMEM((n_gu, kd, GU_COLS), BF16),
                pltpu.VMEM((n_gu, kd, GU_COLS), BF16),
                pltpu.VMEM((n_k, width, Y_COLS), BF16),
                pltpu.VMEM((rows, GU_COLS), F32),
                pltpu.VMEM((rows, GU_COLS), F32),
                pltpu.VMEM((rows, width), BF16),
                pltpu.VMEM((n_k, half, Y_COLS), F32),
                pltpu.VMEM((n_k, half, Y_COLS), BF16),
                pltpu.VMEM((n_k, half, Y_COLS), BF16),
                pltpu.VMEM((n_k, half, Y_COLS), BF16),
                pltpu.VMEM((n_k, half, Y_COLS), BF16),
                pltpu.VMEM((n_k, half, Y_COLS), BF16),
                dma((2,)),
                dma((n_gu,)),
                dma((n_gu,)),
                dma((n_k,)),
                dma((n_k,)),
                dma((n_k,)),
                dma((n_k,)),
                dma((2, n_k)),
                dma((n_k,)),
                dma((n_k,)),
                dma((n_k,)),
                dma((n_k,)),
            ],
            compiler_params=pltpu.CompilerParams(
                collective_id=0, has_side_effects=True, vmem_limit_bytes=58 * 1024 * 1024
            ),
        )(x, w_gate, w_up, w_down)

    return jax.shard_map(
        step,
        mesh=mesh,
        in_specs=(P("dp", None), P(None, "tp"), P(None, "tp"), P("tp", None)),
        out_specs=P("dp", None),
        check_vma=False,
    )
```

```python
import functools

import jax
import jax.numpy as jnp
from jax import lax
from jax.experimental import pallas as pl
from jax.experimental.pallas import tpu as pltpu
from jax.sharding import PartitionSpec as P

MESH = pl.DeviceIdType.MESH
F32, BF16 = jnp.float32, jnp.bfloat16

GU_COLS = 256
GU_PARTS = 4
Y_COLS = 256
WD_PIECES = 4
D2D_LAG = 2
IN_START = 8
FIN_LAG = 5


def kernel(
    x_hbm, wg_hbm, wu_hbm, wd_hbm, y_ref,
    x_v, wg_v, wu_v, wd_v, g_acc, u_acc, hid, own, snd, rcv, part, a_rcv, b_rcv,
    x_sem, wg_sem, wu_sem, wd_sem,
    d_ss, d_rs, p_ss, p_rs, f_ss, f_rs, g_ss, g_rs,
):
    tp = lax.axis_index("tp")
    core = lax.rem(tp, 2)
    z = lax.div(tp, 2)
    sibling = tp + 1 - 2 * core
    inner = jnp.logical_and(z > 0, z < 3)
    outer = jnp.logical_not(inner)
    low = z < 2
    onward = jnp.where(low, tp + 2, tp - 2)
    back = jnp.where(low, tp - 2, tp + 2)

    rows, half = x_v.shape[0], x_v.shape[0] // 2
    kd = wg_v.shape[1]
    n_j = wg_v.shape[0] // GU_PARTS
    n_k = wd_v.shape[0] * WD_PIECES
    wd_cols = WD_PIECES * Y_COLS
    mine = pl.ds(pl.multiple_of(core * half, half), half)
    theirs = pl.ds(pl.multiple_of((1 - core) * half, half), half)

    barrier = pltpu.get_barrier_semaphore()
    pl.semaphore_signal(barrier, inc=1, device_id={"tp": sibling}, device_id_type=MESH)
    pl.semaphore_signal(barrier, inc=1, device_id={"tp": onward}, device_id_type=MESH)

    @pl.when(inner)
    def _():
        pl.semaphore_signal(barrier, inc=1, device_id={"tp": back}, device_id_type=MESH)

    def ycols(k):
        return pl.ds(pl.multiple_of(k * Y_COLS, Y_COLS), Y_COLS)

    def x_copy(part_rows, i):
        return pltpu.make_async_copy(
            x_hbm.at[part_rows, :], x_v.at[pl.ds(i * half, half), :], x_sem.at[i]
        )

    def gu_copy(hbm, vmem, sem, j, p):
        i = j * GU_PARTS + p
        return pltpu.make_async_copy(
            hbm.at[
                pl.ds(pl.multiple_of(p * kd, kd), kd),
                pl.ds(pl.multiple_of(j * GU_COLS, GU_COLS), GU_COLS),
            ],
            vmem.at[i],
            sem.at[i],
        )

    def wd_copy(k):
        block = pl.ds(pl.multiple_of(k * wd_cols, wd_cols), wd_cols)
        return pltpu.make_async_copy(wd_hbm.at[:, block], wd_v.at[k], wd_sem.at[k])

    x_copy(mine, 0).start()
    x_copy(theirs, 1).start()

    def start_gu(j, c):
        for p in range(GU_PARTS):
            gu_copy(wg_hbm, wg_v, wg_sem, j, p).start()
            gu_copy(wu_hbm, wu_v, wu_sem, j, p).start()
        return c

    lax.fori_loop(0, n_j, start_gu, 0)

    def start_wd(k, c):
        wd_copy(k).start()
        return c

    lax.fori_loop(0, n_k // WD_PIECES, start_wd, 0)

    x_copy(mine, 0).wait()
    x_copy(theirs, 1).wait()

    def gate_up(j, c):
        for p in range(GU_PARTS):
            i = j * GU_PARTS + p
            xs = x_v[:, p * kd : (p + 1) * kd]
            gu_copy(wg_hbm, wg_v, wg_sem, j, p).wait()
            gu_copy(wu_hbm, wu_v, wu_sem, j, p).wait()
            g = jnp.dot(xs, wg_v[i], preferred_element_type=F32)
            u = jnp.dot(xs, wu_v[i], preferred_element_type=F32)
            if p == 0:
                g_acc[...] = g
                u_acc[...] = u
            elif p < GU_PARTS - 1:
                g_acc[...] += g
                u_acc[...] += u
            else:
                g = g_acc[...] + g
                u = u_acc[...] + u
                hid[:, pl.ds(pl.multiple_of(j * GU_COLS, GU_COLS), GU_COLS)] = (
                    jax.nn.silu(g) * u
                ).astype(BF16)
        return c

    lax.fori_loop(0, n_j, gate_up, 0)

    def d2d(k):
        return pltpu.make_async_remote_copy(
            src_ref=snd.at[k], dst_ref=rcv.at[k], send_sem=d_ss.at[k], recv_sem=d_rs.at[k],
            device_id={"tp": sibling}, device_id_type=MESH,
        )

    def to_inner(k):
        return pltpu.make_async_remote_copy(
            src_ref=part.at[k], dst_ref=a_rcv.at[k], send_sem=p_ss.at[k], recv_sem=p_rs.at[0, k],
            device_id={"tp": onward}, device_id_type=MESH,
        )

    def across(k):
        return pltpu.make_async_remote_copy(
            src_ref=part.at[k], dst_ref=b_rcv.at[k], send_sem=p_ss.at[k], recv_sem=p_rs.at[1, k],
            device_id={"tp": onward}, device_id_type=MESH,
        )

    def to_outer(k):
        return pltpu.make_async_remote_copy(
            src_ref=y_ref.at[mine, ycols(k)], dst_ref=y_ref.at[mine, ycols(k)],
            send_sem=f_ss.at[k], recv_sem=f_rs.at[k],
            device_id={"tp": back}, device_id_type=MESH,
        )

    def share(k):
        return pltpu.make_async_remote_copy(
            src_ref=y_ref.at[mine, ycols(k)], dst_ref=y_ref.at[mine, ycols(k)],
            send_sem=g_ss.at[k], recv_sem=g_rs.at[k],
            device_id={"tp": sibling}, device_id_type=MESH,
        )

    def share_arrival(k):
        return pltpu.make_async_remote_copy(
            src_ref=y_ref.at[theirs, ycols(k)], dst_ref=y_ref.at[theirs, ycols(k)],
            send_sem=g_ss.at[k], recv_sem=g_rs.at[k],
            device_id={"tp": sibling}, device_id_type=MESH,
        )

    def term(k):
        block, at = lax.div(k, WD_PIECES), lax.rem(k, WD_PIECES)

        @pl.when(at == 0)
        def _():
            wd_copy(block).wait()

        w = wd_v[block, :, pl.ds(pl.multiple_of(at * Y_COLS, Y_COLS), Y_COLS)]
        t = jnp.dot(hid[...], w, preferred_element_type=F32)
        own[k] = t[:half]
        snd[k] = t[half:].astype(BF16)
        d2d(k).start()

    def outer_sum(k):
        d2d(k).wait_recv()
        part[k] = (own[k] + rcv[k].astype(F32)).astype(BF16)
        to_inner(k).start()

    def inner_sum(k):
        d2d(k).wait_recv()
        to_inner(k).wait_recv()
        part[k] = (own[k] + rcv[k].astype(F32) + a_rcv[k].astype(F32)).astype(BF16)
        across(k).start()

    def inner_final(k):
        across(k).wait_recv()
        y_ref[mine, ycols(k)] = (part[k].astype(F32) + b_rcv[k].astype(F32)).astype(BF16)
        to_outer(k).start()
        share(k).start()

    def outer_final(k):
        to_outer(k).wait_recv()
        share(k).start()

    @pl.when(inner)
    def _():
        pl.semaphore_wait(barrier, 3)

    @pl.when(outer)
    def _():
        pl.semaphore_wait(barrier, 2)

    def terms(k, c):
        term(k)

        @pl.when(jnp.logical_and(outer, k >= D2D_LAG))
        def _():
            outer_sum(k - D2D_LAG)

        @pl.when(jnp.logical_and(inner, k >= IN_START))
        def _():
            inner_sum(k - IN_START)

        @pl.when(jnp.logical_and(inner, k >= IN_START + FIN_LAG))
        def _():
            inner_final(k - IN_START - FIN_LAG)

        return c

    lax.fori_loop(0, n_k, terms, 0)

    def loop(lo, hi, f):
        def it(k, c):
            f(k)
            return c

        lax.fori_loop(lo, hi, it, 0)

    @pl.when(outer)
    def _():
        loop(n_k - D2D_LAG, n_k, outer_sum)
        loop(0, n_k, outer_final)
        loop(0, n_k, lambda k: to_inner(k).wait_send())

    @pl.when(inner)
    def _():
        first = n_k - IN_START

        def both(k):
            inner_sum(k)
            inner_final(k - FIN_LAG)

        assert first >= FIN_LAG
        loop(first, n_k, both)
        loop(n_k - FIN_LAG, n_k, inner_final)

        def sent(k):
            across(k).wait_send()
            to_outer(k).wait_send()

        loop(0, n_k, sent)

    def finish(k):
        d2d(k).wait_send()
        share(k).wait_send()
        share_arrival(k).wait_recv()

    loop(0, n_k, finish)


def solution(mesh):
    def step(x, w_gate, w_up, w_down):
        rows, depth = x.shape
        width = w_gate.shape[1]
        out = w_down.shape[1]
        half = rows // 2
        n_gu = (width // GU_COLS) * GU_PARTS
        n_k = out // Y_COLS
        kd = depth // GU_PARTS
        dma = pltpu.SemaphoreType.DMA
        return pl.pallas_call(
            kernel,
            out_shape=pltpu.VMEM((rows, out), BF16),
            in_specs=[pl.BlockSpec(memory_space=pl.ANY)] * 4,
            out_specs=pl.BlockSpec(memory_space=pltpu.VMEM),
            scratch_shapes=[
                pltpu.VMEM((rows, depth), BF16),
                pltpu.VMEM((n_gu, kd, GU_COLS), BF16),
                pltpu.VMEM((n_gu, kd, GU_COLS), BF16),
                pltpu.VMEM((n_k // WD_PIECES, width, WD_PIECES * Y_COLS), BF16),
                pltpu.VMEM((rows, GU_COLS), F32),
                pltpu.VMEM((rows, GU_COLS), F32),
                pltpu.VMEM((rows, width), BF16),
                pltpu.VMEM((n_k, half, Y_COLS), F32),
                pltpu.VMEM((n_k, half, Y_COLS), BF16),
                pltpu.VMEM((n_k, half, Y_COLS), BF16),
                pltpu.VMEM((n_k, half, Y_COLS), BF16),
                pltpu.VMEM((n_k, half, Y_COLS), BF16),
                pltpu.VMEM((n_k, half, Y_COLS), BF16),
                dma((2,)),
                dma((n_gu,)),
                dma((n_gu,)),
                dma((n_k,)),
                dma((n_k,)),
                dma((n_k,)),
                dma((n_k,)),
                dma((2, n_k)),
                dma((n_k,)),
                dma((n_k,)),
                dma((n_k,)),
                dma((n_k,)),
            ],
            compiler_params=pltpu.CompilerParams(
                collective_id=0, has_side_effects=True, vmem_limit_bytes=58 * 1024 * 1024
            ),
        )(x, w_gate, w_up, w_down)

    return jax.shard_map(
        step,
        mesh=mesh,
        in_specs=(P("dp", None), P(None, "tp"), P(None, "tp"), P("tp", None)),
        out_specs=P("dp", None),
        check_vma=False,
    )
```

```python
import jax
import jax.numpy as jnp
from jax import lax
from jax.experimental import pallas as pl
from jax.experimental.pallas import tpu as pltpu
from jax.sharding import PartitionSpec as P

MESH = pl.DeviceIdType.MESH
F32, BF16 = jnp.float32, jnp.bfloat16

GU_COLS = 256
GU_PARTS = 4
Y_COLS = 256
ROWS = ((80, 48), (0, 80))
D2D_LAG = 2
IN_START = 8
FIN_LAG = 5


def kernel(
    x_hbm, wg_hbm, wu_hbm, wd_hbm, y_ref,
    x_v, wg_v, wu_v, wd_v, g_acc, u_acc, hid, own, snd, rcv, part, a_rcv, b_rcv,
    x_sem, wg_sem, wu_sem, wd_sem,
    d_ss, d_rs, p_ss, p_rs, f_ss, f_rs, g_ss, g_rs,
):
    tp = lax.axis_index("tp")
    core = lax.rem(tp, 2)
    z = lax.div(tp, 2)
    sibling = tp + 1 - 2 * core
    inner = jnp.logical_and(z > 0, z < 3)
    outer = jnp.logical_not(inner)
    low = z < 2
    onward = jnp.where(low, tp + 2, tp - 2)
    back = jnp.where(low, tp - 2, tp + 2)

    kd = wg_v.shape[1]
    n_j = wg_v.shape[0] // GU_PARTS
    n_k = wd_v.shape[0]
    barrier = pltpu.get_barrier_semaphore()
    pl.semaphore_signal(barrier, inc=1, device_id={"tp": sibling}, device_id_type=MESH)
    pl.semaphore_signal(barrier, inc=1, device_id={"tp": onward}, device_id_type=MESH)

    @pl.when(inner)
    def _():
        pl.semaphore_signal(barrier, inc=1, device_id={"tp": back}, device_id_type=MESH)

    def ycols(k):
        return pl.ds(pl.multiple_of(k * Y_COLS, Y_COLS), Y_COLS)

    x_copy = pltpu.make_async_copy(x_hbm, x_v, x_sem)

    def gu_copy(hbm, vmem, sem, j, p):
        i = j * GU_PARTS + p
        return pltpu.make_async_copy(
            hbm.at[
                pl.ds(pl.multiple_of(p * kd, kd), kd),
                pl.ds(pl.multiple_of(j * GU_COLS, GU_COLS), GU_COLS),
            ],
            vmem.at[i],
            sem.at[i],
        )

    def wd_copy(k):
        return pltpu.make_async_copy(wd_hbm.at[:, ycols(k)], wd_v.at[k], wd_sem.at[k])

    x_copy.start()

    def start_gu(j, c):
        for p in range(GU_PARTS):
            gu_copy(wg_hbm, wg_v, wg_sem, j, p).start()
            gu_copy(wu_hbm, wu_v, wu_sem, j, p).start()
        return c

    lax.fori_loop(0, n_j, start_gu, 0)

    def start_wd(k, c):
        wd_copy(k).start()
        return c

    lax.fori_loop(0, n_k, start_wd, 0)

    x_copy.wait()

    def gate_up(j, c):
        for p in range(GU_PARTS):
            i = j * GU_PARTS + p
            xs = x_v[:, p * kd : (p + 1) * kd]
            gu_copy(wg_hbm, wg_v, wg_sem, j, p).wait()
            gu_copy(wu_hbm, wu_v, wu_sem, j, p).wait()
            g = jnp.dot(xs, wg_v[i], preferred_element_type=F32)
            u = jnp.dot(xs, wu_v[i], preferred_element_type=F32)
            if p == 0:
                g_acc[...] = g
                u_acc[...] = u
            elif p < GU_PARTS - 1:
                g_acc[...] += g
                u_acc[...] += u
            else:
                g = g_acc[...] + g
                u = u_acc[...] + u
                hid[:, pl.ds(pl.multiple_of(j * GU_COLS, GU_COLS), GU_COLS)] = (
                    jax.nn.silu(g) * u
                ).astype(BF16)
        return c

    lax.fori_loop(0, n_j, gate_up, 0)

    @pl.when(inner)
    def _():
        pl.semaphore_wait(barrier, 3)

    @pl.when(outer)
    def _():
        pl.semaphore_wait(barrier, 2)

    def loop(lo, hi, f):
        def it(k, c):
            f(k)
            return c

        lax.fori_loop(lo, hi, it, 0)

    def remote(src, dst, send, recv, dev):
        return pltpu.make_async_remote_copy(
            src_ref=src, dst_ref=dst, send_sem=send, recv_sem=recv,
            device_id={"tp": dev}, device_id_type=MESH,
        )

    def run(me):
        lo, n = ROWS[me]
        other_lo, other_n = ROWS[1 - me]
        mine, theirs = pl.ds(lo, n), pl.ds(other_lo, other_n)
        top = pl.ds(0, n)

        def give(k):
            return remote(
                snd.at[k, theirs], rcv.at[k, pl.ds(0, other_n)], d_ss.at[k], d_rs.at[k], sibling
            )

        def got(k):
            return remote(snd.at[k, mine], rcv.at[k, top], d_ss.at[k], d_rs.at[k], sibling)

        def to_inner(k):
            return remote(
                part.at[k, top], a_rcv.at[k, top], p_ss.at[k], p_rs.at[0, k], onward
            )

        def across(k):
            return remote(
                part.at[k, top], b_rcv.at[k, top], p_ss.at[k], p_rs.at[1, k], onward
            )

        def to_outer(k):
            y_k = y_ref.at[mine, ycols(k)]
            return remote(y_k, y_k, f_ss.at[k], f_rs.at[k], back)

        def share(k):
            y_k = y_ref.at[mine, ycols(k)]
            return remote(y_k, y_k, g_ss.at[k], g_rs.at[k], sibling)

        def shared(k):
            y_k = y_ref.at[theirs, ycols(k)]
            return remote(y_k, y_k, g_ss.at[k], g_rs.at[k], sibling)

        def term(k):
            wd_copy(k).wait()
            t = jnp.dot(hid[...], wd_v[k], preferred_element_type=F32)
            own[k, top] = t[lo : lo + n]
            snd[k, theirs] = t[other_lo : other_lo + other_n].astype(BF16)
            give(k).start()

        def outer_sum(k):
            got(k).wait_recv()
            part[k, top] = (own[k, top] + rcv[k, top].astype(F32)).astype(BF16)
            to_inner(k).start()

        def inner_sum(k):
            got(k).wait_recv()
            to_inner(k).wait_recv()
            part[k, top] = (
                own[k, top] + rcv[k, top].astype(F32) + a_rcv[k, top].astype(F32)
            ).astype(BF16)
            across(k).start()

        def inner_final(k):
            across(k).wait_recv()
            y_ref[mine, ycols(k)] = (
                part[k, top].astype(F32) + b_rcv[k, top].astype(F32)
            ).astype(BF16)
            to_outer(k).start()
            share(k).start()

        def outer_final(k):
            to_outer(k).wait_recv()
            share(k).start()

        def terms(k):
            term(k)

            @pl.when(jnp.logical_and(outer, k >= D2D_LAG))
            def _():
                outer_sum(k - D2D_LAG)

            @pl.when(jnp.logical_and(inner, k >= IN_START))
            def _():
                inner_sum(k - IN_START)

            @pl.when(jnp.logical_and(inner, k >= IN_START + FIN_LAG))
            def _():
                inner_final(k - IN_START - FIN_LAG)

        loop(0, n_k, terms)

        @pl.when(outer)
        def _():
            loop(n_k - D2D_LAG, n_k, outer_sum)
            loop(0, n_k, outer_final)
            loop(0, n_k, lambda k: to_inner(k).wait_send())

        @pl.when(inner)
        def _():
            first = n_k - IN_START
            assert first >= FIN_LAG

            def both(k):
                inner_sum(k)
                inner_final(k - FIN_LAG)

            loop(first, n_k, both)
            loop(n_k - FIN_LAG, n_k, inner_final)

            def sent(k):
                across(k).wait_send()
                to_outer(k).wait_send()

            loop(0, n_k, sent)

        def finish(k):
            give(k).wait_send()
            share(k).wait_send()
            shared(k).wait_recv()

        loop(0, n_k, finish)

    for me in (0, 1):

        @pl.when(core == me)
        def _():
            run(me)


def solution(mesh):
    def step(x, w_gate, w_up, w_down):
        rows, depth = x.shape
        width = w_gate.shape[1]
        out = w_down.shape[1]
        most = max(n for _, n in ROWS)
        n_gu = (width // GU_COLS) * GU_PARTS
        n_k = out // Y_COLS
        kd = depth // GU_PARTS
        dma = pltpu.SemaphoreType.DMA
        return pl.pallas_call(
            kernel,
            out_shape=pltpu.VMEM((rows, out), BF16),
            in_specs=[pl.BlockSpec(memory_space=pl.ANY)] * 4,
            out_specs=pl.BlockSpec(memory_space=pltpu.VMEM),
            scratch_shapes=[
                pltpu.VMEM((rows, depth), BF16),
                pltpu.VMEM((n_gu, kd, GU_COLS), BF16),
                pltpu.VMEM((n_gu, kd, GU_COLS), BF16),
                pltpu.VMEM((n_k, width, Y_COLS), BF16),
                pltpu.VMEM((rows, GU_COLS), F32),
                pltpu.VMEM((rows, GU_COLS), F32),
                pltpu.VMEM((rows, width), BF16),
                pltpu.VMEM((n_k, most, Y_COLS), F32),
                pltpu.VMEM((n_k, rows, Y_COLS), BF16),
                pltpu.VMEM((n_k, most, Y_COLS), BF16),
                pltpu.VMEM((n_k, most, Y_COLS), BF16),
                pltpu.VMEM((n_k, most, Y_COLS), BF16),
                pltpu.VMEM((n_k, most, Y_COLS), BF16),
                dma,
                dma((n_gu,)),
                dma((n_gu,)),
                dma((n_k,)),
                dma((n_k,)),
                dma((n_k,)),
                dma((n_k,)),
                dma((2, n_k)),
                dma((n_k,)),
                dma((n_k,)),
                dma((n_k,)),
                dma((n_k,)),
            ],
            compiler_params=pltpu.CompilerParams(
                collective_id=0, has_side_effects=True, vmem_limit_bytes=58 * 1024 * 1024
            ),
        )(x, w_gate, w_up, w_down)

    return jax.shard_map(
        step,
        mesh=mesh,
        in_specs=(P("dp", None), P(None, "tp"), P(None, "tp"), P("tp", None)),
        out_specs=P("dp", None),
        check_vma=False,
    )
```

```python
import jax
import jax.numpy as jnp
from jax import lax
from jax.experimental import pallas as pl
from jax.experimental.pallas import tpu as pltpu
from jax.sharding import PartitionSpec as P

MESH = pl.DeviceIdType.MESH
F32, BF16 = jnp.float32, jnp.bfloat16

GU_COLS = 256
GU_PARTS = 4
Y_COLS = 256
ROWS = ((80, 48), (0, 80))
D2D_LAG = 2
IN_START = 8
TAKE_LAG = 8
FIN_LAG = 5


def kernel(
    x_hbm, wg_hbm, wu_hbm, wd_hbm, y_ref,
    x_v, wg_v, wu_v, wd_v, g_acc, u_acc, hid, own, snd, rcv, part, a_rcv, b_rcv, fin, fin_other,
    x_sem, wg_sem, wu_sem, wd_sem,
    d_ss, d_rs, p_ss, p_rs, f_ss, f_rs, g_ss, g_rs,
):
    tp = lax.axis_index("tp")
    core = lax.rem(tp, 2)
    z = lax.div(tp, 2)
    sibling = tp + 1 - 2 * core
    inner = jnp.logical_and(z > 0, z < 3)
    outer = jnp.logical_not(inner)
    low = z < 2
    onward = jnp.where(low, tp + 2, tp - 2)
    back = jnp.where(low, tp - 2, tp + 2)

    kd = wg_v.shape[1]
    n_j = wg_v.shape[0] // GU_PARTS
    n_k = wd_v.shape[0]
    barrier = pltpu.get_barrier_semaphore()
    pl.semaphore_signal(barrier, inc=1, device_id={"tp": sibling}, device_id_type=MESH)
    pl.semaphore_signal(barrier, inc=1, device_id={"tp": onward}, device_id_type=MESH)

    @pl.when(inner)
    def _():
        pl.semaphore_signal(barrier, inc=1, device_id={"tp": back}, device_id_type=MESH)

    def ycols(k):
        return pl.ds(pl.multiple_of(k * Y_COLS, Y_COLS), Y_COLS)

    x_copy = pltpu.make_async_copy(x_hbm, x_v, x_sem)

    def gu_copy(hbm, vmem, sem, j, p):
        i = j * GU_PARTS + p
        return pltpu.make_async_copy(
            hbm.at[
                pl.ds(pl.multiple_of(p * kd, kd), kd),
                pl.ds(pl.multiple_of(j * GU_COLS, GU_COLS), GU_COLS),
            ],
            vmem.at[i],
            sem.at[i],
        )

    def wd_copy(k):
        return pltpu.make_async_copy(wd_hbm.at[:, ycols(k)], wd_v.at[k], wd_sem.at[k])

    x_copy.start()

    def start_gu(j, c):
        for p in range(GU_PARTS):
            gu_copy(wg_hbm, wg_v, wg_sem, j, p).start()
            gu_copy(wu_hbm, wu_v, wu_sem, j, p).start()
        return c

    lax.fori_loop(0, n_j, start_gu, 0)

    def start_wd(k, c):
        wd_copy(k).start()
        return c

    lax.fori_loop(0, n_k, start_wd, 0)

    x_copy.wait()

    def gate_up(j, c):
        for p in range(GU_PARTS):
            i = j * GU_PARTS + p
            xs = x_v[:, p * kd : (p + 1) * kd]
            gu_copy(wg_hbm, wg_v, wg_sem, j, p).wait()
            gu_copy(wu_hbm, wu_v, wu_sem, j, p).wait()
            g = jnp.dot(xs, wg_v[i], preferred_element_type=F32)
            u = jnp.dot(xs, wu_v[i], preferred_element_type=F32)
            if p == 0:
                g_acc[...] = g
                u_acc[...] = u
            elif p < GU_PARTS - 1:
                g_acc[...] += g
                u_acc[...] += u
            else:
                g = g_acc[...] + g
                u = u_acc[...] + u
                hid[:, pl.ds(pl.multiple_of(j * GU_COLS, GU_COLS), GU_COLS)] = (
                    jax.nn.silu(g) * u
                ).astype(BF16)
        return c

    lax.fori_loop(0, n_j, gate_up, 0)

    @pl.when(inner)
    def _():
        pl.semaphore_wait(barrier, 3)

    @pl.when(outer)
    def _():
        pl.semaphore_wait(barrier, 2)

    def loop(lo, hi, f):
        def it(k, c):
            f(k)
            return c

        lax.fori_loop(lo, hi, it, 0)

    def remote(src, dst, send, recv, dev):
        return pltpu.make_async_remote_copy(
            src_ref=src, dst_ref=dst, send_sem=send, recv_sem=recv,
            device_id={"tp": dev}, device_id_type=MESH,
        )

    def run(me):
        lo, n = ROWS[me]
        other_lo, other_n = ROWS[1 - me]
        mine, theirs = pl.ds(lo, n), pl.ds(other_lo, other_n)
        top = pl.ds(0, n)

        def give(k):
            return remote(
                snd.at[k, theirs], rcv.at[k, pl.ds(0, other_n)], d_ss.at[k], d_rs.at[k], sibling
            )

        def got(k):
            return remote(snd.at[k, mine], rcv.at[k, top], d_ss.at[k], d_rs.at[k], sibling)

        def to_inner(k):
            return remote(
                part.at[k, top], a_rcv.at[k, top], p_ss.at[k], p_rs.at[0, k], onward
            )

        def across(k):
            return remote(
                part.at[k, top], b_rcv.at[k, top], p_ss.at[k], p_rs.at[1, k], onward
            )

        def to_outer(k):
            return remote(fin.at[k, top], fin.at[k, top], f_ss.at[k], f_rs.at[k], back)

        def share(k):
            return remote(fin.at[k, top], fin_other.at[k, top], g_ss.at[k], g_rs.at[k], sibling)

        def shared(k):
            got_k = fin_other.at[k, pl.ds(0, other_n)]
            return remote(got_k, got_k, g_ss.at[k], g_rs.at[k], sibling)

        def take(k):
            @pl.when(k >= 0)
            def _():
                shared(k).wait_recv()
                y_ref[theirs, ycols(k)] = fin_other[k, pl.ds(0, other_n)]

        def term(k):
            wd_copy(k).wait()
            t = jnp.dot(hid[...], wd_v[k], preferred_element_type=F32)
            own[k, top] = t[lo : lo + n]
            snd[k, theirs] = t[other_lo : other_lo + other_n].astype(BF16)
            give(k).start()

        def outer_sum(k):
            got(k).wait_recv()
            part[k, top] = (own[k, top] + rcv[k, top].astype(F32)).astype(BF16)
            to_inner(k).start()

        def inner_sum(k):
            got(k).wait_recv()
            to_inner(k).wait_recv()
            part[k, top] = (
                own[k, top] + rcv[k, top].astype(F32) + a_rcv[k, top].astype(F32)
            ).astype(BF16)
            across(k).start()

        def inner_final(k):
            across(k).wait_recv()
            fin[k, top] = (part[k, top].astype(F32) + b_rcv[k, top].astype(F32)).astype(BF16)
            to_outer(k).start()
            share(k).start()
            y_ref[mine, ycols(k)] = fin[k, top]
            take(k - TAKE_LAG)

        def outer_final(k):
            to_outer(k).wait_recv()
            share(k).start()
            y_ref[mine, ycols(k)] = fin[k, top]
            take(k - TAKE_LAG)

        def terms(k):
            term(k)

            @pl.when(jnp.logical_and(outer, k >= D2D_LAG))
            def _():
                outer_sum(k - D2D_LAG)

            @pl.when(jnp.logical_and(inner, k >= IN_START))
            def _():
                inner_sum(k - IN_START)

            @pl.when(jnp.logical_and(inner, k >= IN_START + FIN_LAG))
            def _():
                inner_final(k - IN_START - FIN_LAG)

        loop(0, n_k, terms)

        @pl.when(outer)
        def _():
            loop(n_k - D2D_LAG, n_k, outer_sum)
            loop(0, n_k, outer_final)
            loop(0, n_k, lambda k: to_inner(k).wait_send())

        @pl.when(inner)
        def _():
            first = n_k - IN_START
            assert first >= FIN_LAG

            def both(k):
                inner_sum(k)
                inner_final(k - FIN_LAG)

            loop(first, n_k, both)
            loop(n_k - FIN_LAG, n_k, inner_final)

            def sent(k):
                across(k).wait_send()
                to_outer(k).wait_send()

            loop(0, n_k, sent)

        def finish(k):
            give(k).wait_send()
            share(k).wait_send()

        loop(n_k - TAKE_LAG, n_k, take)
        loop(0, n_k, finish)

    for me in (0, 1):

        @pl.when(core == me)
        def _():
            run(me)


def solution(mesh):
    def step(x, w_gate, w_up, w_down):
        rows, depth = x.shape
        width = w_gate.shape[1]
        out = w_down.shape[1]
        most = max(n for _, n in ROWS)
        n_gu = (width // GU_COLS) * GU_PARTS
        n_k = out // Y_COLS
        kd = depth // GU_PARTS
        dma = pltpu.SemaphoreType.DMA
        return pl.pallas_call(
            kernel,
            out_shape=pltpu.VMEM((rows, out), BF16),
            in_specs=[pl.BlockSpec(memory_space=pl.ANY)] * 4,
            out_specs=pl.BlockSpec(memory_space=pltpu.VMEM),
            scratch_shapes=[
                pltpu.VMEM((rows, depth), BF16),
                pltpu.VMEM((n_gu, kd, GU_COLS), BF16),
                pltpu.VMEM((n_gu, kd, GU_COLS), BF16),
                pltpu.VMEM((n_k, width, Y_COLS), BF16),
                pltpu.VMEM((rows, GU_COLS), F32),
                pltpu.VMEM((rows, GU_COLS), F32),
                pltpu.VMEM((rows, width), BF16),
                pltpu.VMEM((n_k, most, Y_COLS), F32),
                pltpu.VMEM((n_k, rows, Y_COLS), BF16),
                pltpu.VMEM((n_k, most, Y_COLS), BF16),
                pltpu.VMEM((n_k, most, Y_COLS), BF16),
                pltpu.VMEM((n_k, most, Y_COLS), BF16),
                pltpu.VMEM((n_k, most, Y_COLS), BF16),
                pltpu.VMEM((n_k, most, Y_COLS), BF16),
                pltpu.VMEM((n_k, most, Y_COLS), BF16),
                dma,
                dma((n_gu,)),
                dma((n_gu,)),
                dma((n_k,)),
                dma((n_k,)),
                dma((n_k,)),
                dma((n_k,)),
                dma((2, n_k)),
                dma((n_k,)),
                dma((n_k,)),
                dma((n_k,)),
                dma((n_k,)),
            ],
            compiler_params=pltpu.CompilerParams(
                collective_id=0, has_side_effects=True, vmem_limit_bytes=58 * 1024 * 1024
            ),
        )(x, w_gate, w_up, w_down)

    return jax.shard_map(
        step,
        mesh=mesh,
        in_specs=(P("dp", None), P(None, "tp"), P(None, "tp"), P("tp", None)),
        out_specs=P("dp", None),
        check_vma=False,
    )
```

```python
import jax
import jax.numpy as jnp
from jax import lax
from jax.experimental import pallas as pl
from jax.experimental.pallas import tpu as pltpu
from jax.sharding import PartitionSpec as P

MESH = pl.DeviceIdType.MESH
F32, BF16 = jnp.float32, jnp.bfloat16

GU_COLS = 256
GU_PARTS = 4
Y_COLS = 512
ROWS = ((80, 48), (0, 80))
D2D_LAG = 1
IN_START = 5
FIN_LAG = 3


def kernel(
    x_hbm, wg_hbm, wu_hbm, wd_hbm, y_ref,
    x_v, wg_v, wu_v, wd_v, g_acc, u_acc, hid, own, snd, rcv, part, a_rcv, b_rcv,
    x_sem, wg_sem, wu_sem, wd_sem,
    d_ss, d_rs, p_ss, p_rs, f_ss, f_rs, g_ss, g_rs,
):
    tp = lax.axis_index("tp")
    core = lax.rem(tp, 2)
    z = lax.div(tp, 2)
    sibling = tp + 1 - 2 * core
    inner = jnp.logical_and(z > 0, z < 3)
    outer = jnp.logical_not(inner)
    low = z < 2
    onward = jnp.where(low, tp + 2, tp - 2)
    back = jnp.where(low, tp - 2, tp + 2)

    kd = wg_v.shape[1]
    n_j = wg_v.shape[0] // GU_PARTS
    n_k = wd_v.shape[0]
    barrier = pltpu.get_barrier_semaphore()
    pl.semaphore_signal(barrier, inc=1, device_id={"tp": sibling}, device_id_type=MESH)
    pl.semaphore_signal(barrier, inc=1, device_id={"tp": onward}, device_id_type=MESH)

    @pl.when(inner)
    def _():
        pl.semaphore_signal(barrier, inc=1, device_id={"tp": back}, device_id_type=MESH)

    def ycols(k):
        return pl.ds(pl.multiple_of(k * Y_COLS, Y_COLS), Y_COLS)

    x_copy = pltpu.make_async_copy(x_hbm, x_v, x_sem)

    def gu_copy(hbm, vmem, sem, j, p):
        i = j * GU_PARTS + p
        return pltpu.make_async_copy(
            hbm.at[
                pl.ds(pl.multiple_of(p * kd, kd), kd),
                pl.ds(pl.multiple_of(j * GU_COLS, GU_COLS), GU_COLS),
            ],
            vmem.at[i],
            sem.at[i],
        )

    def wd_copy(k):
        return pltpu.make_async_copy(wd_hbm.at[:, ycols(k)], wd_v.at[k], wd_sem.at[k])

    x_copy.start()

    def start_gu(j, c):
        for p in range(GU_PARTS):
            gu_copy(wg_hbm, wg_v, wg_sem, j, p).start()
            gu_copy(wu_hbm, wu_v, wu_sem, j, p).start()
        return c

    lax.fori_loop(0, n_j, start_gu, 0)

    def start_wd(k, c):
        wd_copy(k).start()
        return c

    lax.fori_loop(0, n_k, start_wd, 0)

    x_copy.wait()

    def gate_up(j, c):
        for p in range(GU_PARTS):
            i = j * GU_PARTS + p
            xs = x_v[:, p * kd : (p + 1) * kd]
            gu_copy(wg_hbm, wg_v, wg_sem, j, p).wait()
            gu_copy(wu_hbm, wu_v, wu_sem, j, p).wait()
            g = jnp.dot(xs, wg_v[i], preferred_element_type=F32)
            u = jnp.dot(xs, wu_v[i], preferred_element_type=F32)
            if p == 0:
                g_acc[...] = g
                u_acc[...] = u
            elif p < GU_PARTS - 1:
                g_acc[...] += g
                u_acc[...] += u
            else:
                g = g_acc[...] + g
                u = u_acc[...] + u
                hid[:, pl.ds(pl.multiple_of(j * GU_COLS, GU_COLS), GU_COLS)] = (
                    jax.nn.silu(g) * u
                ).astype(BF16)
        return c

    lax.fori_loop(0, n_j, gate_up, 0)

    @pl.when(inner)
    def _():
        pl.semaphore_wait(barrier, 3)

    @pl.when(outer)
    def _():
        pl.semaphore_wait(barrier, 2)

    def loop(lo, hi, f):
        def it(k, c):
            f(k)
            return c

        lax.fori_loop(lo, hi, it, 0)

    def remote(src, dst, send, recv, dev):
        return pltpu.make_async_remote_copy(
            src_ref=src, dst_ref=dst, send_sem=send, recv_sem=recv,
            device_id={"tp": dev}, device_id_type=MESH,
        )

    def run(me):
        lo, n = ROWS[me]
        other_lo, other_n = ROWS[1 - me]
        mine, theirs = pl.ds(lo, n), pl.ds(other_lo, other_n)
        top = pl.ds(0, n)

        def give(k):
            return remote(
                snd.at[k, theirs], rcv.at[k, pl.ds(0, other_n)], d_ss.at[k], d_rs.at[k], sibling
            )

        def got(k):
            return remote(snd.at[k, mine], rcv.at[k, top], d_ss.at[k], d_rs.at[k], sibling)

        def to_inner(k):
            return remote(
                part.at[k, top], a_rcv.at[k, top], p_ss.at[k], p_rs.at[0, k], onward
            )

        def across(k):
            return remote(
                part.at[k, top], b_rcv.at[k, top], p_ss.at[k], p_rs.at[1, k], onward
            )

        def to_outer(k):
            y_k = y_ref.at[mine, ycols(k)]
            return remote(y_k, y_k, f_ss.at[k], f_rs.at[k], back)

        def share(k):
            y_k = y_ref.at[mine, ycols(k)]
            return remote(y_k, y_k, g_ss.at[k], g_rs.at[k], sibling)

        def shared(k):
            y_k = y_ref.at[theirs, ycols(k)]
            return remote(y_k, y_k, g_ss.at[k], g_rs.at[k], sibling)

        def term(k):
            wd_copy(k).wait()
            t = jnp.dot(hid[...], wd_v[k], preferred_element_type=F32)
            own[k, top] = t[lo : lo + n]
            snd[k, theirs] = t[other_lo : other_lo + other_n].astype(BF16)
            give(k).start()

        def outer_sum(k):
            got(k).wait_recv()
            part[k, top] = (own[k, top] + rcv[k, top].astype(F32)).astype(BF16)
            to_inner(k).start()

        def inner_sum(k):
            got(k).wait_recv()
            to_inner(k).wait_recv()
            part[k, top] = (
                own[k, top] + rcv[k, top].astype(F32) + a_rcv[k, top].astype(F32)
            ).astype(BF16)
            across(k).start()

        def inner_final(k):
            across(k).wait_recv()
            y_ref[mine, ycols(k)] = (
                part[k, top].astype(F32) + b_rcv[k, top].astype(F32)
            ).astype(BF16)
            to_outer(k).start()
            share(k).start()

        def outer_final(k):
            to_outer(k).wait_recv()
            share(k).start()

        def terms(k):
            term(k)

            @pl.when(jnp.logical_and(outer, k >= D2D_LAG))
            def _():
                outer_sum(k - D2D_LAG)

            @pl.when(jnp.logical_and(inner, k >= IN_START))
            def _():
                inner_sum(k - IN_START)

            @pl.when(jnp.logical_and(inner, k >= IN_START + FIN_LAG))
            def _():
                inner_final(k - IN_START - FIN_LAG)

        loop(0, n_k, terms)

        @pl.when(outer)
        def _():
            loop(n_k - D2D_LAG, n_k, outer_sum)
            loop(0, n_k, outer_final)
            loop(0, n_k, lambda k: to_inner(k).wait_send())

        @pl.when(inner)
        def _():
            first = n_k - IN_START
            assert first >= FIN_LAG

            def both(k):
                inner_sum(k)
                inner_final(k - FIN_LAG)

            loop(first, n_k, both)
            loop(n_k - FIN_LAG, n_k, inner_final)

            def sent(k):
                across(k).wait_send()
                to_outer(k).wait_send()

            loop(0, n_k, sent)

        def finish(k):
            give(k).wait_send()
            share(k).wait_send()
            shared(k).wait_recv()

        loop(0, n_k, finish)

    for me in (0, 1):

        @pl.when(core == me)
        def _():
            run(me)


def solution(mesh):
    def step(x, w_gate, w_up, w_down):
        rows, depth = x.shape
        width = w_gate.shape[1]
        out = w_down.shape[1]
        most = max(n for _, n in ROWS)
        n_gu = (width // GU_COLS) * GU_PARTS
        n_k = out // Y_COLS
        kd = depth // GU_PARTS
        dma = pltpu.SemaphoreType.DMA
        return pl.pallas_call(
            kernel,
            out_shape=pltpu.VMEM((rows, out), BF16),
            in_specs=[pl.BlockSpec(memory_space=pl.ANY)] * 4,
            out_specs=pl.BlockSpec(memory_space=pltpu.VMEM),
            scratch_shapes=[
                pltpu.VMEM((rows, depth), BF16),
                pltpu.VMEM((n_gu, kd, GU_COLS), BF16),
                pltpu.VMEM((n_gu, kd, GU_COLS), BF16),
                pltpu.VMEM((n_k, width, Y_COLS), BF16),
                pltpu.VMEM((rows, GU_COLS), F32),
                pltpu.VMEM((rows, GU_COLS), F32),
                pltpu.VMEM((rows, width), BF16),
                pltpu.VMEM((n_k, most, Y_COLS), F32),
                pltpu.VMEM((n_k, rows, Y_COLS), BF16),
                pltpu.VMEM((n_k, most, Y_COLS), BF16),
                pltpu.VMEM((n_k, most, Y_COLS), BF16),
                pltpu.VMEM((n_k, most, Y_COLS), BF16),
                pltpu.VMEM((n_k, most, Y_COLS), BF16),
                dma,
                dma((n_gu,)),
                dma((n_gu,)),
                dma((n_k,)),
                dma((n_k,)),
                dma((n_k,)),
                dma((n_k,)),
                dma((2, n_k)),
                dma((n_k,)),
                dma((n_k,)),
                dma((n_k,)),
                dma((n_k,)),
            ],
            compiler_params=pltpu.CompilerParams(
                collective_id=0, has_side_effects=True, vmem_limit_bytes=58 * 1024 * 1024
            ),
        )(x, w_gate, w_up, w_down)

    return jax.shard_map(
        step,
        mesh=mesh,
        in_specs=(P("dp", None), P(None, "tp"), P(None, "tp"), P("tp", None)),
        out_specs=P("dp", None),
        check_vma=False,
    )
```

```python
import jax
import jax.numpy as jnp
from jax import lax
from jax.experimental import pallas as pl
from jax.experimental.pallas import tpu as pltpu
from jax.sharding import PartitionSpec as P

MESH = pl.DeviceIdType.MESH
F32, BF16 = jnp.float32, jnp.bfloat16

GU_COLS = 256
GU_PARTS = 4
Y_COLS = 256
ROWS = ((80, 48), (0, 80))
D2D_LAG = 2
IN_START = 8
FIN_LAG = (4, 3)


def kernel(
    x_hbm, wg_hbm, wu_hbm, wd_hbm, y_ref,
    x_v, wg_v, wu_v, wd_v, g_acc, u_acc, hid, own, snd, rcv, part, a_rcv, b_rcv,
    x_sem, wg_sem, wu_sem, wd_sem,
    d_ss, d_rs, p_ss, p_rs, f_ss, f_rs, g_ss, g_rs,
):
    tp = lax.axis_index("tp")
    core = lax.rem(tp, 2)
    z = lax.div(tp, 2)
    sibling = tp + 1 - 2 * core
    inner = jnp.logical_and(z > 0, z < 3)
    outer = jnp.logical_not(inner)
    low = z < 2
    onward = jnp.where(low, tp + 2, tp - 2)
    back = jnp.where(low, tp - 2, tp + 2)

    kd = wg_v.shape[1]
    n_j = wg_v.shape[0] // GU_PARTS
    n_k = wd_v.shape[0]
    barrier = pltpu.get_barrier_semaphore()
    pl.semaphore_signal(barrier, inc=1, device_id={"tp": sibling}, device_id_type=MESH)
    pl.semaphore_signal(barrier, inc=1, device_id={"tp": onward}, device_id_type=MESH)

    @pl.when(inner)
    def _():
        pl.semaphore_signal(barrier, inc=1, device_id={"tp": back}, device_id_type=MESH)

    def ycols(k):
        return pl.ds(pl.multiple_of(k * Y_COLS, Y_COLS), Y_COLS)

    x_copy = pltpu.make_async_copy(x_hbm, x_v, x_sem)

    def gu_copy(hbm, vmem, sem, j, p):
        i = j * GU_PARTS + p
        return pltpu.make_async_copy(
            hbm.at[
                pl.ds(pl.multiple_of(p * kd, kd), kd),
                pl.ds(pl.multiple_of(j * GU_COLS, GU_COLS), GU_COLS),
            ],
            vmem.at[i],
            sem.at[i],
        )

    def wd_copy(k):
        return pltpu.make_async_copy(wd_hbm.at[:, ycols(k)], wd_v.at[k], wd_sem.at[k])

    x_copy.start()

    def start_gu(j, c):
        for p in range(GU_PARTS):
            gu_copy(wg_hbm, wg_v, wg_sem, j, p).start()
            gu_copy(wu_hbm, wu_v, wu_sem, j, p).start()
        return c

    lax.fori_loop(0, n_j, start_gu, 0)

    def start_wd(k, c):
        wd_copy(k).start()
        return c

    lax.fori_loop(0, n_k, start_wd, 0)

    x_copy.wait()

    def gate_up(j, c):
        for p in range(GU_PARTS):
            i = j * GU_PARTS + p
            xs = x_v[:, p * kd : (p + 1) * kd]
            gu_copy(wg_hbm, wg_v, wg_sem, j, p).wait()
            gu_copy(wu_hbm, wu_v, wu_sem, j, p).wait()
            g = jnp.dot(xs, wg_v[i], preferred_element_type=F32)
            u = jnp.dot(xs, wu_v[i], preferred_element_type=F32)
            if p == 0:
                g_acc[...] = g
                u_acc[...] = u
            elif p < GU_PARTS - 1:
                g_acc[...] += g
                u_acc[...] += u
            else:
                g = g_acc[...] + g
                u = u_acc[...] + u
                hid[:, pl.ds(pl.multiple_of(j * GU_COLS, GU_COLS), GU_COLS)] = (
                    jax.nn.silu(g) * u
                ).astype(BF16)
        return c

    lax.fori_loop(0, n_j, gate_up, 0)

    @pl.when(inner)
    def _():
        pl.semaphore_wait(barrier, 3)

    @pl.when(outer)
    def _():
        pl.semaphore_wait(barrier, 2)

    def loop(lo, hi, f):
        def it(k, c):
            f(k)
            return c

        lax.fori_loop(lo, hi, it, 0)

    def remote(src, dst, send, recv, dev):
        return pltpu.make_async_remote_copy(
            src_ref=src, dst_ref=dst, send_sem=send, recv_sem=recv,
            device_id={"tp": dev}, device_id_type=MESH,
        )

    def run(me):
        lo, n = ROWS[me]
        other_lo, other_n = ROWS[1 - me]
        mine, theirs = pl.ds(lo, n), pl.ds(other_lo, other_n)
        top = pl.ds(0, n)
        lag = FIN_LAG[me]

        def give(k):
            return remote(
                snd.at[k, theirs], rcv.at[k, pl.ds(0, other_n)], d_ss.at[k], d_rs.at[k], sibling
            )

        def got(k):
            return remote(snd.at[k, mine], rcv.at[k, top], d_ss.at[k], d_rs.at[k], sibling)

        def to_inner(k):
            return remote(
                part.at[k, top], a_rcv.at[k, top], p_ss.at[k], p_rs.at[0, k], onward
            )

        def across(k):
            return remote(
                part.at[k, top], b_rcv.at[k, top], p_ss.at[k], p_rs.at[1, k], onward
            )

        def to_outer(k):
            y_k = y_ref.at[mine, ycols(k)]
            return remote(y_k, y_k, f_ss.at[k], f_rs.at[k], back)

        def share(k):
            y_k = y_ref.at[mine, ycols(k)]
            return remote(y_k, y_k, g_ss.at[k], g_rs.at[k], sibling)

        def shared(k):
            y_k = y_ref.at[theirs, ycols(k)]
            return remote(y_k, y_k, g_ss.at[k], g_rs.at[k], sibling)

        def term(k):
            wd_copy(k).wait()
            t = jnp.dot(hid[...], wd_v[k], preferred_element_type=F32)
            own[k, top] = t[lo : lo + n]
            snd[k, theirs] = t[other_lo : other_lo + other_n].astype(BF16)
            give(k).start()

        def outer_sum(k):
            got(k).wait_recv()
            part[k, top] = (own[k, top] + rcv[k, top].astype(F32)).astype(BF16)
            to_inner(k).start()

        def inner_sum(k):
            got(k).wait_recv()
            to_inner(k).wait_recv()
            part[k, top] = (
                own[k, top] + rcv[k, top].astype(F32) + a_rcv[k, top].astype(F32)
            ).astype(BF16)
            across(k).start()

        def inner_final(k):
            across(k).wait_recv()
            y_ref[mine, ycols(k)] = (
                part[k, top].astype(F32) + b_rcv[k, top].astype(F32)
            ).astype(BF16)
            to_outer(k).start()
            share(k).start()

        def outer_final(k):
            to_outer(k).wait_recv()
            share(k).start()

        def terms(k):
            term(k)

            @pl.when(jnp.logical_and(outer, k >= D2D_LAG))
            def _():
                outer_sum(k - D2D_LAG)

            @pl.when(jnp.logical_and(inner, k >= IN_START))
            def _():
                inner_sum(k - IN_START)

            @pl.when(jnp.logical_and(inner, k >= IN_START + lag))
            def _():
                inner_final(k - IN_START - lag)

        loop(0, n_k, terms)

        @pl.when(outer)
        def _():
            loop(n_k - D2D_LAG, n_k, outer_sum)
            loop(0, n_k, outer_final)
            loop(0, n_k, lambda k: to_inner(k).wait_send())

        @pl.when(inner)
        def _():
            first = n_k - IN_START
            assert first >= lag

            def both(k):
                inner_sum(k)
                inner_final(k - lag)

            loop(first, n_k, both)
            loop(n_k - lag, n_k, inner_final)

            def sent(k):
                across(k).wait_send()
                to_outer(k).wait_send()

            loop(0, n_k, sent)

        def finish(k):
            give(k).wait_send()
            share(k).wait_send()
            shared(k).wait_recv()

        loop(0, n_k, finish)

    for me in (0, 1):

        @pl.when(core == me)
        def _():
            run(me)


def solution(mesh):
    def step(x, w_gate, w_up, w_down):
        rows, depth = x.shape
        width = w_gate.shape[1]
        out = w_down.shape[1]
        most = max(n for _, n in ROWS)
        n_gu = (width // GU_COLS) * GU_PARTS
        n_k = out // Y_COLS
        kd = depth // GU_PARTS
        dma = pltpu.SemaphoreType.DMA
        return pl.pallas_call(
            kernel,
            out_shape=pltpu.VMEM((rows, out), BF16),
            in_specs=[pl.BlockSpec(memory_space=pl.ANY)] * 4,
            out_specs=pl.BlockSpec(memory_space=pltpu.VMEM),
            scratch_shapes=[
                pltpu.VMEM((rows, depth), BF16),
                pltpu.VMEM((n_gu, kd, GU_COLS), BF16),
                pltpu.VMEM((n_gu, kd, GU_COLS), BF16),
                pltpu.VMEM((n_k, width, Y_COLS), BF16),
                pltpu.VMEM((rows, GU_COLS), F32),
                pltpu.VMEM((rows, GU_COLS), F32),
                pltpu.VMEM((rows, width), BF16),
                pltpu.VMEM((n_k, most, Y_COLS), F32),
                pltpu.VMEM((n_k, rows, Y_COLS), BF16),
                pltpu.VMEM((n_k, most, Y_COLS), BF16),
                pltpu.VMEM((n_k, most, Y_COLS), BF16),
                pltpu.VMEM((n_k, most, Y_COLS), BF16),
                pltpu.VMEM((n_k, most, Y_COLS), BF16),
                dma,
                dma((n_gu,)),
                dma((n_gu,)),
                dma((n_k,)),
                dma((n_k,)),
                dma((n_k,)),
                dma((n_k,)),
                dma((2, n_k)),
                dma((n_k,)),
                dma((n_k,)),
                dma((n_k,)),
                dma((n_k,)),
            ],
            compiler_params=pltpu.CompilerParams(
                collective_id=0, has_side_effects=True, vmem_limit_bytes=58 * 1024 * 1024
            ),
        )(x, w_gate, w_up, w_down)

    return jax.shard_map(
        step,
        mesh=mesh,
        in_specs=(P("dp", None), P(None, "tp"), P(None, "tp"), P("tp", None)),
        out_specs=P("dp", None),
        check_vma=False,
    )
```

```python
import jax
import jax.numpy as jnp
from jax import lax
from jax.experimental import pallas as pl
from jax.experimental.pallas import tpu as pltpu
from jax.sharding import PartitionSpec as P

MESH = pl.DeviceIdType.MESH
F32, BF16 = jnp.float32, jnp.bfloat16

GU_COLS = 256
GU_PARTS = 4
Y_COLS = 256
ROWS = ((80, 48), (0, 80))
D2D_LAG = 2
IN_START = 8
FIN_LAG = ((4, 6), (3, 5))


def kernel(
    x_hbm, wg_hbm, wu_hbm, wd_hbm, y_ref,
    x_v, wg_v, wu_v, wd_v, g_acc, u_acc, hid, own, snd, rcv, part, a_rcv, b_rcv,
    x_sem, wg_sem, wu_sem, wd_sem,
    d_ss, d_rs, p_ss, p_rs, f_ss, f_rs, g_ss, g_rs,
):
    tp = lax.axis_index("tp")
    core = lax.rem(tp, 2)
    z = lax.div(tp, 2)
    sibling = tp + 1 - 2 * core
    inner = jnp.logical_and(z > 0, z < 3)
    outer = jnp.logical_not(inner)
    low = z < 2
    onward = jnp.where(low, tp + 2, tp - 2)
    back = jnp.where(low, tp - 2, tp + 2)

    kd = wg_v.shape[1]
    n_j = wg_v.shape[0] // GU_PARTS
    n_k = wd_v.shape[0]
    barrier = pltpu.get_barrier_semaphore()
    pl.semaphore_signal(barrier, inc=1, device_id={"tp": sibling}, device_id_type=MESH)
    pl.semaphore_signal(barrier, inc=1, device_id={"tp": onward}, device_id_type=MESH)

    @pl.when(inner)
    def _():
        pl.semaphore_signal(barrier, inc=1, device_id={"tp": back}, device_id_type=MESH)

    def ycols(k):
        return pl.ds(pl.multiple_of(k * Y_COLS, Y_COLS), Y_COLS)

    x_copy = pltpu.make_async_copy(x_hbm, x_v, x_sem)

    def gu_copy(hbm, vmem, sem, j, p):
        i = j * GU_PARTS + p
        return pltpu.make_async_copy(
            hbm.at[
                pl.ds(pl.multiple_of(p * kd, kd), kd),
                pl.ds(pl.multiple_of(j * GU_COLS, GU_COLS), GU_COLS),
            ],
            vmem.at[i],
            sem.at[i],
        )

    def wd_copy(k):
        return pltpu.make_async_copy(wd_hbm.at[:, ycols(k)], wd_v.at[k], wd_sem.at[k])

    x_copy.start()

    def start_gu(j, c):
        for p in range(GU_PARTS):
            gu_copy(wg_hbm, wg_v, wg_sem, j, p).start()
            gu_copy(wu_hbm, wu_v, wu_sem, j, p).start()
        return c

    lax.fori_loop(0, n_j, start_gu, 0)

    def start_wd(k, c):
        wd_copy(k).start()
        return c

    lax.fori_loop(0, n_k, start_wd, 0)

    x_copy.wait()

    def gate_up(j, c):
        for p in range(GU_PARTS):
            i = j * GU_PARTS + p
            xs = x_v[:, p * kd : (p + 1) * kd]
            gu_copy(wg_hbm, wg_v, wg_sem, j, p).wait()
            gu_copy(wu_hbm, wu_v, wu_sem, j, p).wait()
            g = jnp.dot(xs, wg_v[i], preferred_element_type=F32)
            u = jnp.dot(xs, wu_v[i], preferred_element_type=F32)
            if p == 0:
                g_acc[...] = g
                u_acc[...] = u
            elif p < GU_PARTS - 1:
                g_acc[...] += g
                u_acc[...] += u
            else:
                g = g_acc[...] + g
                u = u_acc[...] + u
                hid[:, pl.ds(pl.multiple_of(j * GU_COLS, GU_COLS), GU_COLS)] = (
                    jax.nn.silu(g) * u
                ).astype(BF16)
        return c

    lax.fori_loop(0, n_j, gate_up, 0)

    @pl.when(inner)
    def _():
        pl.semaphore_wait(barrier, 3)

    @pl.when(outer)
    def _():
        pl.semaphore_wait(barrier, 2)

    def loop(lo, hi, f):
        def it(k, c):
            f(k)
            return c

        lax.fori_loop(lo, hi, it, 0)

    def remote(src, dst, send, recv, dev):
        return pltpu.make_async_remote_copy(
            src_ref=src, dst_ref=dst, send_sem=send, recv_sem=recv,
            device_id={"tp": dev}, device_id_type=MESH,
        )

    def run(me):
        lo, n = ROWS[me]
        other_lo, other_n = ROWS[1 - me]
        mine, theirs = pl.ds(lo, n), pl.ds(other_lo, other_n)
        top = pl.ds(0, n)
        lag = jnp.where(low, *FIN_LAG[me])

        def give(k):
            return remote(
                snd.at[k, theirs], rcv.at[k, pl.ds(0, other_n)], d_ss.at[k], d_rs.at[k], sibling
            )

        def got(k):
            return remote(snd.at[k, mine], rcv.at[k, top], d_ss.at[k], d_rs.at[k], sibling)

        def to_inner(k):
            return remote(
                part.at[k, top], a_rcv.at[k, top], p_ss.at[k], p_rs.at[0, k], onward
            )

        def across(k):
            return remote(
                part.at[k, top], b_rcv.at[k, top], p_ss.at[k], p_rs.at[1, k], onward
            )

        def to_outer(k):
            y_k = y_ref.at[mine, ycols(k)]
            return remote(y_k, y_k, f_ss.at[k], f_rs.at[k], back)

        def share(k):
            y_k = y_ref.at[mine, ycols(k)]
            return remote(y_k, y_k, g_ss.at[k], g_rs.at[k], sibling)

        def shared(k):
            y_k = y_ref.at[theirs, ycols(k)]
            return remote(y_k, y_k, g_ss.at[k], g_rs.at[k], sibling)

        def term(k):
            wd_copy(k).wait()
            t = jnp.dot(hid[...], wd_v[k], preferred_element_type=F32)
            own[k, top] = t[lo : lo + n]
            snd[k, theirs] = t[other_lo : other_lo + other_n].astype(BF16)
            give(k).start()

        def outer_sum(k):
            got(k).wait_recv()
            part[k, top] = (own[k, top] + rcv[k, top].astype(F32)).astype(BF16)
            to_inner(k).start()

        def inner_sum(k):
            got(k).wait_recv()
            to_inner(k).wait_recv()
            part[k, top] = (
                own[k, top] + rcv[k, top].astype(F32) + a_rcv[k, top].astype(F32)
            ).astype(BF16)
            across(k).start()

        def inner_final(k):
            across(k).wait_recv()
            y_ref[mine, ycols(k)] = (
                part[k, top].astype(F32) + b_rcv[k, top].astype(F32)
            ).astype(BF16)
            to_outer(k).start()
            share(k).start()

        def outer_final(k):
            to_outer(k).wait_recv()
            share(k).start()

        def terms(k):
            term(k)

            @pl.when(jnp.logical_and(outer, k >= D2D_LAG))
            def _():
                outer_sum(k - D2D_LAG)

            @pl.when(jnp.logical_and(inner, k >= IN_START))
            def _():
                inner_sum(k - IN_START)

            @pl.when(jnp.logical_and(inner, k >= IN_START + lag))
            def _():
                inner_final(k - IN_START - lag)

        loop(0, n_k, terms)

        @pl.when(outer)
        def _():
            loop(n_k - D2D_LAG, n_k, outer_sum)
            loop(0, n_k, outer_final)
            loop(0, n_k, lambda k: to_inner(k).wait_send())

        @pl.when(inner)
        def _():
            first = n_k - IN_START
            assert first >= max(FIN_LAG[me])

            def both(k):
                inner_sum(k)
                inner_final(k - lag)

            loop(first, n_k, both)
            loop(n_k - lag, n_k, inner_final)

            def sent(k):
                across(k).wait_send()
                to_outer(k).wait_send()

            loop(0, n_k, sent)

        def finish(k):
            give(k).wait_send()
            share(k).wait_send()
            shared(k).wait_recv()

        loop(0, n_k, finish)

    for me in (0, 1):

        @pl.when(core == me)
        def _():
            run(me)


def solution(mesh):
    def step(x, w_gate, w_up, w_down):
        rows, depth = x.shape
        width = w_gate.shape[1]
        out = w_down.shape[1]
        most = max(n for _, n in ROWS)
        n_gu = (width // GU_COLS) * GU_PARTS
        n_k = out // Y_COLS
        kd = depth // GU_PARTS
        dma = pltpu.SemaphoreType.DMA
        return pl.pallas_call(
            kernel,
            out_shape=pltpu.VMEM((rows, out), BF16),
            in_specs=[pl.BlockSpec(memory_space=pl.ANY)] * 4,
            out_specs=pl.BlockSpec(memory_space=pltpu.VMEM),
            scratch_shapes=[
                pltpu.VMEM((rows, depth), BF16),
                pltpu.VMEM((n_gu, kd, GU_COLS), BF16),
                pltpu.VMEM((n_gu, kd, GU_COLS), BF16),
                pltpu.VMEM((n_k, width, Y_COLS), BF16),
                pltpu.VMEM((rows, GU_COLS), F32),
                pltpu.VMEM((rows, GU_COLS), F32),
                pltpu.VMEM((rows, width), BF16),
                pltpu.VMEM((n_k, most, Y_COLS), F32),
                pltpu.VMEM((n_k, rows, Y_COLS), BF16),
                pltpu.VMEM((n_k, most, Y_COLS), BF16),
                pltpu.VMEM((n_k, most, Y_COLS), BF16),
                pltpu.VMEM((n_k, most, Y_COLS), BF16),
                pltpu.VMEM((n_k, most, Y_COLS), BF16),
                dma,
                dma((n_gu,)),
                dma((n_gu,)),
                dma((n_k,)),
                dma((n_k,)),
                dma((n_k,)),
                dma((n_k,)),
                dma((2, n_k)),
                dma((n_k,)),
                dma((n_k,)),
                dma((n_k,)),
                dma((n_k,)),
            ],
            compiler_params=pltpu.CompilerParams(
                collective_id=0, has_side_effects=True, vmem_limit_bytes=58 * 1024 * 1024
            ),
        )(x, w_gate, w_up, w_down)

    return jax.shard_map(
        step,
        mesh=mesh,
        in_specs=(P("dp", None), P(None, "tp"), P(None, "tp"), P("tp", None)),
        out_specs=P("dp", None),
        check_vma=False,
    )
```

```python
import jax
import jax.numpy as jnp
from jax import lax
from jax.experimental import pallas as pl
from jax.experimental.pallas import tpu as pltpu
from jax.sharding import PartitionSpec as P

MESH = pl.DeviceIdType.MESH
F32, BF16 = jnp.float32, jnp.bfloat16

GU_COLS = 256
GU_PARTS = 4
Y_COLS = 256
ROWS = ((0, 80), (80, 48))
D2D_LAG = 2
IN_START = 8
FIN_LAG = 5


def kernel(
    x_hbm, wg_hbm, wu_hbm, wd_hbm, y_ref,
    x_v, wg_v, wu_v, wd_v, g_acc, u_acc, hid, own, snd, rcv, part, a_rcv, b_rcv,
    x_sem, wg_sem, wu_sem, wd_sem,
    d_ss, d_rs, p_ss, p_rs, f_ss, f_rs, g_ss, g_rs,
):
    tp = lax.axis_index("tp")
    core = lax.rem(tp, 2)
    z = lax.div(tp, 2)
    sibling = tp + 1 - 2 * core
    inner = jnp.logical_and(z > 0, z < 3)
    outer = jnp.logical_not(inner)
    low = z < 2
    onward = jnp.where(low, tp + 2, tp - 2)
    back = jnp.where(low, tp - 2, tp + 2)

    kd = wg_v.shape[1]
    n_j = wg_v.shape[0] // GU_PARTS
    n_k = wd_v.shape[0]
    barrier = pltpu.get_barrier_semaphore()
    pl.semaphore_signal(barrier, inc=1, device_id={"tp": sibling}, device_id_type=MESH)
    pl.semaphore_signal(barrier, inc=1, device_id={"tp": onward}, device_id_type=MESH)

    @pl.when(inner)
    def _():
        pl.semaphore_signal(barrier, inc=1, device_id={"tp": back}, device_id_type=MESH)

    def ycols(k):
        return pl.ds(pl.multiple_of(k * Y_COLS, Y_COLS), Y_COLS)

    x_copy = pltpu.make_async_copy(x_hbm, x_v, x_sem)

    def gu_copy(hbm, vmem, sem, j, p):
        i = j * GU_PARTS + p
        return pltpu.make_async_copy(
            hbm.at[
                pl.ds(pl.multiple_of(p * kd, kd), kd),
                pl.ds(pl.multiple_of(j * GU_COLS, GU_COLS), GU_COLS),
            ],
            vmem.at[i],
            sem.at[i],
        )

    def wd_copy(k):
        return pltpu.make_async_copy(wd_hbm.at[:, ycols(k)], wd_v.at[k], wd_sem.at[k])

    x_copy.start()

    def start_gu(j, c):
        for p in range(GU_PARTS):
            gu_copy(wg_hbm, wg_v, wg_sem, j, p).start()
            gu_copy(wu_hbm, wu_v, wu_sem, j, p).start()
        return c

    lax.fori_loop(0, n_j, start_gu, 0)

    def start_wd(k, c):
        wd_copy(k).start()
        return c

    lax.fori_loop(0, n_k, start_wd, 0)

    x_copy.wait()

    def gate_up(j, c):
        for p in range(GU_PARTS):
            i = j * GU_PARTS + p
            xs = x_v[:, p * kd : (p + 1) * kd]
            gu_copy(wg_hbm, wg_v, wg_sem, j, p).wait()
            gu_copy(wu_hbm, wu_v, wu_sem, j, p).wait()
            g = jnp.dot(xs, wg_v[i], preferred_element_type=F32)
            u = jnp.dot(xs, wu_v[i], preferred_element_type=F32)
            if p == 0:
                g_acc[...] = g
                u_acc[...] = u
            elif p < GU_PARTS - 1:
                g_acc[...] += g
                u_acc[...] += u
            else:
                g = g_acc[...] + g
                u = u_acc[...] + u
                hid[:, pl.ds(pl.multiple_of(j * GU_COLS, GU_COLS), GU_COLS)] = (
                    jax.nn.silu(g) * u
                ).astype(BF16)
        return c

    lax.fori_loop(0, n_j, gate_up, 0)

    @pl.when(inner)
    def _():
        pl.semaphore_wait(barrier, 3)

    @pl.when(outer)
    def _():
        pl.semaphore_wait(barrier, 2)

    def loop(lo, hi, f):
        def it(k, c):
            f(k)
            return c

        lax.fori_loop(lo, hi, it, 0)

    def remote(src, dst, send, recv, dev):
        return pltpu.make_async_remote_copy(
            src_ref=src, dst_ref=dst, send_sem=send, recv_sem=recv,
            device_id={"tp": dev}, device_id_type=MESH,
        )

    def run(me):
        lo, n = ROWS[me]
        other_lo, other_n = ROWS[1 - me]
        mine, theirs = pl.ds(lo, n), pl.ds(other_lo, other_n)
        top = pl.ds(0, n)

        def give(k):
            return remote(
                snd.at[k, theirs], rcv.at[k, pl.ds(0, other_n)], d_ss.at[k], d_rs.at[k], sibling
            )

        def got(k):
            return remote(snd.at[k, mine], rcv.at[k, top], d_ss.at[k], d_rs.at[k], sibling)

        def to_inner(k):
            return remote(
                part.at[k, top], a_rcv.at[k, top], p_ss.at[k], p_rs.at[0, k], onward
            )

        def across(k):
            return remote(
                part.at[k, top], b_rcv.at[k, top], p_ss.at[k], p_rs.at[1, k], onward
            )

        def to_outer(k):
            y_k = y_ref.at[mine, ycols(k)]
            return remote(y_k, y_k, f_ss.at[k], f_rs.at[k], back)

        def share(k):
            y_k = y_ref.at[mine, ycols(k)]
            return remote(y_k, y_k, g_ss.at[k], g_rs.at[k], sibling)

        def shared(k):
            y_k = y_ref.at[theirs, ycols(k)]
            return remote(y_k, y_k, g_ss.at[k], g_rs.at[k], sibling)

        def term(k):
            wd_copy(k).wait()
            t = jnp.dot(hid[...], wd_v[k], preferred_element_type=F32)
            own[k, top] = t[lo : lo + n]
            snd[k, theirs] = t[other_lo : other_lo + other_n].astype(BF16)
            give(k).start()

        def outer_sum(k):
            got(k).wait_recv()
            part[k, top] = (own[k, top] + rcv[k, top].astype(F32)).astype(BF16)
            to_inner(k).start()

        def inner_sum(k):
            got(k).wait_recv()
            to_inner(k).wait_recv()
            part[k, top] = (
                own[k, top] + rcv[k, top].astype(F32) + a_rcv[k, top].astype(F32)
            ).astype(BF16)
            across(k).start()

        def inner_final(k):
            across(k).wait_recv()
            y_ref[mine, ycols(k)] = (
                part[k, top].astype(F32) + b_rcv[k, top].astype(F32)
            ).astype(BF16)
            to_outer(k).start()
            share(k).start()

        def outer_final(k):
            to_outer(k).wait_recv()
            share(k).start()

        def terms(k):
            term(k)

            @pl.when(jnp.logical_and(outer, k >= D2D_LAG))
            def _():
                outer_sum(k - D2D_LAG)

            @pl.when(jnp.logical_and(inner, k >= IN_START))
            def _():
                inner_sum(k - IN_START)

            @pl.when(jnp.logical_and(inner, k >= IN_START + FIN_LAG))
            def _():
                inner_final(k - IN_START - FIN_LAG)

        loop(0, n_k, terms)

        @pl.when(outer)
        def _():
            loop(n_k - D2D_LAG, n_k, outer_sum)
            loop(0, n_k, outer_final)
            loop(0, n_k, lambda k: to_inner(k).wait_send())

        @pl.when(inner)
        def _():
            first = n_k - IN_START
            assert first >= FIN_LAG

            def both(k):
                inner_sum(k)
                inner_final(k - FIN_LAG)

            loop(first, n_k, both)
            loop(n_k - FIN_LAG, n_k, inner_final)

            def sent(k):
                across(k).wait_send()
                to_outer(k).wait_send()

            loop(0, n_k, sent)

        def finish(k):
            give(k).wait_send()
            share(k).wait_send()
            shared(k).wait_recv()

        loop(0, n_k, finish)

    for me in (0, 1):

        @pl.when(core == me)
        def _():
            run(me)


def solution(mesh):
    def step(x, w_gate, w_up, w_down):
        rows, depth = x.shape
        width = w_gate.shape[1]
        out = w_down.shape[1]
        most = max(n for _, n in ROWS)
        n_gu = (width // GU_COLS) * GU_PARTS
        n_k = out // Y_COLS
        kd = depth // GU_PARTS
        dma = pltpu.SemaphoreType.DMA
        return pl.pallas_call(
            kernel,
            out_shape=pltpu.VMEM((rows, out), BF16),
            in_specs=[pl.BlockSpec(memory_space=pl.ANY)] * 4,
            out_specs=pl.BlockSpec(memory_space=pltpu.VMEM),
            scratch_shapes=[
                pltpu.VMEM((rows, depth), BF16),
                pltpu.VMEM((n_gu, kd, GU_COLS), BF16),
                pltpu.VMEM((n_gu, kd, GU_COLS), BF16),
                pltpu.VMEM((n_k, width, Y_COLS), BF16),
                pltpu.VMEM((rows, GU_COLS), F32),
                pltpu.VMEM((rows, GU_COLS), F32),
                pltpu.VMEM((rows, width), BF16),
                pltpu.VMEM((n_k, most, Y_COLS), F32),
                pltpu.VMEM((n_k, rows, Y_COLS), BF16),
                pltpu.VMEM((n_k, most, Y_COLS), BF16),
                pltpu.VMEM((n_k, most, Y_COLS), BF16),
                pltpu.VMEM((n_k, most, Y_COLS), BF16),
                pltpu.VMEM((n_k, most, Y_COLS), BF16),
                dma,
                dma((n_gu,)),
                dma((n_gu,)),
                dma((n_k,)),
                dma((n_k,)),
                dma((n_k,)),
                dma((n_k,)),
                dma((2, n_k)),
                dma((n_k,)),
                dma((n_k,)),
                dma((n_k,)),
                dma((n_k,)),
            ],
            compiler_params=pltpu.CompilerParams(
                collective_id=0, has_side_effects=True, vmem_limit_bytes=58 * 1024 * 1024
            ),
        )(x, w_gate, w_up, w_down)

    return jax.shard_map(
        step,
        mesh=mesh,
        in_specs=(P("dp", None), P(None, "tp"), P(None, "tp"), P("tp", None)),
        out_specs=P("dp", None),
        check_vma=False,
    )
```

```python
import jax
import jax.numpy as jnp
from jax import lax
from jax.experimental import pallas as pl
from jax.experimental.pallas import tpu as pltpu
from jax.sharding import PartitionSpec as P

MESH = pl.DeviceIdType.MESH
F32, BF16 = jnp.float32, jnp.bfloat16

GU_COLS = 256
GU_PARTS = 4
Y_COLS = 256
ROWS = ((80, 48), (0, 80))
FAR = 2
D2D_LAG = 2
IN_START = 8
FIN_LAG = 5


def kernel(
    x_hbm, wg_hbm, wu_hbm, wd_hbm, y_ref,
    x_v, wg_v, wu_v, wd_v, g_acc, u_acc, hid, own, snd, rcv, part, a_rcv, b_rcv,
    x_sem, wg_sem, wu_sem, wd_sem,
    d_ss, d_rs, p_ss, p_rs, f_ss, f_rs, g_ss, g_rs, t_ss,
):
    tp = lax.axis_index("tp")
    core = lax.rem(tp, 2)
    z = lax.div(tp, 2)
    sibling = tp + 1 - 2 * core
    inner = jnp.logical_and(z > 0, z < 3)
    outer = jnp.logical_not(inner)
    low = z < 2
    onward = jnp.where(low, tp + 2, tp - 2)
    back = jnp.where(low, tp - 2, tp + 2)

    kd = wg_v.shape[1]
    n_j = wg_v.shape[0] // GU_PARTS
    n_k = wd_v.shape[0]
    barrier = pltpu.get_barrier_semaphore()
    pl.semaphore_signal(barrier, inc=1, device_id={"tp": sibling}, device_id_type=MESH)
    pl.semaphore_signal(barrier, inc=1, device_id={"tp": onward}, device_id_type=MESH)

    @pl.when(inner)
    def _():
        pl.semaphore_signal(barrier, inc=1, device_id={"tp": back}, device_id_type=MESH)

    far = jnp.where(low, tp + 4, tp - 4)
    met = lax.rem(z, 2) == 0

    @pl.when(met)
    def _():
        pl.semaphore_signal(barrier, inc=1, device_id={"tp": far}, device_id_type=MESH)

    def ycols(k):
        return pl.ds(pl.multiple_of(k * Y_COLS, Y_COLS), Y_COLS)

    x_copy = pltpu.make_async_copy(x_hbm, x_v, x_sem)

    def gu_copy(hbm, vmem, sem, j, p):
        i = j * GU_PARTS + p
        return pltpu.make_async_copy(
            hbm.at[
                pl.ds(pl.multiple_of(p * kd, kd), kd),
                pl.ds(pl.multiple_of(j * GU_COLS, GU_COLS), GU_COLS),
            ],
            vmem.at[i],
            sem.at[i],
        )

    def wd_copy(k):
        return pltpu.make_async_copy(wd_hbm.at[:, ycols(k)], wd_v.at[k], wd_sem.at[k])

    x_copy.start()

    def start_gu(j, c):
        for p in range(GU_PARTS):
            gu_copy(wg_hbm, wg_v, wg_sem, j, p).start()
            gu_copy(wu_hbm, wu_v, wu_sem, j, p).start()
        return c

    lax.fori_loop(0, n_j, start_gu, 0)

    def start_wd(k, c):
        wd_copy(k).start()
        return c

    lax.fori_loop(0, n_k, start_wd, 0)

    x_copy.wait()

    def gate_up(j, c):
        for p in range(GU_PARTS):
            i = j * GU_PARTS + p
            xs = x_v[:, p * kd : (p + 1) * kd]
            gu_copy(wg_hbm, wg_v, wg_sem, j, p).wait()
            gu_copy(wu_hbm, wu_v, wu_sem, j, p).wait()
            g = jnp.dot(xs, wg_v[i], preferred_element_type=F32)
            u = jnp.dot(xs, wu_v[i], preferred_element_type=F32)
            if p == 0:
                g_acc[...] = g
                u_acc[...] = u
            elif p < GU_PARTS - 1:
                g_acc[...] += g
                u_acc[...] += u
            else:
                g = g_acc[...] + g
                u = u_acc[...] + u
                hid[:, pl.ds(pl.multiple_of(j * GU_COLS, GU_COLS), GU_COLS)] = (
                    jax.nn.silu(g) * u
                ).astype(BF16)
        return c

    lax.fori_loop(0, n_j, gate_up, 0)

    for place, others in enumerate((3, 3, 4, 2)):

        @pl.when(z == place)
        def _():
            pl.semaphore_wait(barrier, others)

    def loop(lo, hi, f):
        def it(k, c):
            f(k)
            return c

        lax.fori_loop(lo, hi, it, 0)

    def remote(src, dst, send, recv, dev):
        return pltpu.make_async_remote_copy(
            src_ref=src, dst_ref=dst, send_sem=send, recv_sem=recv,
            device_id={"tp": dev}, device_id_type=MESH,
        )

    def run(me):
        lo, n = ROWS[me]
        other_lo, other_n = ROWS[1 - me]
        mine, theirs = pl.ds(lo, n), pl.ds(other_lo, other_n)
        top = pl.ds(0, n)

        def give(k):
            return remote(
                snd.at[k, theirs], rcv.at[k, pl.ds(0, other_n)], d_ss.at[k], d_rs.at[k], sibling
            )

        def got(k):
            return remote(snd.at[k, mine], rcv.at[k, top], d_ss.at[k], d_rs.at[k], sibling)

        def to_inner(k):
            return remote(
                part.at[k, top], a_rcv.at[k, top], p_ss.at[k], p_rs.at[0, k], onward
            )

        def across(k):
            return remote(
                part.at[k, top], b_rcv.at[k, top], p_ss.at[k], p_rs.at[1, k], onward
            )

        def straight(k):
            return remote(part.at[k, top], b_rcv.at[k, top], t_ss.at[k], p_rs.at[1, k], far)

        def half_out(k):
            return remote(part.at[k, top], a_rcv.at[k, top], t_ss.at[k], p_rs.at[0, k], back)

        def to_outer(k):
            y_k = y_ref.at[mine, ycols(k)]
            return remote(y_k, y_k, f_ss.at[k], f_rs.at[k], back)

        def share(k):
            y_k = y_ref.at[mine, ycols(k)]
            return remote(y_k, y_k, g_ss.at[k], g_rs.at[k], sibling)

        def shared(k):
            y_k = y_ref.at[theirs, ycols(k)]
            return remote(y_k, y_k, g_ss.at[k], g_rs.at[k], sibling)

        def term(k):
            wd_copy(k).wait()
            t = jnp.dot(hid[...], wd_v[k], preferred_element_type=F32)
            own[k, top] = t[lo : lo + n]
            snd[k, theirs] = t[other_lo : other_lo + other_n].astype(BF16)
            give(k).start()

        def outer_sum(k):
            got(k).wait_recv()
            part[k, top] = (own[k, top] + rcv[k, top].astype(F32)).astype(BF16)
            to_inner(k).start()

        def inner_sum(k):
            got(k).wait_recv()
            to_inner(k).wait_recv()
            part[k, top] = (
                own[k, top] + rcv[k, top].astype(F32) + a_rcv[k, top].astype(F32)
            ).astype(BF16)
            late = k >= n_k - FAR

            @pl.when(jnp.logical_and(late, z == 2))
            def _():
                straight(k).start()

            across(k).start()

            @pl.when(jnp.logical_and(late, z == 1))
            def _():
                half_out(k).start()

        def inner_final(k):
            across(k).wait_recv()
            y_ref[mine, ycols(k)] = (
                part[k, top].astype(F32) + b_rcv[k, top].astype(F32)
            ).astype(BF16)

            @pl.when(jnp.logical_or(k < n_k - FAR, z == 2))
            def _():
                to_outer(k).start()

            share(k).start()

        def outer_final(k):
            to_outer(k).wait_recv()
            share(k).start()

        def last_final(k):
            half_out(k).wait_recv()
            straight(k).wait_recv()
            y_ref[mine, ycols(k)] = (
                a_rcv[k, top].astype(F32) + b_rcv[k, top].astype(F32)
            ).astype(BF16)
            share(k).start()

        def terms(k):
            term(k)

            @pl.when(jnp.logical_and(outer, k >= D2D_LAG))
            def _():
                outer_sum(k - D2D_LAG)

            @pl.when(jnp.logical_and(inner, k >= IN_START))
            def _():
                inner_sum(k - IN_START)

            @pl.when(jnp.logical_and(inner, k >= IN_START + FIN_LAG))
            def _():
                inner_final(k - IN_START - FIN_LAG)

        loop(0, n_k, terms)

        @pl.when(outer)
        def _():
            loop(n_k - D2D_LAG, n_k, outer_sum)
            ends = jnp.where(z == 0, n_k - FAR, n_k)
            loop(0, ends, outer_final)
            loop(ends, n_k, last_final)
            loop(0, n_k, lambda k: to_inner(k).wait_send())

        @pl.when(inner)
        def _():
            first = n_k - IN_START
            assert first >= FIN_LAG

            def both(k):
                inner_sum(k)
                inner_final(k - FIN_LAG)

            loop(first, n_k, both)
            loop(n_k - FIN_LAG, n_k, inner_final)

            def sent(k):
                across(k).wait_send()
                late = k >= n_k - FAR

                @pl.when(late)
                def _():
                    straight(k).wait_send()

                @pl.when(jnp.logical_or(jnp.logical_not(late), z == 2))
                def _():
                    to_outer(k).wait_send()

            loop(0, n_k, sent)

        def finish(k):
            give(k).wait_send()
            share(k).wait_send()
            shared(k).wait_recv()

        loop(0, n_k, finish)

    for me in (0, 1):

        @pl.when(core == me)
        def _():
            run(me)


def solution(mesh):
    def step(x, w_gate, w_up, w_down):
        rows, depth = x.shape
        width = w_gate.shape[1]
        out = w_down.shape[1]
        most = max(n for _, n in ROWS)
        n_gu = (width // GU_COLS) * GU_PARTS
        n_k = out // Y_COLS
        kd = depth // GU_PARTS
        dma = pltpu.SemaphoreType.DMA
        return pl.pallas_call(
            kernel,
            out_shape=pltpu.VMEM((rows, out), BF16),
            in_specs=[pl.BlockSpec(memory_space=pl.ANY)] * 4,
            out_specs=pl.BlockSpec(memory_space=pltpu.VMEM),
            scratch_shapes=[
                pltpu.VMEM((rows, depth), BF16),
                pltpu.VMEM((n_gu, kd, GU_COLS), BF16),
                pltpu.VMEM((n_gu, kd, GU_COLS), BF16),
                pltpu.VMEM((n_k, width, Y_COLS), BF16),
                pltpu.VMEM((rows, GU_COLS), F32),
                pltpu.VMEM((rows, GU_COLS), F32),
                pltpu.VMEM((rows, width), BF16),
                pltpu.VMEM((n_k, most, Y_COLS), F32),
                pltpu.VMEM((n_k, rows, Y_COLS), BF16),
                pltpu.VMEM((n_k, most, Y_COLS), BF16),
                pltpu.VMEM((n_k, most, Y_COLS), BF16),
                pltpu.VMEM((n_k, most, Y_COLS), BF16),
                pltpu.VMEM((n_k, most, Y_COLS), BF16),
                dma,
                dma((n_gu,)),
                dma((n_gu,)),
                dma((n_k,)),
                dma((n_k,)),
                dma((n_k,)),
                dma((n_k,)),
                dma((2, n_k)),
                dma((n_k,)),
                dma((n_k,)),
                dma((n_k,)),
                dma((n_k,)),
                dma((n_k,)),
            ],
            compiler_params=pltpu.CompilerParams(
                collective_id=0, has_side_effects=True, vmem_limit_bytes=58 * 1024 * 1024
            ),
        )(x, w_gate, w_up, w_down)

    return jax.shard_map(
        step,
        mesh=mesh,
        in_specs=(P("dp", None), P(None, "tp"), P(None, "tp"), P("tp", None)),
        out_specs=P("dp", None),
        check_vma=False,
    )
```

```python
import jax
import jax.numpy as jnp
from jax import lax
from jax.experimental import pallas as pl
from jax.experimental.pallas import tpu as pltpu
from jax.sharding import PartitionSpec as P

MESH = pl.DeviceIdType.MESH
F32, BF16 = jnp.float32, jnp.bfloat16

GU_COLS = 256
GU_PARTS = 4
Y_COLS = 256
ROWS = ((72, 56), (0, 72))
D2D_LAG = 2
IN_START = 8
FIN_LAG = 5


def kernel(
    x_hbm, wg_hbm, wu_hbm, wd_hbm, y_ref,
    x_v, wg_v, wu_v, wd_v, g_acc, u_acc, hid, own, snd, rcv, part, a_rcv, b_rcv,
    x_sem, wg_sem, wu_sem, wd_sem,
    d_ss, d_rs, p_ss, p_rs, f_ss, f_rs, g_ss, g_rs,
):
    tp = lax.axis_index("tp")
    core = lax.rem(tp, 2)
    z = lax.div(tp, 2)
    sibling = tp + 1 - 2 * core
    inner = jnp.logical_and(z > 0, z < 3)
    outer = jnp.logical_not(inner)
    low = z < 2
    onward = jnp.where(low, tp + 2, tp - 2)
    back = jnp.where(low, tp - 2, tp + 2)

    kd = wg_v.shape[1]
    n_j = wg_v.shape[0] // GU_PARTS
    n_k = wd_v.shape[0]
    barrier = pltpu.get_barrier_semaphore()
    pl.semaphore_signal(barrier, inc=1, device_id={"tp": sibling}, device_id_type=MESH)
    pl.semaphore_signal(barrier, inc=1, device_id={"tp": onward}, device_id_type=MESH)

    @pl.when(inner)
    def _():
        pl.semaphore_signal(barrier, inc=1, device_id={"tp": back}, device_id_type=MESH)

    def ycols(k):
        return pl.ds(pl.multiple_of(k * Y_COLS, Y_COLS), Y_COLS)

    x_copy = pltpu.make_async_copy(x_hbm, x_v, x_sem)

    def gu_copy(hbm, vmem, sem, j, p):
        i = j * GU_PARTS + p
        return pltpu.make_async_copy(
            hbm.at[
                pl.ds(pl.multiple_of(p * kd, kd), kd),
                pl.ds(pl.multiple_of(j * GU_COLS, GU_COLS), GU_COLS),
            ],
            vmem.at[i],
            sem.at[i],
        )

    def wd_copy(k):
        return pltpu.make_async_copy(wd_hbm.at[:, ycols(k)], wd_v.at[k], wd_sem.at[k])

    x_copy.start()

    def start_gu(j, c):
        for p in range(GU_PARTS):
            gu_copy(wg_hbm, wg_v, wg_sem, j, p).start()
            gu_copy(wu_hbm, wu_v, wu_sem, j, p).start()
        return c

    lax.fori_loop(0, n_j, start_gu, 0)

    def start_wd(k, c):
        wd_copy(k).start()
        return c

    lax.fori_loop(0, n_k, start_wd, 0)

    x_copy.wait()

    def gate_up(j, c):
        for p in range(GU_PARTS):
            i = j * GU_PARTS + p
            xs = x_v[:, p * kd : (p + 1) * kd]
            gu_copy(wg_hbm, wg_v, wg_sem, j, p).wait()
            gu_copy(wu_hbm, wu_v, wu_sem, j, p).wait()
            g = jnp.dot(xs, wg_v[i], preferred_element_type=F32)
            u = jnp.dot(xs, wu_v[i], preferred_element_type=F32)
            if p == 0:
                g_acc[...] = g
                u_acc[...] = u
            elif p < GU_PARTS - 1:
                g_acc[...] += g
                u_acc[...] += u
            else:
                g = g_acc[...] + g
                u = u_acc[...] + u
                hid[:, pl.ds(pl.multiple_of(j * GU_COLS, GU_COLS), GU_COLS)] = (
                    jax.nn.silu(g) * u
                ).astype(BF16)
        return c

    lax.fori_loop(0, n_j, gate_up, 0)

    @pl.when(inner)
    def _():
        pl.semaphore_wait(barrier, 3)

    @pl.when(outer)
    def _():
        pl.semaphore_wait(barrier, 2)

    def loop(lo, hi, f):
        def it(k, c):
            f(k)
            return c

        lax.fori_loop(lo, hi, it, 0)

    def remote(src, dst, send, recv, dev):
        return pltpu.make_async_remote_copy(
            src_ref=src, dst_ref=dst, send_sem=send, recv_sem=recv,
            device_id={"tp": dev}, device_id_type=MESH,
        )

    def run(me):
        lo, n = ROWS[me]
        other_lo, other_n = ROWS[1 - me]
        mine, theirs = pl.ds(lo, n), pl.ds(other_lo, other_n)
        top = pl.ds(0, n)

        def give(k):
            return remote(
                snd.at[k, theirs], rcv.at[k, pl.ds(0, other_n)], d_ss.at[k], d_rs.at[k], sibling
            )

        def got(k):
            return remote(snd.at[k, mine], rcv.at[k, top], d_ss.at[k], d_rs.at[k], sibling)

        def to_inner(k):
            return remote(
                part.at[k, top], a_rcv.at[k, top], p_ss.at[k], p_rs.at[0, k], onward
            )

        def across(k):
            return remote(
                part.at[k, top], b_rcv.at[k, top], p_ss.at[k], p_rs.at[1, k], onward
            )

        def to_outer(k):
            y_k = y_ref.at[mine, ycols(k)]
            return remote(y_k, y_k, f_ss.at[k], f_rs.at[k], back)

        def share(k):
            y_k = y_ref.at[mine, ycols(k)]
            return remote(y_k, y_k, g_ss.at[k], g_rs.at[k], sibling)

        def shared(k):
            y_k = y_ref.at[theirs, ycols(k)]
            return remote(y_k, y_k, g_ss.at[k], g_rs.at[k], sibling)

        def term(k):
            wd_copy(k).wait()
            t = jnp.dot(hid[...], wd_v[k], preferred_element_type=F32)
            own[k, top] = t[lo : lo + n]
            snd[k, theirs] = t[other_lo : other_lo + other_n].astype(BF16)
            give(k).start()

        def outer_sum(k):
            got(k).wait_recv()
            part[k, top] = (own[k, top] + rcv[k, top].astype(F32)).astype(BF16)
            to_inner(k).start()

        def inner_sum(k):
            got(k).wait_recv()
            to_inner(k).wait_recv()
            part[k, top] = (
                own[k, top] + rcv[k, top].astype(F32) + a_rcv[k, top].astype(F32)
            ).astype(BF16)
            across(k).start()

        def inner_final(k):
            across(k).wait_recv()
            y_ref[mine, ycols(k)] = (
                part[k, top].astype(F32) + b_rcv[k, top].astype(F32)
            ).astype(BF16)
            to_outer(k).start()
            share(k).start()

        def outer_final(k):
            to_outer(k).wait_recv()
            share(k).start()

        def terms(k):
            term(k)

            @pl.when(jnp.logical_and(outer, k >= D2D_LAG))
            def _():
                outer_sum(k - D2D_LAG)

            @pl.when(jnp.logical_and(inner, k >= IN_START))
            def _():
                inner_sum(k - IN_START)

            @pl.when(jnp.logical_and(inner, k >= IN_START + FIN_LAG))
            def _():
                inner_final(k - IN_START - FIN_LAG)

        loop(0, n_k, terms)

        @pl.when(outer)
        def _():
            loop(n_k - D2D_LAG, n_k, outer_sum)
            loop(0, n_k, outer_final)
            loop(0, n_k, lambda k: to_inner(k).wait_send())

        @pl.when(inner)
        def _():
            first = n_k - IN_START
            assert first >= FIN_LAG

            def both(k):
                inner_sum(k)
                inner_final(k - FIN_LAG)

            loop(first, n_k, both)
            loop(n_k - FIN_LAG, n_k, inner_final)

            def sent(k):
                across(k).wait_send()
                to_outer(k).wait_send()

            loop(0, n_k, sent)

        def finish(k):
            give(k).wait_send()
            share(k).wait_send()
            shared(k).wait_recv()

        loop(0, n_k, finish)

    for me in (0, 1):

        @pl.when(core == me)
        def _():
            run(me)


def solution(mesh):
    def step(x, w_gate, w_up, w_down):
        rows, depth = x.shape
        width = w_gate.shape[1]
        out = w_down.shape[1]
        most = max(n for _, n in ROWS)
        n_gu = (width // GU_COLS) * GU_PARTS
        n_k = out // Y_COLS
        kd = depth // GU_PARTS
        dma = pltpu.SemaphoreType.DMA
        return pl.pallas_call(
            kernel,
            out_shape=pltpu.VMEM((rows, out), BF16),
            in_specs=[pl.BlockSpec(memory_space=pl.ANY)] * 4,
            out_specs=pl.BlockSpec(memory_space=pltpu.VMEM),
            scratch_shapes=[
                pltpu.VMEM((rows, depth), BF16),
                pltpu.VMEM((n_gu, kd, GU_COLS), BF16),
                pltpu.VMEM((n_gu, kd, GU_COLS), BF16),
                pltpu.VMEM((n_k, width, Y_COLS), BF16),
                pltpu.VMEM((rows, GU_COLS), F32),
                pltpu.VMEM((rows, GU_COLS), F32),
                pltpu.VMEM((rows, width), BF16),
                pltpu.VMEM((n_k, most, Y_COLS), F32),
                pltpu.VMEM((n_k, rows, Y_COLS), BF16),
                pltpu.VMEM((n_k, most, Y_COLS), BF16),
                pltpu.VMEM((n_k, most, Y_COLS), BF16),
                pltpu.VMEM((n_k, most, Y_COLS), BF16),
                pltpu.VMEM((n_k, most, Y_COLS), BF16),
                dma,
                dma((n_gu,)),
                dma((n_gu,)),
                dma((n_k,)),
                dma((n_k,)),
                dma((n_k,)),
                dma((n_k,)),
                dma((2, n_k)),
                dma((n_k,)),
                dma((n_k,)),
                dma((n_k,)),
                dma((n_k,)),
            ],
            compiler_params=pltpu.CompilerParams(
                collective_id=0, has_side_effects=True, vmem_limit_bytes=58 * 1024 * 1024
            ),
        )(x, w_gate, w_up, w_down)

    return jax.shard_map(
        step,
        mesh=mesh,
        in_specs=(P("dp", None), P(None, "tp"), P(None, "tp"), P("tp", None)),
        out_specs=P("dp", None),
        check_vma=False,
    )
```

```python
import jax
import jax.numpy as jnp
from jax import lax
from jax.experimental import pallas as pl
from jax.experimental.pallas import tpu as pltpu
from jax.sharding import PartitionSpec as P

MESH = pl.DeviceIdType.MESH
F32, BF16 = jnp.float32, jnp.bfloat16

GU_COLS = 512
GU_PARTS = 8
Y_COLS = 256
ROWS = ((80, 48), (0, 80))
D2D_LAG = 2
IN_START = 8
FIN_LAG = 5


def kernel(
    x_hbm, wg_hbm, wu_hbm, wd_hbm, y_ref,
    x_v, wg_v, wu_v, wd_v, g_acc, u_acc, hid, own, snd, rcv, part, a_rcv, b_rcv,
    x_sem, wg_sem, wu_sem, wd_sem,
    d_ss, d_rs, p_ss, p_rs, f_ss, f_rs, g_ss, g_rs,
):
    tp = lax.axis_index("tp")
    core = lax.rem(tp, 2)
    z = lax.div(tp, 2)
    sibling = tp + 1 - 2 * core
    inner = jnp.logical_and(z > 0, z < 3)
    outer = jnp.logical_not(inner)
    low = z < 2
    onward = jnp.where(low, tp + 2, tp - 2)
    back = jnp.where(low, tp - 2, tp + 2)

    kd = wg_v.shape[1]
    n_j = wg_v.shape[0] // GU_PARTS
    n_k = wd_v.shape[0]
    barrier = pltpu.get_barrier_semaphore()
    pl.semaphore_signal(barrier, inc=1, device_id={"tp": sibling}, device_id_type=MESH)
    pl.semaphore_signal(barrier, inc=1, device_id={"tp": onward}, device_id_type=MESH)

    @pl.when(inner)
    def _():
        pl.semaphore_signal(barrier, inc=1, device_id={"tp": back}, device_id_type=MESH)

    def ycols(k):
        return pl.ds(pl.multiple_of(k * Y_COLS, Y_COLS), Y_COLS)

    x_copy = pltpu.make_async_copy(x_hbm, x_v, x_sem)

    def gu_copy(hbm, vmem, sem, j, p):
        i = j * GU_PARTS + p
        return pltpu.make_async_copy(
            hbm.at[
                pl.ds(pl.multiple_of(p * kd, kd), kd),
                pl.ds(pl.multiple_of(j * GU_COLS, GU_COLS), GU_COLS),
            ],
            vmem.at[i],
            sem.at[i],
        )

    def wd_copy(k):
        return pltpu.make_async_copy(wd_hbm.at[:, ycols(k)], wd_v.at[k], wd_sem.at[k])

    x_copy.start()

    def start_gu(j, c):
        for p in range(GU_PARTS):
            gu_copy(wg_hbm, wg_v, wg_sem, j, p).start()
            gu_copy(wu_hbm, wu_v, wu_sem, j, p).start()
        return c

    lax.fori_loop(0, n_j, start_gu, 0)

    def start_wd(k, c):
        wd_copy(k).start()
        return c

    lax.fori_loop(0, n_k, start_wd, 0)

    x_copy.wait()

    def gate_up(j, c):
        for p in range(GU_PARTS):
            i = j * GU_PARTS + p
            xs = x_v[:, p * kd : (p + 1) * kd]
            gu_copy(wg_hbm, wg_v, wg_sem, j, p).wait()
            gu_copy(wu_hbm, wu_v, wu_sem, j, p).wait()
            g = jnp.dot(xs, wg_v[i], preferred_element_type=F32)
            u = jnp.dot(xs, wu_v[i], preferred_element_type=F32)
            if p == 0:
                g_acc[...] = g
                u_acc[...] = u
            elif p < GU_PARTS - 1:
                g_acc[...] += g
                u_acc[...] += u
            else:
                g = g_acc[...] + g
                u = u_acc[...] + u
                hid[:, pl.ds(pl.multiple_of(j * GU_COLS, GU_COLS), GU_COLS)] = (
                    jax.nn.silu(g) * u
                ).astype(BF16)
        return c

    lax.fori_loop(0, n_j, gate_up, 0)

    @pl.when(inner)
    def _():
        pl.semaphore_wait(barrier, 3)

    @pl.when(outer)
    def _():
        pl.semaphore_wait(barrier, 2)

    def loop(lo, hi, f):
        def it(k, c):
            f(k)
            return c

        lax.fori_loop(lo, hi, it, 0)

    def remote(src, dst, send, recv, dev):
        return pltpu.make_async_remote_copy(
            src_ref=src, dst_ref=dst, send_sem=send, recv_sem=recv,
            device_id={"tp": dev}, device_id_type=MESH,
        )

    def run(me):
        lo, n = ROWS[me]
        other_lo, other_n = ROWS[1 - me]
        mine, theirs = pl.ds(lo, n), pl.ds(other_lo, other_n)
        top = pl.ds(0, n)

        def give(k):
            return remote(
                snd.at[k, theirs], rcv.at[k, pl.ds(0, other_n)], d_ss.at[k], d_rs.at[k], sibling
            )

        def got(k):
            return remote(snd.at[k, mine], rcv.at[k, top], d_ss.at[k], d_rs.at[k], sibling)

        def to_inner(k):
            return remote(
                part.at[k, top], a_rcv.at[k, top], p_ss.at[k], p_rs.at[0, k], onward
            )

        def across(k):
            return remote(
                part.at[k, top], b_rcv.at[k, top], p_ss.at[k], p_rs.at[1, k], onward
            )

        def to_outer(k):
            y_k = y_ref.at[mine, ycols(k)]
            return remote(y_k, y_k, f_ss.at[k], f_rs.at[k], back)

        def share(k):
            y_k = y_ref.at[mine, ycols(k)]
            return remote(y_k, y_k, g_ss.at[k], g_rs.at[k], sibling)

        def shared(k):
            y_k = y_ref.at[theirs, ycols(k)]
            return remote(y_k, y_k, g_ss.at[k], g_rs.at[k], sibling)

        def term(k):
            wd_copy(k).wait()
            t = jnp.dot(hid[...], wd_v[k], preferred_element_type=F32)
            own[k, top] = t[lo : lo + n]
            snd[k, theirs] = t[other_lo : other_lo + other_n].astype(BF16)
            give(k).start()

        def outer_sum(k):
            got(k).wait_recv()
            part[k, top] = (own[k, top] + rcv[k, top].astype(F32)).astype(BF16)
            to_inner(k).start()

        def inner_sum(k):
            got(k).wait_recv()
            to_inner(k).wait_recv()
            part[k, top] = (
                own[k, top] + rcv[k, top].astype(F32) + a_rcv[k, top].astype(F32)
            ).astype(BF16)
            across(k).start()

        def inner_final(k):
            across(k).wait_recv()
            y_ref[mine, ycols(k)] = (
                part[k, top].astype(F32) + b_rcv[k, top].astype(F32)
            ).astype(BF16)
            to_outer(k).start()
            share(k).start()

        def outer_final(k):
            to_outer(k).wait_recv()
            share(k).start()

        def terms(k):
            term(k)

            @pl.when(jnp.logical_and(outer, k >= D2D_LAG))
            def _():
                outer_sum(k - D2D_LAG)

            @pl.when(jnp.logical_and(inner, k >= IN_START))
            def _():
                inner_sum(k - IN_START)

            @pl.when(jnp.logical_and(inner, k >= IN_START + FIN_LAG))
            def _():
                inner_final(k - IN_START - FIN_LAG)

        loop(0, n_k, terms)

        @pl.when(outer)
        def _():
            loop(n_k - D2D_LAG, n_k, outer_sum)
            loop(0, n_k, outer_final)
            loop(0, n_k, lambda k: to_inner(k).wait_send())

        @pl.when(inner)
        def _():
            first = n_k - IN_START
            assert first >= FIN_LAG

            def both(k):
                inner_sum(k)
                inner_final(k - FIN_LAG)

            loop(first, n_k, both)
            loop(n_k - FIN_LAG, n_k, inner_final)

            def sent(k):
                across(k).wait_send()
                to_outer(k).wait_send()

            loop(0, n_k, sent)

        def finish(k):
            give(k).wait_send()
            share(k).wait_send()
            shared(k).wait_recv()

        loop(0, n_k, finish)

    for me in (0, 1):

        @pl.when(core == me)
        def _():
            run(me)


def solution(mesh):
    def step(x, w_gate, w_up, w_down):
        rows, depth = x.shape
        width = w_gate.shape[1]
        out = w_down.shape[1]
        most = max(n for _, n in ROWS)
        n_gu = (width // GU_COLS) * GU_PARTS
        n_k = out // Y_COLS
        kd = depth // GU_PARTS
        dma = pltpu.SemaphoreType.DMA
        return pl.pallas_call(
            kernel,
            out_shape=pltpu.VMEM((rows, out), BF16),
            in_specs=[pl.BlockSpec(memory_space=pl.ANY)] * 4,
            out_specs=pl.BlockSpec(memory_space=pltpu.VMEM),
            scratch_shapes=[
                pltpu.VMEM((rows, depth), BF16),
                pltpu.VMEM((n_gu, kd, GU_COLS), BF16),
                pltpu.VMEM((n_gu, kd, GU_COLS), BF16),
                pltpu.VMEM((n_k, width, Y_COLS), BF16),
                pltpu.VMEM((rows, GU_COLS), F32),
                pltpu.VMEM((rows, GU_COLS), F32),
                pltpu.VMEM((rows, width), BF16),
                pltpu.VMEM((n_k, most, Y_COLS), F32),
                pltpu.VMEM((n_k, rows, Y_COLS), BF16),
                pltpu.VMEM((n_k, most, Y_COLS), BF16),
                pltpu.VMEM((n_k, most, Y_COLS), BF16),
                pltpu.VMEM((n_k, most, Y_COLS), BF16),
                pltpu.VMEM((n_k, most, Y_COLS), BF16),
                dma,
                dma((n_gu,)),
                dma((n_gu,)),
                dma((n_k,)),
                dma((n_k,)),
                dma((n_k,)),
                dma((n_k,)),
                dma((2, n_k)),
                dma((n_k,)),
                dma((n_k,)),
                dma((n_k,)),
                dma((n_k,)),
            ],
            compiler_params=pltpu.CompilerParams(
                collective_id=0, has_side_effects=True, vmem_limit_bytes=58 * 1024 * 1024
            ),
        )(x, w_gate, w_up, w_down)

    return jax.shard_map(
        step,
        mesh=mesh,
        in_specs=(P("dp", None), P(None, "tp"), P(None, "tp"), P("tp", None)),
        out_specs=P("dp", None),
        check_vma=False,
    )
```

```python
import jax
import jax.numpy as jnp
from jax import lax
from jax.experimental import pallas as pl
from jax.experimental.pallas import tpu as pltpu
from jax.sharding import PartitionSpec as P

MESH = pl.DeviceIdType.MESH
F32, BF16 = jnp.float32, jnp.bfloat16

GU_COLS = 768
GU_PARTS = 10
Y_COLS = 256
ROWS = ((80, 48), (0, 80))
D2D_LAG = 2
IN_START = 8
FIN_LAG = 5


def kernel(
    x_hbm, wg_hbm, wu_hbm, wd_hbm, y_ref,
    x_v, wg_v, wu_v, wd_v, g_acc, u_acc, hid, own, snd, rcv, part, a_rcv, b_rcv,
    x_sem, wg_sem, wu_sem, wd_sem,
    d_ss, d_rs, p_ss, p_rs, f_ss, f_rs, g_ss, g_rs,
):
    tp = lax.axis_index("tp")
    core = lax.rem(tp, 2)
    z = lax.div(tp, 2)
    sibling = tp + 1 - 2 * core
    inner = jnp.logical_and(z > 0, z < 3)
    outer = jnp.logical_not(inner)
    low = z < 2
    onward = jnp.where(low, tp + 2, tp - 2)
    back = jnp.where(low, tp - 2, tp + 2)

    kd = wg_v.shape[1]
    n_j = wg_v.shape[0] // GU_PARTS
    n_k = wd_v.shape[0]
    barrier = pltpu.get_barrier_semaphore()
    pl.semaphore_signal(barrier, inc=1, device_id={"tp": sibling}, device_id_type=MESH)
    pl.semaphore_signal(barrier, inc=1, device_id={"tp": onward}, device_id_type=MESH)

    @pl.when(inner)
    def _():
        pl.semaphore_signal(barrier, inc=1, device_id={"tp": back}, device_id_type=MESH)

    def ycols(k):
        return pl.ds(pl.multiple_of(k * Y_COLS, Y_COLS), Y_COLS)

    x_copy = pltpu.make_async_copy(x_hbm, x_v, x_sem)

    def gu_copy(hbm, vmem, sem, j, p):
        i = j * GU_PARTS + p
        return pltpu.make_async_copy(
            hbm.at[
                pl.ds(pl.multiple_of(p * kd, kd), kd),
                pl.ds(pl.multiple_of(j * GU_COLS, GU_COLS), GU_COLS),
            ],
            vmem.at[i],
            sem.at[i],
        )

    def wd_copy(k):
        return pltpu.make_async_copy(wd_hbm.at[:, ycols(k)], wd_v.at[k], wd_sem.at[k])

    x_copy.start()

    def start_gu(j, c):
        for p in range(GU_PARTS):
            gu_copy(wg_hbm, wg_v, wg_sem, j, p).start()
            gu_copy(wu_hbm, wu_v, wu_sem, j, p).start()
        return c

    lax.fori_loop(0, n_j, start_gu, 0)

    def start_wd(k, c):
        wd_copy(k).start()
        return c

    lax.fori_loop(0, n_k, start_wd, 0)

    x_copy.wait()

    def gate_up(j, c):
        for p in range(GU_PARTS):
            i = j * GU_PARTS + p
            xs = x_v[:, p * kd : (p + 1) * kd]
            gu_copy(wg_hbm, wg_v, wg_sem, j, p).wait()
            gu_copy(wu_hbm, wu_v, wu_sem, j, p).wait()
            g = jnp.dot(xs, wg_v[i], preferred_element_type=F32)
            u = jnp.dot(xs, wu_v[i], preferred_element_type=F32)
            if p == 0:
                g_acc[...] = g
                u_acc[...] = u
            elif p < GU_PARTS - 1:
                g_acc[...] += g
                u_acc[...] += u
            else:
                g = g_acc[...] + g
                u = u_acc[...] + u
                hid[:, pl.ds(pl.multiple_of(j * GU_COLS, GU_COLS), GU_COLS)] = (
                    jax.nn.silu(g) * u
                ).astype(BF16)
        return c

    lax.fori_loop(0, n_j, gate_up, 0)

    @pl.when(inner)
    def _():
        pl.semaphore_wait(barrier, 3)

    @pl.when(outer)
    def _():
        pl.semaphore_wait(barrier, 2)

    def loop(lo, hi, f):
        def it(k, c):
            f(k)
            return c

        lax.fori_loop(lo, hi, it, 0)

    def remote(src, dst, send, recv, dev):
        return pltpu.make_async_remote_copy(
            src_ref=src, dst_ref=dst, send_sem=send, recv_sem=recv,
            device_id={"tp": dev}, device_id_type=MESH,
        )

    def run(me):
        lo, n = ROWS[me]
        other_lo, other_n = ROWS[1 - me]
        mine, theirs = pl.ds(lo, n), pl.ds(other_lo, other_n)
        top = pl.ds(0, n)

        def give(k):
            return remote(
                snd.at[k, theirs], rcv.at[k, pl.ds(0, other_n)], d_ss.at[k], d_rs.at[k], sibling
            )

        def got(k):
            return remote(snd.at[k, mine], rcv.at[k, top], d_ss.at[k], d_rs.at[k], sibling)

        def to_inner(k):
            return remote(
                part.at[k, top], a_rcv.at[k, top], p_ss.at[k], p_rs.at[0, k], onward
            )

        def across(k):
            return remote(
                part.at[k, top], b_rcv.at[k, top], p_ss.at[k], p_rs.at[1, k], onward
            )

        def to_outer(k):
            y_k = y_ref.at[mine, ycols(k)]
            return remote(y_k, y_k, f_ss.at[k], f_rs.at[k], back)

        def share(k):
            y_k = y_ref.at[mine, ycols(k)]
            return remote(y_k, y_k, g_ss.at[k], g_rs.at[k], sibling)

        def shared(k):
            y_k = y_ref.at[theirs, ycols(k)]
            return remote(y_k, y_k, g_ss.at[k], g_rs.at[k], sibling)

        def term(k):
            wd_copy(k).wait()
            t = jnp.dot(hid[...], wd_v[k], preferred_element_type=F32)
            own[k, top] = t[lo : lo + n]
            snd[k, theirs] = t[other_lo : other_lo + other_n].astype(BF16)
            give(k).start()

        def outer_sum(k):
            got(k).wait_recv()
            part[k, top] = (own[k, top] + rcv[k, top].astype(F32)).astype(BF16)
            to_inner(k).start()

        def inner_sum(k):
            got(k).wait_recv()
            to_inner(k).wait_recv()
            part[k, top] = (
                own[k, top] + rcv[k, top].astype(F32) + a_rcv[k, top].astype(F32)
            ).astype(BF16)
            across(k).start()

        def inner_final(k):
            across(k).wait_recv()
            y_ref[mine, ycols(k)] = (
                part[k, top].astype(F32) + b_rcv[k, top].astype(F32)
            ).astype(BF16)
            to_outer(k).start()
            share(k).start()

        def outer_final(k):
            to_outer(k).wait_recv()
            share(k).start()

        def terms(k):
            term(k)

            @pl.when(jnp.logical_and(outer, k >= D2D_LAG))
            def _():
                outer_sum(k - D2D_LAG)

            @pl.when(jnp.logical_and(inner, k >= IN_START))
            def _():
                inner_sum(k - IN_START)

            @pl.when(jnp.logical_and(inner, k >= IN_START + FIN_LAG))
            def _():
                inner_final(k - IN_START - FIN_LAG)

        loop(0, n_k, terms)

        @pl.when(outer)
        def _():
            loop(n_k - D2D_LAG, n_k, outer_sum)
            loop(0, n_k, outer_final)
            loop(0, n_k, lambda k: to_inner(k).wait_send())

        @pl.when(inner)
        def _():
            first = n_k - IN_START
            assert first >= FIN_LAG

            def both(k):
                inner_sum(k)
                inner_final(k - FIN_LAG)

            loop(first, n_k, both)
            loop(n_k - FIN_LAG, n_k, inner_final)

            def sent(k):
                across(k).wait_send()
                to_outer(k).wait_send()

            loop(0, n_k, sent)

        def finish(k):
            give(k).wait_send()
            share(k).wait_send()
            shared(k).wait_recv()

        loop(0, n_k, finish)

    for me in (0, 1):

        @pl.when(core == me)
        def _():
            run(me)


def solution(mesh):
    def step(x, w_gate, w_up, w_down):
        rows, depth = x.shape
        width = w_gate.shape[1]
        out = w_down.shape[1]
        most = max(n for _, n in ROWS)
        n_gu = (width // GU_COLS) * GU_PARTS
        n_k = out // Y_COLS
        kd = depth // GU_PARTS
        dma = pltpu.SemaphoreType.DMA
        return pl.pallas_call(
            kernel,
            out_shape=pltpu.VMEM((rows, out), BF16),
            in_specs=[pl.BlockSpec(memory_space=pl.ANY)] * 4,
            out_specs=pl.BlockSpec(memory_space=pltpu.VMEM),
            scratch_shapes=[
                pltpu.VMEM((rows, depth), BF16),
                pltpu.VMEM((n_gu, kd, GU_COLS), BF16),
                pltpu.VMEM((n_gu, kd, GU_COLS), BF16),
                pltpu.VMEM((n_k, width, Y_COLS), BF16),
                pltpu.VMEM((rows, GU_COLS), F32),
                pltpu.VMEM((rows, GU_COLS), F32),
                pltpu.VMEM((rows, width), BF16),
                pltpu.VMEM((n_k, most, Y_COLS), F32),
                pltpu.VMEM((n_k, rows, Y_COLS), BF16),
                pltpu.VMEM((n_k, most, Y_COLS), BF16),
                pltpu.VMEM((n_k, most, Y_COLS), BF16),
                pltpu.VMEM((n_k, most, Y_COLS), BF16),
                pltpu.VMEM((n_k, most, Y_COLS), BF16),
                dma,
                dma((n_gu,)),
                dma((n_gu,)),
                dma((n_k,)),
                dma((n_k,)),
                dma((n_k,)),
                dma((n_k,)),
                dma((2, n_k)),
                dma((n_k,)),
                dma((n_k,)),
                dma((n_k,)),
                dma((n_k,)),
            ],
            compiler_params=pltpu.CompilerParams(
                collective_id=0, has_side_effects=True, vmem_limit_bytes=58 * 1024 * 1024
            ),
        )(x, w_gate, w_up, w_down)

    return jax.shard_map(
        step,
        mesh=mesh,
        in_specs=(P("dp", None), P(None, "tp"), P(None, "tp"), P("tp", None)),
        out_specs=P("dp", None),
        check_vma=False,
    )
```

```python
import jax
import jax.numpy as jnp
from jax import lax
from jax.experimental import pallas as pl
from jax.experimental.pallas import tpu as pltpu
from jax.sharding import PartitionSpec as P

MESH = pl.DeviceIdType.MESH
F32, BF16 = jnp.float32, jnp.bfloat16

GU_COLS = 768
GU_PARTS = 10
Y_COLS = 256
ROWS = ((80, 48), (0, 80))
D2D_LAG = 2
IN_START = 8
FIN_LAG = 5


def kernel(
    x_hbm, wg_hbm, wu_hbm, wd_hbm, y_ref,
    x_v, wg_v, wu_v, wd_v, g_acc, u_acc, hid, own, snd, rcv, part, a_rcv, b_rcv,
    x_sem, wg_sem, wu_sem, wd_sem,
    d_ss, d_rs, p_ss, p_rs, f_ss, f_rs, g_ss, g_rs, t_ss,
):
    tp = lax.axis_index("tp")
    core = lax.rem(tp, 2)
    z = lax.div(tp, 2)
    sibling = tp + 1 - 2 * core
    inner = jnp.logical_and(z > 0, z < 3)
    outer = jnp.logical_not(inner)
    low = z < 2
    onward = jnp.where(low, tp + 2, tp - 2)
    back = jnp.where(low, tp - 2, tp + 2)

    kd = wg_v.shape[1]
    n_j = wg_v.shape[0] // GU_PARTS
    n_k = wd_v.shape[0]
    last = n_k - 1
    barrier = pltpu.get_barrier_semaphore()
    pl.semaphore_signal(barrier, inc=1, device_id={"tp": sibling}, device_id_type=MESH)
    pl.semaphore_signal(barrier, inc=1, device_id={"tp": onward}, device_id_type=MESH)

    cross = jnp.where(inner, back, onward) + 1 - 2 * core
    pl.semaphore_signal(barrier, inc=1, device_id={"tp": cross}, device_id_type=MESH)

    @pl.when(inner)
    def _():
        pl.semaphore_signal(barrier, inc=1, device_id={"tp": back}, device_id_type=MESH)

    def ycols(k):
        return pl.ds(pl.multiple_of(k * Y_COLS, Y_COLS), Y_COLS)

    x_copy = pltpu.make_async_copy(x_hbm, x_v, x_sem)

    def gu_copy(hbm, vmem, sem, j, p):
        i = j * GU_PARTS + p
        return pltpu.make_async_copy(
            hbm.at[
                pl.ds(pl.multiple_of(p * kd, kd), kd),
                pl.ds(pl.multiple_of(j * GU_COLS, GU_COLS), GU_COLS),
            ],
            vmem.at[i],
            sem.at[i],
        )

    def wd_copy(k):
        return pltpu.make_async_copy(wd_hbm.at[:, ycols(k)], wd_v.at[k], wd_sem.at[k])

    x_copy.start()

    def start_gu(j, c):
        for p in range(GU_PARTS):
            gu_copy(wg_hbm, wg_v, wg_sem, j, p).start()
            gu_copy(wu_hbm, wu_v, wu_sem, j, p).start()
        return c

    lax.fori_loop(0, n_j, start_gu, 0)

    def start_wd(k, c):
        wd_copy(k).start()
        return c

    lax.fori_loop(0, n_k, start_wd, 0)

    x_copy.wait()

    def gate_up(j, c):
        for p in range(GU_PARTS):
            i = j * GU_PARTS + p
            xs = x_v[:, p * kd : (p + 1) * kd]
            gu_copy(wg_hbm, wg_v, wg_sem, j, p).wait()
            gu_copy(wu_hbm, wu_v, wu_sem, j, p).wait()
            g = jnp.dot(xs, wg_v[i], preferred_element_type=F32)
            u = jnp.dot(xs, wu_v[i], preferred_element_type=F32)
            if p == 0:
                g_acc[...] = g
                u_acc[...] = u
            elif p < GU_PARTS - 1:
                g_acc[...] += g
                u_acc[...] += u
            else:
                g = g_acc[...] + g
                u = u_acc[...] + u
                hid[:, pl.ds(pl.multiple_of(j * GU_COLS, GU_COLS), GU_COLS)] = (
                    jax.nn.silu(g) * u
                ).astype(BF16)
        return c

    lax.fori_loop(0, n_j, gate_up, 0)

    @pl.when(inner)
    def _():
        pl.semaphore_wait(barrier, 4)

    @pl.when(outer)
    def _():
        pl.semaphore_wait(barrier, 3)

    def loop(lo, hi, f):
        def it(k, c):
            f(k)
            return c

        lax.fori_loop(lo, hi, it, 0)

    def remote(src, dst, send, recv, dev):
        return pltpu.make_async_remote_copy(
            src_ref=src, dst_ref=dst, send_sem=send, recv_sem=recv,
            device_id={"tp": dev}, device_id_type=MESH,
        )

    def run(me):
        lo, n = ROWS[me]
        other_lo, other_n = ROWS[1 - me]
        mine, theirs = pl.ds(lo, n), pl.ds(other_lo, other_n)
        top = pl.ds(0, n)

        def give(k):
            return remote(
                snd.at[k, theirs], rcv.at[k, pl.ds(0, other_n)], d_ss.at[k], d_rs.at[k], sibling
            )

        def got(k):
            return remote(snd.at[k, mine], rcv.at[k, top], d_ss.at[k], d_rs.at[k], sibling)

        def to_inner(k):
            return remote(
                part.at[k, top], a_rcv.at[k, top], p_ss.at[k], p_rs.at[0, k], onward
            )

        def across(k):
            return remote(
                part.at[k, top], b_rcv.at[k, top], p_ss.at[k], p_rs.at[1, k], onward
            )

        def to_outer(k):
            y_k = y_ref.at[mine, ycols(k)]
            return remote(y_k, y_k, f_ss.at[k], f_rs.at[k], back)

        def share(k):
            y_k = y_ref.at[mine, ycols(k)]
            return remote(y_k, y_k, g_ss.at[k], g_rs.at[k], sibling)

        def to_other():
            y_k = y_ref.at[mine, ycols(last)]
            return remote(y_k, y_k, t_ss, g_rs.at[last], cross)

        def shared(k):
            y_k = y_ref.at[theirs, ycols(k)]
            return remote(y_k, y_k, g_ss.at[k], g_rs.at[k], sibling)

        def term(k):
            wd_copy(k).wait()
            t = jnp.dot(hid[...], wd_v[k], preferred_element_type=F32)
            own[k, top] = t[lo : lo + n]
            snd[k, theirs] = t[other_lo : other_lo + other_n].astype(BF16)
            give(k).start()

        def outer_sum(k):
            got(k).wait_recv()
            part[k, top] = (own[k, top] + rcv[k, top].astype(F32)).astype(BF16)
            to_inner(k).start()

        def inner_sum(k):
            got(k).wait_recv()
            to_inner(k).wait_recv()
            part[k, top] = (
                own[k, top] + rcv[k, top].astype(F32) + a_rcv[k, top].astype(F32)
            ).astype(BF16)
            across(k).start()

        def inner_final(k):
            across(k).wait_recv()
            y_ref[mine, ycols(k)] = (
                part[k, top].astype(F32) + b_rcv[k, top].astype(F32)
            ).astype(BF16)
            to_outer(k).start()

            @pl.when(k == last)
            def _():
                to_other().start()

            share(k).start()

        def outer_final(k):
            to_outer(k).wait_recv()
            share(k).start()

        def terms(k):
            term(k)

            @pl.when(jnp.logical_and(outer, k >= D2D_LAG))
            def _():
                outer_sum(k - D2D_LAG)

            @pl.when(jnp.logical_and(inner, k >= IN_START))
            def _():
                inner_sum(k - IN_START)

            @pl.when(jnp.logical_and(inner, k >= IN_START + FIN_LAG))
            def _():
                inner_final(k - IN_START - FIN_LAG)

        loop(0, n_k, terms)

        @pl.when(outer)
        def _():
            loop(n_k - D2D_LAG, n_k, outer_sum)
            loop(0, last, outer_final)
            to_outer(last).wait_recv()
            loop(0, n_k, lambda k: to_inner(k).wait_send())

        @pl.when(inner)
        def _():
            first = n_k - IN_START
            assert first >= FIN_LAG

            def both(k):
                inner_sum(k)
                inner_final(k - FIN_LAG)

            loop(first, n_k, both)
            loop(n_k - FIN_LAG, n_k, inner_final)

            def sent(k):
                across(k).wait_send()
                to_outer(k).wait_send()

            loop(0, n_k, sent)
            to_other().wait_send()
            share(last).wait_send()

        def finish(k):
            give(k).wait_send()

            @pl.when(k < last)
            def _():
                share(k).wait_send()

            shared(k).wait_recv()

        loop(0, n_k, finish)

    for me in (0, 1):

        @pl.when(core == me)
        def _():
            run(me)


def solution(mesh):
    def step(x, w_gate, w_up, w_down):
        rows, depth = x.shape
        width = w_gate.shape[1]
        out = w_down.shape[1]
        most = max(n for _, n in ROWS)
        n_gu = (width // GU_COLS) * GU_PARTS
        n_k = out // Y_COLS
        kd = depth // GU_PARTS
        dma = pltpu.SemaphoreType.DMA
        return pl.pallas_call(
            kernel,
            out_shape=pltpu.VMEM((rows, out), BF16),
            in_specs=[pl.BlockSpec(memory_space=pl.ANY)] * 4,
            out_specs=pl.BlockSpec(memory_space=pltpu.VMEM),
            scratch_shapes=[
                pltpu.VMEM((rows, depth), BF16),
                pltpu.VMEM((n_gu, kd, GU_COLS), BF16),
                pltpu.VMEM((n_gu, kd, GU_COLS), BF16),
                pltpu.VMEM((n_k, width, Y_COLS), BF16),
                pltpu.VMEM((rows, GU_COLS), F32),
                pltpu.VMEM((rows, GU_COLS), F32),
                pltpu.VMEM((rows, width), BF16),
                pltpu.VMEM((n_k, most, Y_COLS), F32),
                pltpu.VMEM((n_k, rows, Y_COLS), BF16),
                pltpu.VMEM((n_k, most, Y_COLS), BF16),
                pltpu.VMEM((n_k, most, Y_COLS), BF16),
                pltpu.VMEM((n_k, most, Y_COLS), BF16),
                pltpu.VMEM((n_k, most, Y_COLS), BF16),
                dma,
                dma((n_gu,)),
                dma((n_gu,)),
                dma((n_k,)),
                dma((n_k,)),
                dma((n_k,)),
                dma((n_k,)),
                dma((2, n_k)),
                dma((n_k,)),
                dma((n_k,)),
                dma((n_k,)),
                dma((n_k,)),
                dma,
            ],
            compiler_params=pltpu.CompilerParams(
                collective_id=0, has_side_effects=True, vmem_limit_bytes=58 * 1024 * 1024
            ),
        )(x, w_gate, w_up, w_down)

    return jax.shard_map(
        step,
        mesh=mesh,
        in_specs=(P("dp", None), P(None, "tp"), P(None, "tp"), P("tp", None)),
        out_specs=P("dp", None),
        check_vma=False,
    )
```

```python
import jax
import jax.numpy as jnp
from jax import lax
from jax.experimental import pallas as pl
from jax.experimental.pallas import tpu as pltpu
from jax.sharding import PartitionSpec as P

MESH = pl.DeviceIdType.MESH
F32, BF16 = jnp.float32, jnp.bfloat16

GU_COLS = 768
GU_PARTS = 10
Y_COLS = 256
ROWS = ((80, 48), (0, 80))
D2D_LAG = 2
IN_START = 8
FIN_LAG = 5


def kernel(
    x_hbm, wg_hbm, wu_hbm, wd_hbm, y_ref,
    x_v, wg_v, wu_v, wd_v, g_acc, u_acc, hid, own, snd, rcv, part, a_rcv, b_rcv,
    x_sem, wg_sem, wu_sem, wd_sem,
    d_ss, d_rs, p_ss, p_rs, f_ss, f_rs, g_ss, g_rs,
):
    tp = lax.axis_index("tp")
    core = lax.rem(tp, 2)
    z = lax.div(tp, 2)
    sibling = tp + 1 - 2 * core
    inner = jnp.logical_and(z > 0, z < 3)
    outer = jnp.logical_not(inner)
    low = z < 2
    onward = jnp.where(low, tp + 2, tp - 2)
    back = jnp.where(low, tp - 2, tp + 2)

    kd = wg_v.shape[1]
    n_j = wg_v.shape[0] // GU_PARTS
    n_k = wd_v.shape[0]
    barrier = pltpu.get_barrier_semaphore()
    pl.semaphore_signal(barrier, inc=1, device_id={"tp": sibling}, device_id_type=MESH)
    pl.semaphore_signal(barrier, inc=1, device_id={"tp": onward}, device_id_type=MESH)

    @pl.when(inner)
    def _():
        pl.semaphore_signal(barrier, inc=1, device_id={"tp": back}, device_id_type=MESH)

    def ycols(k):
        return pl.ds(pl.multiple_of(k * Y_COLS, Y_COLS), Y_COLS)

    def loop(lo, hi, f):
        def it(k, c):
            f(k)
            return c

        lax.fori_loop(lo, hi, it, 0)

    def remote(src, dst, send, recv, dev):
        return pltpu.make_async_remote_copy(
            src_ref=src, dst_ref=dst, send_sem=send, recv_sem=recv,
            device_id={"tp": dev}, device_id_type=MESH,
        )

    depth = x_v.shape[1]
    left, right = pl.ds(0, depth // 2), pl.ds(depth // 2, depth // 2)
    x_left = pltpu.make_async_copy(x_hbm.at[:, left], x_v.at[:, left], x_sem.at[0])
    x_right = pltpu.make_async_copy(x_hbm.at[:, right], x_v.at[:, right], x_sem.at[1])
    x_gift = remote(x_v.at[:, right], x_v.at[:, right], x_sem.at[2], x_sem.at[3], sibling)

    def gu_copies(hbm, vmem, sem, j, p):
        i = j * GU_PARTS + p
        parts = 2 if p == GU_PARTS - 1 else 1
        n = kd // parts
        return [
            pltpu.make_async_copy(
                hbm.at[
                    pl.ds(p * kd + h * n, n),
                    pl.ds(pl.multiple_of(j * GU_COLS, GU_COLS), GU_COLS),
                ],
                vmem.at[i, pl.ds(h * n, n)],
                sem.at[j * (GU_PARTS + 1) + p + h],
            )
            for h in range(parts)
        ]

    def wd_copy(k):
        return pltpu.make_async_copy(wd_hbm.at[:, ycols(k)], wd_v.at[k], wd_sem.at[k])

    x_left.start()

    @pl.when(core == 1)
    def _():
        x_right.start()


    def start_gu(j, c):
        for p in range(GU_PARTS):
            gate = gu_copies(wg_hbm, wg_v, wg_sem, j, p)
            up = gu_copies(wu_hbm, wu_v, wu_sem, j, p)
            for g, u in zip(gate, up):
                g.start()
                u.start()
        return c

    lax.fori_loop(0, n_j, start_gu, 0)

    def start_wd(k, c):
        wd_copy(k).start()
        return c

    lax.fori_loop(0, n_k, start_wd, 0)

    @pl.when(inner)
    def _():
        pl.semaphore_wait(barrier, 3)

    @pl.when(outer)
    def _():
        pl.semaphore_wait(barrier, 2)

    x_left.wait()

    @pl.when(core == 1)
    def _():
        x_right.wait()
        x_gift.start()


    def gate_up(j, c):
        for p in range(GU_PARTS):
            i = j * GU_PARTS + p
            if p == GU_PARTS // 2:

                @pl.when(jnp.logical_and(j == 0, core == 0))
                def _():
                    x_gift.wait_recv()

            gate = gu_copies(wg_hbm, wg_v, wg_sem, j, p)
            up = gu_copies(wu_hbm, wu_v, wu_sem, j, p)
            n = kd // len(gate)
            for h in range(len(gate)):
                gate[h].wait()
                up[h].wait()
                lo = h * n
                xs = x_v[:, p * kd + lo : p * kd + lo + n]
                g = jnp.dot(xs, wg_v[i, lo : lo + n], preferred_element_type=F32)
                u = jnp.dot(xs, wu_v[i, lo : lo + n], preferred_element_type=F32)
                if p == 0:
                    g_acc[...] = g
                    u_acc[...] = u
                elif h == 0:
                    g_acc[...] += g
                    u_acc[...] += u
                else:
                    g = g_acc[...] + g
                    u = u_acc[...] + u
                    hid[:, pl.ds(pl.multiple_of(j * GU_COLS, GU_COLS), GU_COLS)] = (
                        jax.nn.silu(g) * u
                    ).astype(BF16)
        return c

    lax.fori_loop(0, n_j, gate_up, 0)

    def run(me):
        lo, n = ROWS[me]
        other_lo, other_n = ROWS[1 - me]
        mine, theirs = pl.ds(lo, n), pl.ds(other_lo, other_n)
        top = pl.ds(0, n)

        def give(k):
            return remote(
                snd.at[k, theirs], rcv.at[k, pl.ds(0, other_n)], d_ss.at[k], d_rs.at[k], sibling
            )

        def got(k):
            return remote(snd.at[k, mine], rcv.at[k, top], d_ss.at[k], d_rs.at[k], sibling)

        def to_inner(k):
            return remote(
                part.at[k, top], a_rcv.at[k, top], p_ss.at[k], p_rs.at[0, k], onward
            )

        def across(k):
            return remote(
                part.at[k, top], b_rcv.at[k, top], p_ss.at[k], p_rs.at[1, k], onward
            )

        def to_outer(k):
            y_k = y_ref.at[mine, ycols(k)]
            return remote(y_k, y_k, f_ss.at[k], f_rs.at[k], back)

        def share(k):
            y_k = y_ref.at[mine, ycols(k)]
            return remote(y_k, y_k, g_ss.at[k], g_rs.at[k], sibling)

        def shared(k):
            y_k = y_ref.at[theirs, ycols(k)]
            return remote(y_k, y_k, g_ss.at[k], g_rs.at[k], sibling)

        def term(k):
            wd_copy(k).wait()
            t = jnp.dot(hid[...], wd_v[k], preferred_element_type=F32)
            own[k, top] = t[lo : lo + n]
            snd[k, theirs] = t[other_lo : other_lo + other_n].astype(BF16)
            give(k).start()

        def outer_sum(k):
            got(k).wait_recv()
            part[k, top] = (own[k, top] + rcv[k, top].astype(F32)).astype(BF16)
            to_inner(k).start()

        def inner_sum(k):
            got(k).wait_recv()
            to_inner(k).wait_recv()
            part[k, top] = (
                own[k, top] + rcv[k, top].astype(F32) + a_rcv[k, top].astype(F32)
            ).astype(BF16)
            across(k).start()

        def inner_final(k):
            across(k).wait_recv()
            y_ref[mine, ycols(k)] = (
                part[k, top].astype(F32) + b_rcv[k, top].astype(F32)
            ).astype(BF16)
            to_outer(k).start()
            share(k).start()

        def outer_final(k):
            to_outer(k).wait_recv()
            share(k).start()

        def terms(k):
            term(k)

            @pl.when(jnp.logical_and(outer, k >= D2D_LAG))
            def _():
                outer_sum(k - D2D_LAG)

            @pl.when(jnp.logical_and(inner, k >= IN_START))
            def _():
                inner_sum(k - IN_START)

            @pl.when(jnp.logical_and(inner, k >= IN_START + FIN_LAG))
            def _():
                inner_final(k - IN_START - FIN_LAG)

        loop(0, n_k, terms)

        @pl.when(outer)
        def _():
            loop(n_k - D2D_LAG, n_k, outer_sum)
            loop(0, n_k, outer_final)
            loop(0, n_k, lambda k: to_inner(k).wait_send())

        @pl.when(inner)
        def _():
            first = n_k - IN_START
            assert first >= FIN_LAG

            def both(k):
                inner_sum(k)
                inner_final(k - FIN_LAG)

            loop(first, n_k, both)
            loop(n_k - FIN_LAG, n_k, inner_final)

            def sent(k):
                across(k).wait_send()
                to_outer(k).wait_send()

            loop(0, n_k, sent)

        def finish(k):
            give(k).wait_send()
            share(k).wait_send()
            shared(k).wait_recv()

        loop(0, n_k, finish)

    @pl.when(core == 1)
    def _():
        x_gift.wait_send()

    for me in (0, 1):

        @pl.when(core == me)
        def _():
            run(me)


def solution(mesh):
    def step(x, w_gate, w_up, w_down):
        rows, depth = x.shape
        width = w_gate.shape[1]
        out = w_down.shape[1]
        most = max(n for _, n in ROWS)
        n_gu = (width // GU_COLS) * GU_PARTS
        n_k = out // Y_COLS
        kd = depth // GU_PARTS
        dma = pltpu.SemaphoreType.DMA
        return pl.pallas_call(
            kernel,
            out_shape=pltpu.VMEM((rows, out), BF16),
            in_specs=[pl.BlockSpec(memory_space=pl.ANY)] * 4,
            out_specs=pl.BlockSpec(memory_space=pltpu.VMEM),
            scratch_shapes=[
                pltpu.VMEM((rows, depth), BF16),
                pltpu.VMEM((n_gu, kd, GU_COLS), BF16),
                pltpu.VMEM((n_gu, kd, GU_COLS), BF16),
                pltpu.VMEM((n_k, width, Y_COLS), BF16),
                pltpu.VMEM((rows, GU_COLS), F32),
                pltpu.VMEM((rows, GU_COLS), F32),
                pltpu.VMEM((rows, width), BF16),
                pltpu.VMEM((n_k, most, Y_COLS), F32),
                pltpu.VMEM((n_k, rows, Y_COLS), BF16),
                pltpu.VMEM((n_k, most, Y_COLS), BF16),
                pltpu.VMEM((n_k, most, Y_COLS), BF16),
                pltpu.VMEM((n_k, most, Y_COLS), BF16),
                pltpu.VMEM((n_k, most, Y_COLS), BF16),
                dma((4,)),
                dma((n_gu + width // GU_COLS,)),
                dma((n_gu + width // GU_COLS,)),
                dma((n_k,)),
                dma((n_k,)),
                dma((n_k,)),
                dma((n_k,)),
                dma((2, n_k)),
                dma((n_k,)),
                dma((n_k,)),
                dma((n_k,)),
                dma((n_k,)),
            ],
            compiler_params=pltpu.CompilerParams(
                collective_id=0, has_side_effects=True, vmem_limit_bytes=58 * 1024 * 1024
            ),
        )(x, w_gate, w_up, w_down)

    return jax.shard_map(
        step,
        mesh=mesh,
        in_specs=(P("dp", None), P(None, "tp"), P(None, "tp"), P("tp", None)),
        out_specs=P("dp", None),
        check_vma=False,
    )
```

```python
import jax
import jax.numpy as jnp
from jax import lax
from jax.experimental import pallas as pl
from jax.experimental.pallas import tpu as pltpu
from jax.sharding import PartitionSpec as P

MESH = pl.DeviceIdType.MESH
F32, BF16 = jnp.float32, jnp.bfloat16

GU_COLS = 768
X_PARTS = 3
GU_PARTS = 10
Y_COLS = 256
ROWS = ((80, 48), (0, 80))
D2D_LAG = 2
IN_START = 8
FIN_LAG = 5


def kernel(
    x_hbm, wg_hbm, wu_hbm, wd_hbm, y_ref,
    x_v, wg_v, wu_v, wd_v, g_acc, u_acc, hid, own, snd, rcv, part, a_rcv, b_rcv,
    x_sem, wg_sem, wu_sem, wd_sem,
    d_ss, d_rs, p_ss, p_rs, f_ss, f_rs, g_ss, g_rs,
):
    tp = lax.axis_index("tp")
    core = lax.rem(tp, 2)
    z = lax.div(tp, 2)
    sibling = tp + 1 - 2 * core
    inner = jnp.logical_and(z > 0, z < 3)
    outer = jnp.logical_not(inner)
    low = z < 2
    onward = jnp.where(low, tp + 2, tp - 2)
    back = jnp.where(low, tp - 2, tp + 2)

    kd = wg_v.shape[1]
    n_j = wg_v.shape[0] // GU_PARTS
    n_k = wd_v.shape[0]
    barrier = pltpu.get_barrier_semaphore()
    pl.semaphore_signal(barrier, inc=1, device_id={"tp": sibling}, device_id_type=MESH)
    pl.semaphore_signal(barrier, inc=1, device_id={"tp": onward}, device_id_type=MESH)

    @pl.when(inner)
    def _():
        pl.semaphore_signal(barrier, inc=1, device_id={"tp": back}, device_id_type=MESH)

    def ycols(k):
        return pl.ds(pl.multiple_of(k * Y_COLS, Y_COLS), Y_COLS)

    def loop(lo, hi, f):
        def it(k, c):
            f(k)
            return c

        lax.fori_loop(lo, hi, it, 0)

    def remote(src, dst, send, recv, dev):
        return pltpu.make_async_remote_copy(
            src_ref=src, dst_ref=dst, send_sem=send, recv_sem=recv,
            device_id={"tp": dev}, device_id_type=MESH,
        )

    depth = x_v.shape[1]
    split = X_PARTS * kd
    left, right = pl.ds(0, split), pl.ds(split, depth - split)
    x_left = pltpu.make_async_copy(x_hbm.at[:, left], x_v.at[:, left], x_sem.at[0])
    x_right = pltpu.make_async_copy(x_hbm.at[:, right], x_v.at[:, right], x_sem.at[1])
    x_gift = remote(x_v.at[:, right], x_v.at[:, right], x_sem.at[2], x_sem.at[3], sibling)

    def gu_copies(hbm, vmem, sem, j, p):
        i = j * GU_PARTS + p
        parts = 2 if p == GU_PARTS - 1 else 1
        n = kd // parts
        return [
            pltpu.make_async_copy(
                hbm.at[
                    pl.ds(p * kd + h * n, n),
                    pl.ds(pl.multiple_of(j * GU_COLS, GU_COLS), GU_COLS),
                ],
                vmem.at[i, pl.ds(h * n, n)],
                sem.at[j * (GU_PARTS + 1) + p + h],
            )
            for h in range(parts)
        ]

    def wd_copy(k):
        return pltpu.make_async_copy(wd_hbm.at[:, ycols(k)], wd_v.at[k], wd_sem.at[k])

    x_left.start()

    @pl.when(core == 1)
    def _():
        x_right.start()


    def start_gu(j, c):
        for p in range(GU_PARTS):
            gate = gu_copies(wg_hbm, wg_v, wg_sem, j, p)
            up = gu_copies(wu_hbm, wu_v, wu_sem, j, p)
            for g, u in zip(gate, up):
                g.start()
                u.start()
        return c

    lax.fori_loop(0, n_j, start_gu, 0)

    def start_wd(k, c):
        wd_copy(k).start()
        return c

    lax.fori_loop(0, n_k, start_wd, 0)

    @pl.when(inner)
    def _():
        pl.semaphore_wait(barrier, 3)

    @pl.when(outer)
    def _():
        pl.semaphore_wait(barrier, 2)

    x_left.wait()

    @pl.when(core == 1)
    def _():
        x_right.wait()
        x_gift.start()


    def gate_up(j, c):
        for p in range(GU_PARTS):
            i = j * GU_PARTS + p
            if p == X_PARTS:

                @pl.when(jnp.logical_and(j == 0, core == 0))
                def _():
                    x_gift.wait_recv()

            gate = gu_copies(wg_hbm, wg_v, wg_sem, j, p)
            up = gu_copies(wu_hbm, wu_v, wu_sem, j, p)
            n = kd // len(gate)
            for h in range(len(gate)):
                gate[h].wait()
                up[h].wait()
                lo = h * n
                xs = x_v[:, p * kd + lo : p * kd + lo + n]
                g = jnp.dot(xs, wg_v[i, lo : lo + n], preferred_element_type=F32)
                u = jnp.dot(xs, wu_v[i, lo : lo + n], preferred_element_type=F32)
                if p == 0:
                    g_acc[...] = g
                    u_acc[...] = u
                elif h == 0:
                    g_acc[...] += g
                    u_acc[...] += u
                else:
                    g = g_acc[...] + g
                    u = u_acc[...] + u
                    hid[:, pl.ds(pl.multiple_of(j * GU_COLS, GU_COLS), GU_COLS)] = (
                        jax.nn.silu(g) * u
                    ).astype(BF16)
        return c

    lax.fori_loop(0, n_j, gate_up, 0)

    def run(me):
        lo, n = ROWS[me]
        other_lo, other_n = ROWS[1 - me]
        mine, theirs = pl.ds(lo, n), pl.ds(other_lo, other_n)
        top = pl.ds(0, n)

        def give(k):
            return remote(
                snd.at[k, theirs], rcv.at[k, pl.ds(0, other_n)], d_ss.at[k], d_rs.at[k], sibling
            )

        def got(k):
            return remote(snd.at[k, mine], rcv.at[k, top], d_ss.at[k], d_rs.at[k], sibling)

        def to_inner(k):
            return remote(
                part.at[k, top], a_rcv.at[k, top], p_ss.at[k], p_rs.at[0, k], onward
            )

        def across(k):
            return remote(
                part.at[k, top], b_rcv.at[k, top], p_ss.at[k], p_rs.at[1, k], onward
            )

        def to_outer(k):
            y_k = y_ref.at[mine, ycols(k)]
            return remote(y_k, y_k, f_ss.at[k], f_rs.at[k], back)

        def share(k):
            y_k = y_ref.at[mine, ycols(k)]
            return remote(y_k, y_k, g_ss.at[k], g_rs.at[k], sibling)

        def shared(k):
            y_k = y_ref.at[theirs, ycols(k)]
            return remote(y_k, y_k, g_ss.at[k], g_rs.at[k], sibling)

        def term(k):
            wd_copy(k).wait()
            t = jnp.dot(hid[...], wd_v[k], preferred_element_type=F32)
            own[k, top] = t[lo : lo + n]
            snd[k, theirs] = t[other_lo : other_lo + other_n].astype(BF16)
            give(k).start()

        def outer_sum(k):
            got(k).wait_recv()
            part[k, top] = (own[k, top] + rcv[k, top].astype(F32)).astype(BF16)
            to_inner(k).start()

        def inner_sum(k):
            got(k).wait_recv()
            to_inner(k).wait_recv()
            part[k, top] = (
                own[k, top] + rcv[k, top].astype(F32) + a_rcv[k, top].astype(F32)
            ).astype(BF16)
            across(k).start()

        def inner_final(k):
            across(k).wait_recv()
            y_ref[mine, ycols(k)] = (
                part[k, top].astype(F32) + b_rcv[k, top].astype(F32)
            ).astype(BF16)
            to_outer(k).start()
            share(k).start()

        def outer_final(k):
            to_outer(k).wait_recv()
            share(k).start()

        def terms(k):
            term(k)

            @pl.when(jnp.logical_and(outer, k >= D2D_LAG))
            def _():
                outer_sum(k - D2D_LAG)

            @pl.when(jnp.logical_and(inner, k >= IN_START))
            def _():
                inner_sum(k - IN_START)

            @pl.when(jnp.logical_and(inner, k >= IN_START + FIN_LAG))
            def _():
                inner_final(k - IN_START - FIN_LAG)

        loop(0, n_k, terms)

        @pl.when(outer)
        def _():
            loop(n_k - D2D_LAG, n_k, outer_sum)
            loop(0, n_k, outer_final)
            loop(0, n_k, lambda k: to_inner(k).wait_send())

        @pl.when(inner)
        def _():
            first = n_k - IN_START
            assert first >= FIN_LAG

            def both(k):
                inner_sum(k)
                inner_final(k - FIN_LAG)

            loop(first, n_k, both)
            loop(n_k - FIN_LAG, n_k, inner_final)

            def sent(k):
                across(k).wait_send()
                to_outer(k).wait_send()

            loop(0, n_k, sent)

        def finish(k):
            give(k).wait_send()
            share(k).wait_send()
            shared(k).wait_recv()

        loop(0, n_k, finish)

    @pl.when(core == 1)
    def _():
        x_gift.wait_send()

    for me in (0, 1):

        @pl.when(core == me)
        def _():
            run(me)


def solution(mesh):
    def step(x, w_gate, w_up, w_down):
        rows, depth = x.shape
        width = w_gate.shape[1]
        out = w_down.shape[1]
        most = max(n for _, n in ROWS)
        n_gu = (width // GU_COLS) * GU_PARTS
        n_k = out // Y_COLS
        kd = depth // GU_PARTS
        dma = pltpu.SemaphoreType.DMA
        return pl.pallas_call(
            kernel,
            out_shape=pltpu.VMEM((rows, out), BF16),
            in_specs=[pl.BlockSpec(memory_space=pl.ANY)] * 4,
            out_specs=pl.BlockSpec(memory_space=pltpu.VMEM),
            scratch_shapes=[
                pltpu.VMEM((rows, depth), BF16),
                pltpu.VMEM((n_gu, kd, GU_COLS), BF16),
                pltpu.VMEM((n_gu, kd, GU_COLS), BF16),
                pltpu.VMEM((n_k, width, Y_COLS), BF16),
                pltpu.VMEM((rows, GU_COLS), F32),
                pltpu.VMEM((rows, GU_COLS), F32),
                pltpu.VMEM((rows, width), BF16),
                pltpu.VMEM((n_k, most, Y_COLS), F32),
                pltpu.VMEM((n_k, rows, Y_COLS), BF16),
                pltpu.VMEM((n_k, most, Y_COLS), BF16),
                pltpu.VMEM((n_k, most, Y_COLS), BF16),
                pltpu.VMEM((n_k, most, Y_COLS), BF16),
                pltpu.VMEM((n_k, most, Y_COLS), BF16),
                dma((4,)),
                dma((n_gu + width // GU_COLS,)),
                dma((n_gu + width // GU_COLS,)),
                dma((n_k,)),
                dma((n_k,)),
                dma((n_k,)),
                dma((n_k,)),
                dma((2, n_k)),
                dma((n_k,)),
                dma((n_k,)),
                dma((n_k,)),
                dma((n_k,)),
            ],
            compiler_params=pltpu.CompilerParams(
                collective_id=0, has_side_effects=True, vmem_limit_bytes=58 * 1024 * 1024
            ),
        )(x, w_gate, w_up, w_down)

    return jax.shard_map(
        step,
        mesh=mesh,
        in_specs=(P("dp", None), P(None, "tp"), P(None, "tp"), P("tp", None)),
        out_specs=P("dp", None),
        check_vma=False,
    )
```

```python
import jax
import jax.numpy as jnp
from jax import lax
from jax.experimental import pallas as pl
from jax.experimental.pallas import tpu as pltpu
from jax.sharding import PartitionSpec as P

MESH = pl.DeviceIdType.MESH
F32, BF16 = jnp.float32, jnp.bfloat16

GU_COLS = 768
X_PARTS = 1
GU_PARTS = 10
Y_COLS = 256
ROWS = ((80, 48), (0, 80))
D2D_LAG = 2
IN_START = 8
FIN_LAG = 5


def kernel(
    x_hbm, wg_hbm, wu_hbm, wd_hbm, y_ref,
    x_v, wg_v, wu_v, wd_v, g_acc, u_acc, hid, own, snd, rcv, part, a_rcv, b_rcv,
    x_sem, wg_sem, wu_sem, wd_sem,
    d_ss, d_rs, p_ss, p_rs, f_ss, f_rs, g_ss, g_rs,
):
    tp = lax.axis_index("tp")
    core = lax.rem(tp, 2)
    z = lax.div(tp, 2)
    sibling = tp + 1 - 2 * core
    inner = jnp.logical_and(z > 0, z < 3)
    outer = jnp.logical_not(inner)
    low = z < 2
    onward = jnp.where(low, tp + 2, tp - 2)
    back = jnp.where(low, tp - 2, tp + 2)

    kd = wg_v.shape[1]
    n_j = wg_v.shape[0] // GU_PARTS
    n_k = wd_v.shape[0]
    barrier = pltpu.get_barrier_semaphore()
    pl.semaphore_signal(barrier, inc=1, device_id={"tp": sibling}, device_id_type=MESH)
    pl.semaphore_signal(barrier, inc=1, device_id={"tp": onward}, device_id_type=MESH)

    @pl.when(inner)
    def _():
        pl.semaphore_signal(barrier, inc=1, device_id={"tp": back}, device_id_type=MESH)

    def ycols(k):
        return pl.ds(pl.multiple_of(k * Y_COLS, Y_COLS), Y_COLS)

    def loop(lo, hi, f):
        def it(k, c):
            f(k)
            return c

        lax.fori_loop(lo, hi, it, 0)

    def remote(src, dst, send, recv, dev):
        return pltpu.make_async_remote_copy(
            src_ref=src, dst_ref=dst, send_sem=send, recv_sem=recv,
            device_id={"tp": dev}, device_id_type=MESH,
        )

    depth = x_v.shape[1]
    split = X_PARTS * kd
    left, right = pl.ds(0, split), pl.ds(split, depth - split)
    x_left = pltpu.make_async_copy(x_hbm.at[:, left], x_v.at[:, left], x_sem.at[0])
    x_right = pltpu.make_async_copy(x_hbm.at[:, right], x_v.at[:, right], x_sem.at[1])
    x_gift = remote(x_v.at[:, right], x_v.at[:, right], x_sem.at[2], x_sem.at[3], sibling)

    def gu_copies(hbm, vmem, sem, j, p):
        i = j * GU_PARTS + p
        parts = 2 if p == GU_PARTS - 1 else 1
        n = kd // parts
        return [
            pltpu.make_async_copy(
                hbm.at[
                    pl.ds(p * kd + h * n, n),
                    pl.ds(pl.multiple_of(j * GU_COLS, GU_COLS), GU_COLS),
                ],
                vmem.at[i, pl.ds(h * n, n)],
                sem.at[j * (GU_PARTS + 1) + p + h],
            )
            for h in range(parts)
        ]

    def wd_copy(k):
        return pltpu.make_async_copy(wd_hbm.at[:, ycols(k)], wd_v.at[k], wd_sem.at[k])

    x_left.start()

    @pl.when(core == 1)
    def _():
        x_right.start()


    def start_gu(j, c):
        for p in range(GU_PARTS):
            gate = gu_copies(wg_hbm, wg_v, wg_sem, j, p)
            up = gu_copies(wu_hbm, wu_v, wu_sem, j, p)
            for g, u in zip(gate, up):
                g.start()
                u.start()
        return c

    lax.fori_loop(0, n_j, start_gu, 0)

    def start_wd(k, c):
        wd_copy(k).start()
        return c

    lax.fori_loop(0, n_k, start_wd, 0)

    @pl.when(inner)
    def _():
        pl.semaphore_wait(barrier, 3)

    @pl.when(outer)
    def _():
        pl.semaphore_wait(barrier, 2)

    x_left.wait()

    @pl.when(core == 1)
    def _():
        x_right.wait()
        x_gift.start()


    def gate_up(j, c):
        for p in range(GU_PARTS):
            i = j * GU_PARTS + p
            if p == X_PARTS:

                @pl.when(jnp.logical_and(j == 0, core == 0))
                def _():
                    x_gift.wait_recv()

            gate = gu_copies(wg_hbm, wg_v, wg_sem, j, p)
            up = gu_copies(wu_hbm, wu_v, wu_sem, j, p)
            n = kd // len(gate)
            for h in range(len(gate)):
                gate[h].wait()
                up[h].wait()
                lo = h * n
                xs = x_v[:, p * kd + lo : p * kd + lo + n]
                g = jnp.dot(xs, wg_v[i, lo : lo + n], preferred_element_type=F32)
                u = jnp.dot(xs, wu_v[i, lo : lo + n], preferred_element_type=F32)
                if p == 0:
                    g_acc[...] = g
                    u_acc[...] = u
                elif h == 0:
                    g_acc[...] += g
                    u_acc[...] += u
                else:
                    g = g_acc[...] + g
                    u = u_acc[...] + u
                    hid[:, pl.ds(pl.multiple_of(j * GU_COLS, GU_COLS), GU_COLS)] = (
                        jax.nn.silu(g) * u
                    ).astype(BF16)
        return c

    lax.fori_loop(0, n_j, gate_up, 0)

    def run(me):
        lo, n = ROWS[me]
        other_lo, other_n = ROWS[1 - me]
        mine, theirs = pl.ds(lo, n), pl.ds(other_lo, other_n)
        top = pl.ds(0, n)

        def give(k):
            return remote(
                snd.at[k, theirs], rcv.at[k, pl.ds(0, other_n)], d_ss.at[k], d_rs.at[k], sibling
            )

        def got(k):
            return remote(snd.at[k, mine], rcv.at[k, top], d_ss.at[k], d_rs.at[k], sibling)

        def to_inner(k):
            return remote(
                part.at[k, top], a_rcv.at[k, top], p_ss.at[k], p_rs.at[0, k], onward
            )

        def across(k):
            return remote(
                part.at[k, top], b_rcv.at[k, top], p_ss.at[k], p_rs.at[1, k], onward
            )

        def to_outer(k):
            y_k = y_ref.at[mine, ycols(k)]
            return remote(y_k, y_k, f_ss.at[k], f_rs.at[k], back)

        def share(k):
            y_k = y_ref.at[mine, ycols(k)]
            return remote(y_k, y_k, g_ss.at[k], g_rs.at[k], sibling)

        def shared(k):
            y_k = y_ref.at[theirs, ycols(k)]
            return remote(y_k, y_k, g_ss.at[k], g_rs.at[k], sibling)

        def term(k):
            wd_copy(k).wait()
            t = jnp.dot(hid[...], wd_v[k], preferred_element_type=F32)
            own[k, top] = t[lo : lo + n]
            snd[k, theirs] = t[other_lo : other_lo + other_n].astype(BF16)
            give(k).start()

        def outer_sum(k):
            got(k).wait_recv()
            part[k, top] = (own[k, top] + rcv[k, top].astype(F32)).astype(BF16)
            to_inner(k).start()

        def inner_sum(k):
            got(k).wait_recv()
            to_inner(k).wait_recv()
            part[k, top] = (
                own[k, top] + rcv[k, top].astype(F32) + a_rcv[k, top].astype(F32)
            ).astype(BF16)
            across(k).start()

        def inner_final(k):
            across(k).wait_recv()
            y_ref[mine, ycols(k)] = (
                part[k, top].astype(F32) + b_rcv[k, top].astype(F32)
            ).astype(BF16)
            to_outer(k).start()
            share(k).start()

        def outer_final(k):
            to_outer(k).wait_recv()
            share(k).start()

        def terms(k):
            term(k)

            @pl.when(jnp.logical_and(outer, k >= D2D_LAG))
            def _():
                outer_sum(k - D2D_LAG)

            @pl.when(jnp.logical_and(inner, k >= IN_START))
            def _():
                inner_sum(k - IN_START)

            @pl.when(jnp.logical_and(inner, k >= IN_START + FIN_LAG))
            def _():
                inner_final(k - IN_START - FIN_LAG)

        loop(0, n_k, terms)

        @pl.when(outer)
        def _():
            loop(n_k - D2D_LAG, n_k, outer_sum)
            loop(0, n_k, outer_final)
            loop(0, n_k, lambda k: to_inner(k).wait_send())

        @pl.when(inner)
        def _():
            first = n_k - IN_START
            assert first >= FIN_LAG

            def both(k):
                inner_sum(k)
                inner_final(k - FIN_LAG)

            loop(first, n_k, both)
            loop(n_k - FIN_LAG, n_k, inner_final)

            def sent(k):
                across(k).wait_send()
                to_outer(k).wait_send()

            loop(0, n_k, sent)

        def finish(k):
            give(k).wait_send()
            share(k).wait_send()
            shared(k).wait_recv()

        loop(0, n_k, finish)

    @pl.when(core == 1)
    def _():
        x_gift.wait_send()

    for me in (0, 1):

        @pl.when(core == me)
        def _():
            run(me)


def solution(mesh):
    def step(x, w_gate, w_up, w_down):
        rows, depth = x.shape
        width = w_gate.shape[1]
        out = w_down.shape[1]
        most = max(n for _, n in ROWS)
        n_gu = (width // GU_COLS) * GU_PARTS
        n_k = out // Y_COLS
        kd = depth // GU_PARTS
        dma = pltpu.SemaphoreType.DMA
        return pl.pallas_call(
            kernel,
            out_shape=pltpu.VMEM((rows, out), BF16),
            in_specs=[pl.BlockSpec(memory_space=pl.ANY)] * 4,
            out_specs=pl.BlockSpec(memory_space=pltpu.VMEM),
            scratch_shapes=[
                pltpu.VMEM((rows, depth), BF16),
                pltpu.VMEM((n_gu, kd, GU_COLS), BF16),
                pltpu.VMEM((n_gu, kd, GU_COLS), BF16),
                pltpu.VMEM((n_k, width, Y_COLS), BF16),
                pltpu.VMEM((rows, GU_COLS), F32),
                pltpu.VMEM((rows, GU_COLS), F32),
                pltpu.VMEM((rows, width), BF16),
                pltpu.VMEM((n_k, most, Y_COLS), F32),
                pltpu.VMEM((n_k, rows, Y_COLS), BF16),
                pltpu.VMEM((n_k, most, Y_COLS), BF16),
                pltpu.VMEM((n_k, most, Y_COLS), BF16),
                pltpu.VMEM((n_k, most, Y_COLS), BF16),
                pltpu.VMEM((n_k, most, Y_COLS), BF16),
                dma((4,)),
                dma((n_gu + width // GU_COLS,)),
                dma((n_gu + width // GU_COLS,)),
                dma((n_k,)),
                dma((n_k,)),
                dma((n_k,)),
                dma((n_k,)),
                dma((2, n_k)),
                dma((n_k,)),
                dma((n_k,)),
                dma((n_k,)),
                dma((n_k,)),
            ],
            compiler_params=pltpu.CompilerParams(
                collective_id=0, has_side_effects=True, vmem_limit_bytes=58 * 1024 * 1024
            ),
        )(x, w_gate, w_up, w_down)

    return jax.shard_map(
        step,
        mesh=mesh,
        in_specs=(P("dp", None), P(None, "tp"), P(None, "tp"), P("tp", None)),
        out_specs=P("dp", None),
        check_vma=False,
    )
```
